16 devices in a mesh: dp: 1, sp: 16 (over x, y, z, core).
Axes of the slice: x: 2, y: 2, z: 2, core: 2. Of those that a mesh axis runs over, the one named last changes fastest.
Arguments:
- x: bfloat16 [8192, 2048], P(('dp', 'sp'))
- gain: bfloat16 [2048], replicated
- wq: bfloat16 [2048, 2048], P('sp')
- wk: bfloat16 [2048, 2048], P('sp')
- wv: bfloat16 [2048, 2048], P('sp')
- wo: bfloat16 [2048, 2048], P('sp')
Outputs:
- output: bfloat16 [8192, 2048], P(('dp', 'sp'))
All inputs are finite; a program needn't handle non-finite values.
Results may differ from the reference program's by a relative error of at most 0.012.
Values are sent between devices in bfloat16 or wider.
A program may use at most 2 GiB of HBM per device.

```python
import jax
import jax.numpy as jnp
from jax import lax

ROWS = 8192
D = 2048
HEADS = 8
KV_HEADS = 8
HEAD = 256
THETA = 10000


def setup_inputs(seed: int = 0, part: int = 0) -> dict:
    kx, kn, kq, kk, kv, ko = jax.random.split(jax.random.key(seed), 6)

    def weights(key, rows, columns):
        return jax.random.normal(key, (rows, columns), jnp.float32) * rows**-0.5

    drawn = {
        "x": jax.random.normal(jax.random.fold_in(kx, part), (ROWS, D), jnp.float32),
        "gain": 1 + 0.1 * jax.random.normal(kn, (D,), jnp.float32),
        "wq": 2 * weights(kq, D, HEADS * HEAD),
        "wk": 2 * weights(kk, D, KV_HEADS * HEAD),
        "wv": 4 * weights(kv, D, KV_HEADS * HEAD),
        "wo": weights(ko, HEADS * HEAD, D),
    }
    return {k: v.astype(jnp.bfloat16) for k, v in drawn.items()}


def normed(x, gain):
    wide = x.astype(jnp.float32)
    scale = lax.rsqrt(jnp.mean(wide * wide, -1, keepdims=True) + 1e-6)
    return (wide * scale * gain.astype(jnp.float32)).astype(jnp.bfloat16)


def turned(t, place, theta):
    half = t.shape[-1] // 2
    angle = place.astype(jnp.float32)[:, None] * theta ** (-jnp.arange(half, dtype=jnp.float32) / half)
    cos, sin = jnp.cos(angle)[:, None], jnp.sin(angle)[:, None]
    a, b = t[..., :half].astype(jnp.float32), t[..., half:].astype(jnp.float32)
    return jnp.concatenate([a * cos - b * sin, b * cos + a * sin], -1).astype(jnp.bfloat16)


def matmul(a, w):
    return jnp.dot(a, w, preferred_element_type=jnp.float32).astype(jnp.bfloat16)


def einsum(form, a, b):
    return jnp.einsum(form, a.astype(jnp.float32), b.astype(jnp.float32))


def attention(q, k, v):
    scores = einsum("tgsd,ugd->gstu", q, k) * q.shape[-1] ** -0.5
    token = jnp.arange(q.shape[0])
    scores = jnp.where(token[:, None] >= token, scores, -jnp.inf)
    weights = jax.nn.softmax(scores, -1).astype(jnp.bfloat16)
    return einsum("gstu,ugd->tgsd", weights, v).astype(jnp.bfloat16)


def reference(x, gain, wq, wk, wv, wo):
    a, place = normed(x, gain), jnp.arange(ROWS)
    q = turned(matmul(a, wq).reshape(ROWS, HEADS, HEAD), place, THETA).reshape(ROWS, KV_HEADS, -1, HEAD)
    k = turned(matmul(a, wk).reshape(ROWS, KV_HEADS, HEAD), place, THETA)
    v = matmul(a, wv).reshape(ROWS, KV_HEADS, HEAD)
    seen = attention(q, k, v).reshape(ROWS, HEADS * HEAD)
    return (x.astype(jnp.float32) + jnp.dot(seen, wo, preferred_element_type=jnp.float32)).astype(jnp.bfloat16)
```

```python
import functools

import jax
import jax.numpy as jnp
import numpy as np
from jax import lax
from jax.experimental import pallas as pl
from jax.experimental.pallas import tpu as pltpu
from jax.sharding import PartitionSpec as P

NEG = -1e30
HIDDEN = 2 * NEG
LOG2E = 1.4426950408889634
HEAD = 256
THETA = 10000
D = 2048
OWN = 512
SUM = 8
F32, BF16 = jnp.float32, jnp.bfloat16
MESH = pl.DeviceIdType.MESH


def _dot(a, b, ca, cb):
    return lax.dot_general(a, b, (((ca,), (cb,)), ((), ())), preferred_element_type=F32)


def kernel(x_h, gain_ref, wq_h, wk_h, wv_h, wo_h, fine_ref, coarse_ref, y_h,
           xv, av, wi, wf, ws, wov, kv_k, kv_v, qv, ov, og, top_s, mix_s,
           ld, w_s, wf_r, ws_r, a_s, a_r, wo_s, wo_r, kv_s, kv_r, o_s, o_r):
    me = lax.axis_index("sp")
    x, y, z, c, p = me // 8, (me // 4) % 2, (me // 2) % 2, me % 2, me // 4
    X, Y, Z, C = me + 8 - 16 * x, me + 4 - 8 * y, me + 2 - 4 * z, me + 1 - 2 * c
    Dg = X + Y - me
    pX, pY, pD = X // 4, Y // 4, Dg // 4
    oc, oz = 1 - c, 1 - z
    head = 2 * p + c
    mine = 2 * p + c
    planes = (p, pX, pY, pD)

    def row(q, zz, cc):
        return 4 * q + 2 * zz + cc

    def rc(src, dst, ssem, rsem, dev):
        return pltpu.make_async_remote_copy(src_ref=src, dst_ref=dst, send_sem=ssem, recv_sem=rsem, device_id={"sp": dev}, device_id_type=MESH)

    def got(ref, sem):
        pltpu.make_async_copy(ref, ref, sem).wait()

    def local(src, dst, n):
        cp = pltpu.make_async_copy(src, dst, ld.at[n])
        cp.start()
        return cp

    loads_w = [local(w, wi.at[n], n) for n, w in enumerate((wk_h, wv_h, wq_h))]
    here = pl.ds(pl.multiple_of(head * HEAD, HEAD), HEAD)
    other = pl.ds(pl.multiple_of((2 * p + oc) * HEAD, HEAD), HEAD)
    sme = 2 * p + z
    load_x = local(x_h, xv, 3)
    load_wo = local(wo_h, wov.at[me], 4)
    loads_own = [local(w.at[:, here], wf.at[n, me], 5 + n) for n, w in enumerate((wk_h, wv_h, wq_h))]
    loads_own += [local(w.at[:, other], ws.at[n, sme], 8 + n) for n, w in enumerate((wk_h, wv_h, wq_h))]

    barrier = pltpu.get_barrier_semaphore()
    partners = (X, Y, Dg, X + C - me, Y + C - me, Dg + C - me, C, Z)
    for dev in partners:
        pl.semaphore_signal(barrier, inc=1, device_id={"sp": dev}, device_id_type=MESH)
    pl.semaphore_wait(barrier, len(partners))

    sends = []

    def send(src, dst, ssem, rsem, dev):
        cp = rc(src, dst, ssem, rsem, dev)
        cp.start()
        sends.append(cp)

    for cp in loads_w:
        cp.wait()
    for n, (dev, q) in enumerate(((X, pX), (Y, pY), (Dg, pD))):
        for m, (hd, dst, rs) in enumerate(((2 * q + c, wf.at[:, me], wf_r.at[me]), (2 * q + oc, ws.at[:, sme], ws_r.at[sme]))):
            cols = pl.ds(pl.multiple_of(hd * HEAD, HEAD), HEAD)
            send(wi.at[:, :, cols], dst, w_s.at[2 * n + m], rs, dev)

    def w_on(n, q, zz, on):
        i, s = row(q, zz, c), 2 * q + zz
        if on:
            send(wf.at[:, i], wf.at[:, i], w_s.at[6 + 2 * n], wf_r.at[i], Z)
            send(ws.at[:, s], ws.at[:, s], w_s.at[7 + 2 * n], ws_r.at[s], Z)
        send(ws.at[:, s], wf.at[:, i], w_s.at[14 + n + (0 if on else 4)], wf_r.at[i], C)

    for cp in loads_own:
        cp.wait()
    w_on(0, p, z, True)
    load_wo.wait()
    send(wov.at[me], wov.at[me], wo_s.at[0], wo_r.at[me], Z)

    load_x.wait()

    def norm(n, _):
        rows = pl.ds(pl.multiple_of(n * 128, 128), 128)
        wide = xv[rows, :].astype(F32)
        scale = lax.rsqrt(jnp.mean(wide * wide, -1, keepdims=True) + 1e-6)
        av[mine, rows, :] = (wide * scale * gain_ref[...].astype(F32)).astype(BF16)

    lax.fori_loop(0, OWN // 128, norm, None)
    lo, hi = pl.ds(0, OWN // 2), pl.ds(OWN // 2, OWN // 2)

    def send_a(b, half, n, dev):
        rows = (lo, hi)[half]
        send(av.at[b, rows], av.at[b, rows], a_s.at[n], a_r.at[b, half], dev)

    def got_a(b, half):
        rows = (lo, hi)[half]
        got(av.at[b, rows], a_r.at[b, half])

    send_a(mine, 0, 0, X)
    send_a(mine, 1, 1, Y)
    send_a(mine, 1, 2, X)
    send_a(mine, 0, 3, Y)
    send_a(mine, 0, 4, C)
    send_a(mine, 1, 5, C)

    for n, q in ((1, pX), (2, pY), (3, pD)):
        got(wf.at[:, row(q, z, c)], wf_r.at[row(q, z, c)])
        got(ws.at[:, 2 * q + z], ws_r.at[2 * q + z])
        w_on(n, q, z, True)

    bX, bY, bD = 2 * pX + c, 2 * pY + c, 2 * pD + c
    got_a(bX, 0)
    send_a(bX, 0, 6, Y)
    send_a(bX, 0, 7, C)
    got_a(bY, 1)
    send_a(bY, 1, 8, X)
    send_a(bY, 1, 9, C)

    iz = row(p, oz, c)
    got(wov.at[iz], wo_r.at[iz])
    for n, i in enumerate((row(p, 0, c), row(p, 1, c))):
        send(wov.at[i], wov.at[i], wo_s.at[1 + n], wo_r.at[i], X)
        send(wov.at[i], wov.at[i], wo_s.at[3 + n], wo_r.at[i], Y)
        send(wov.at[i], wov.at[i], wo_s.at[7 + n], wo_r.at[i], C)

    for n, q in enumerate(planes):
        i, s = row(q, oz, c), 2 * q + oz
        got(wf.at[:, i], wf_r.at[i])
        got(ws.at[:, s], ws_r.at[s])
        w_on(n, q, oz, False)
    for q in planes:
        for zz in (0, 1):
            got(wf.at[:, row(q, zz, oc)], wf_r.at[row(q, zz, oc)])

    def project(b):
        a = av[b]
        i = 4 * (b // 2) + 2 * z + b % 2
        cb, sb = coarse_ref[0, pl.ds(i, 1), :], coarse_ref[1, pl.ds(i, 1), :]
        cos = cb * fine_ref[0] - sb * fine_ref[1]
        sin = sb * fine_ref[0] + cb * fine_ref[1]

        def turned(t):
            t = t.astype(BF16).astype(F32)
            u, v = t[:, : HEAD // 2], t[:, HEAD // 2 :]
            return jnp.concatenate([u * cos - v * sin, v * cos + u * sin], -1).astype(BF16)

        kv_k[z, b] = turned(_dot(a, wf[0].reshape(D, HEAD), 1, 0))
        kv_v[z, b] = _dot(a, wf[1].reshape(D, HEAD), 1, 0).astype(BF16).T
        qv[b] = turned(_dot(a, wf[2].reshape(D, HEAD), 1, 0))

    def kv_copies(b):
        return (rc(kv_k.at[z, b], kv_k.at[z, b], kv_s.at[b, 0], kv_r.at[b, 0], Z),
                rc(kv_v.at[z, b], kv_v.at[z, b], kv_s.at[b, 1], kv_r.at[b, 1], Z))

    def projects(q, n):
        b = 2 * q + (c + n) - 2 * ((c + n) // 2)
        project(b)
        for cp in kv_copies(b):
            cp.start()

    def got_other(b):
        for half in (0, 1):
            got_a(b, half)

    got_other(2 * p + oc)
    lax.fori_loop(0, 2, lambda n, _: projects(p, n), None)
    got_a(bX, 1)
    send_a(bX, 1, 10, C)
    got_a(bY, 0)
    send_a(bY, 0, 11, C)
    got_other(2 * pX + oc)
    got_other(2 * pY + oc)
    lax.fori_loop(0, 4, lambda n, _: projects(pX + (n // 2) * (pY - pX), n), None)
    got_a(bD, 0)
    send_a(bD, 0, 12, C)
    got_a(bD, 1)
    send_a(bD, 1, 13, C)
    got_other(2 * pD + oc)
    lax.fori_loop(0, 2, lambda n, _: projects(pD, n), None)

    e = HEAD**-0.5 * LOG2E
    top_s[...] = jnp.full(top_s.shape, NEG, F32)
    mix_s[...] = jnp.zeros(mix_s.shape, F32)

    def tile(zz, kb, bq, masked):
        s = _dot(kv_k[zz, kb], qv[bq], 1, 1)
        if masked:
            ok = lax.broadcasted_iota(jnp.int32, s.shape, 1) >= lax.broadcasted_iota(jnp.int32, s.shape, 0)
            s = jnp.where(ok, s, HIDDEN)
        return s

    ones = jnp.ones((SUM, OWN), BF16)

    def attend(work):
        scores = [[tile(zz, kb, bq, masked) for zz, kb, masked in keys] for bq, keys in work]
        for (bq, keys), ss in zip(work, scores):
            old = top_s[bq]
            top = old
            for s in ss:
                top = jnp.maximum(top, s.max(axis=0, keepdims=True))
            top_s[bq] = top
            keep = jnp.exp2((old - top) * e)
            total = mix_s[bq] * keep
            for (zz, kb, _), s in zip(keys, ss):
                w = jnp.exp2((s - top) * e).astype(BF16)
                total = total + _dot(jnp.concatenate([kv_v[zz, kb], ones], axis=0), w, 1, 0)
            mix_s[bq] = total

    def pair(zz, kp, qp):
        keys = [(zz, 2 * kp, False), (zz, 2 * kp + 1, False)]
        attend([(2 * qp, keys), (2 * qp + 1, keys)])

    def local_piece(kp, _):
        attend([(2 * kp, [(z, 2 * kp, True)]), (2 * kp + 1, [(z, 2 * kp, False), (z, 2 * kp + 1, True)])])
        lax.fori_loop(kp + 1, 4, lambda qp, _: pair(z, kp, qp), None)

    lax.fori_loop(0, 4, local_piece, None)

    i0, i1 = row(pX, 0, c), row(pY, 1, c)
    for n, (i, dev) in enumerate(((i0, Y), (i1, X))):
        got(wov.at[i], wo_r.at[i])
        send(wov.at[i], wov.at[i], wo_s.at[5 + n], wo_r.at[i], dev)
        send(wov.at[i], wov.at[i], wo_s.at[9 + n], wo_r.at[i], C)
    for n, i in enumerate((row(pX, 1, c), row(pY, 0, c))):
        got(wov.at[i], wo_r.at[i])
        send(wov.at[i], wov.at[i], wo_s.at[11 + n], wo_r.at[i], C)

    for kp in planes:
        for n in (0, 1):
            got(kv_k.at[oz, 2 * kp + n], kv_r.at[2 * kp + n, 0])
            got(kv_v.at[oz, 2 * kp + n], kv_r.at[2 * kp + n, 1])
        lax.fori_loop(kp + 1 - z, 4, lambda qp, _: pair(oz, kp, qp), None)

    cols = pl.ds(pl.multiple_of(head * HEAD, HEAD), HEAD)

    def finish(bq):
        mix = mix_s[bq]
        return (mix[:HEAD] * (1 / mix[HEAD : HEAD + 1])).T.astype(BF16)

    def finish_all(bq, _):
        ov[bq] = finish(bq)

    lax.fori_loop(0, 8, finish_all, None)
    n = 0
    for q in (pX, pY, pD, p):
        for cc in (c, oc):
            dev = row(q, z, cc)
            if q is p and cc is c:
                og[:, cols] = ov[mine]
            else:
                send(ov.at[2 * q + cc], og.at[:, cols], o_s.at[n], o_r.at[head], dev)
            n += 1

    for n, i in enumerate((row(pD, 0, c), row(pD, 1, c))):
        got(wov.at[i], wo_r.at[i])
        send(wov.at[i], wov.at[i], wo_s.at[13 + n], wo_r.at[i], C)
    for q in planes:
        for zz in (0, 1):
            got(wov.at[row(q, zz, oc)], wo_r.at[row(q, zz, oc)])
    for q in planes:
        for cc in (c, oc):
            if not (q is p and cc is c):
                hd = 2 * q + cc
                got(og.at[:, pl.ds(pl.multiple_of(hd * HEAD, HEAD), HEAD)], o_r.at[hd])

    def out(n, _):
        cols = pl.ds(pl.multiple_of(n * 256, 256), 256)
        y = _dot(og[...], wov[:, :, cols].reshape(D, 256), 1, 0)
        xv[:, cols] = (xv[:, cols].astype(F32) + y).astype(BF16)

    lax.fori_loop(0, D // 256, out, None)
    local(xv, y_h, 11).wait()

    for cp in sends:
        cp.wait_send()

    def sent(b, _):
        for cp in kv_copies(b):
            cp.wait_send()

    lax.fori_loop(0, 8, sent, None)


def tables():
    half = HEAD // 2
    rate = (THETA ** (-np.arange(half, dtype=np.float64) / half))[None]
    fine = np.arange(OWN, dtype=np.float64)[:, None] * rate
    coarse = np.arange(16, dtype=np.float64)[:, None] * OWN * rate
    return (np.stack([np.cos(t), np.sin(t)]).astype(np.float32) for t in (fine, coarse))


def solution(mesh):
    def step(x, gain, wq, wk, wv, wo):
        fine, coarse = tables()
        anywhere, vmem = pl.BlockSpec(memory_space=pltpu.HBM), pl.BlockSpec(memory_space=pltpu.VMEM)
        dma = pltpu.SemaphoreType.DMA
        return pl.pallas_call(
            kernel,
            out_shape=jax.ShapeDtypeStruct((OWN, D), BF16),
            in_specs=[anywhere, vmem, anywhere, anywhere, anywhere, anywhere, vmem, vmem],
            out_specs=anywhere,
            scratch_shapes=[
                pltpu.VMEM((OWN, D), BF16),
                pltpu.VMEM((8, OWN, D), BF16),
                pltpu.VMEM((3, 128, D), BF16),
                pltpu.VMEM((3, 16, 128, HEAD), BF16),
                pltpu.VMEM((3, 8, 128, HEAD), BF16),
                pltpu.VMEM((16, 128, D), BF16),
                pltpu.VMEM((2, 8, OWN, HEAD), BF16),
                pltpu.VMEM((2, 8, HEAD, OWN), BF16),
                pltpu.VMEM((8, OWN, HEAD), BF16),
                pltpu.VMEM((8, OWN, HEAD), BF16),
                pltpu.VMEM((OWN, D), BF16),
                pltpu.VMEM((8, 1, OWN), F32),
                pltpu.VMEM((8, HEAD + SUM, OWN), F32),
                dma((12,)), dma((22,)), dma((16,)), dma((8,)), dma((14,)), dma((8, 2)), dma((15,)), dma((16,)),
                dma((8, 2)), dma((8, 2)), dma((8,)), dma((8,)),
            ],
            compiler_params=pltpu.CompilerParams(collective_id=0, has_side_effects=True, vmem_limit_bytes=67043328),
            name="decoder_attention",
        )(x, gain.reshape(1, D), wq, wk, wv, wo, jnp.asarray(fine), jnp.asarray(coarse))

    tokens, whole = P(("dp", "sp"), None), P("sp", None)
    return jax.shard_map(
        step,
        mesh=mesh,
        in_specs=(tokens, P(None), whole, whole, whole, whole),
        out_specs=tokens,
        check_vma=False,
    )
```

```python
import functools

import jax
import jax.numpy as jnp
import numpy as np
from jax import lax
from jax.experimental import pallas as pl
from jax.experimental.pallas import tpu as pltpu
from jax.sharding import PartitionSpec as P

NEG = -1e30
HIDDEN = 2 * NEG
LOG2E = 1.4426950408889634
HEAD = 256
THETA = 10000
D = 2048
OWN = 512
HALF = 256
SUM = 8
F32, BF16 = jnp.float32, jnp.bfloat16
MESH = pl.DeviceIdType.MESH


def _dot(a, b, ca, cb):
    return lax.dot_general(a, b, (((ca,), (cb,)), ((), ())), preferred_element_type=F32)


def kernel(x_h, gain_ref, wq_h, wk_h, wv_h, wo_h, fine_ref, coarse_ref, y_h,
           xv, av, wi, wf, ws, wov, kv_k, kv_v, qv, ov, og, top_s, mix_s, part, part_f,
           ld, w_s, wf_r, ws_r, a_s, a_r, wo_s, wo_r, kv_s, kv_r, o_s, o_r, q_s, q_r, part_s, part_r):
    me = lax.axis_index("sp")
    x, y, z, c, p = me // 8, (me // 4) % 2, (me // 2) % 2, me % 2, me // 4
    X, Y, Z, C = me + 8 - 16 * x, me + 4 - 8 * y, me + 2 - 4 * z, me + 1 - 2 * c
    Dg = X + Y - me
    pX, pY, pD = X // 4, Y // 4, Dg // 4
    oc, oz = 1 - c, 1 - z
    head = 2 * p + c
    mine = 2 * p + c
    planes = (p, pX, pY, pD)

    def row(q, zz, cc):
        return 4 * q + 2 * zz + cc

    def rc(src, dst, ssem, rsem, dev):
        return pltpu.make_async_remote_copy(src_ref=src, dst_ref=dst, send_sem=ssem, recv_sem=rsem, device_id={"sp": dev}, device_id_type=MESH)

    def got(ref, sem, name="wait"):
        with jax.named_scope(name):
            pltpu.make_async_copy(ref, ref, sem).wait()

    def local(src, dst, n):
        cp = pltpu.make_async_copy(src, dst, ld.at[n])
        cp.start()
        return cp

    loads_w = [local(w, wi.at[n], n) for n, w in enumerate((wk_h, wv_h, wq_h))]
    here = pl.ds(pl.multiple_of(head * HEAD, HEAD), HEAD)
    other = pl.ds(pl.multiple_of((2 * p + oc) * HEAD, HEAD), HEAD)
    sme = 2 * p + z
    load_x = local(x_h, xv, 3)
    load_wo = local(wo_h, wov.at[me], 4)
    loads_own = [local(w.at[:, here], wf.at[n, me], 5 + n) for n, w in enumerate((wk_h, wv_h, wq_h))]
    loads_own += [local(w.at[:, other], ws.at[n, sme], 8 + n) for n, w in enumerate((wk_h, wv_h, wq_h))]

    barrier = pltpu.get_barrier_semaphore()
    partners = (X, Y, Dg, X + C - me, Y + C - me, Dg + C - me, C, Z)
    for dev in partners:
        pl.semaphore_signal(barrier, inc=1, device_id={"sp": dev}, device_id_type=MESH)
    pl.semaphore_wait(barrier, len(partners))

    sends = []

    def send(src, dst, ssem, rsem, dev):
        cp = rc(src, dst, ssem, rsem, dev)
        cp.start()
        sends.append(cp)

    for cp in loads_w:
        cp.wait()
    for n, (dev, q) in enumerate(((X, pX), (Y, pY), (Dg, pD))):
        for m, (hd, dst, rs) in enumerate(((2 * q + c, wf.at[:, me], wf_r.at[me]), (2 * q + oc, ws.at[:, sme], ws_r.at[sme]))):
            cols = pl.ds(pl.multiple_of(hd * HEAD, HEAD), HEAD)
            send(wi.at[:, :, cols], dst, w_s.at[2 * n + m], rs, dev)

    def w_on(n, q, zz, on):
        i, s = row(q, zz, c), 2 * q + zz
        if on:
            send(wf.at[:, i], wf.at[:, i], w_s.at[6 + 2 * n], wf_r.at[i], Z)
            send(ws.at[:, s], ws.at[:, s], w_s.at[7 + 2 * n], ws_r.at[s], Z)
        send(ws.at[:, s], wf.at[:, i], w_s.at[14 + n + (0 if on else 4)], wf_r.at[i], C)

    for cp in loads_own:
        cp.wait()
    w_on(0, p, z, True)

    load_x.wait()

    @jax.named_scope("norm")
    def norm(n, _):
        rows = pl.ds(pl.multiple_of(n * 128, 128), 128)
        wide = xv[rows, :].astype(F32)
        scale = lax.rsqrt(jnp.mean(wide * wide, -1, keepdims=True) + 1e-6)
        av[mine, rows, :] = (wide * scale * gain_ref[...].reshape(1, D).astype(F32)).astype(BF16)

    lax.fori_loop(0, OWN // 128, norm, None)

    def half_rows(half):
        return pl.ds(half * HALF if isinstance(half, int) else pl.multiple_of(half * HALF, HALF), HALF)

    def send_a(b, half, n, dev):
        rows = half_rows(half)
        send(av.at[b, rows], av.at[b, rows], a_s.at[n], a_r.at[b, half], dev)

    def got_a(b, half):
        got(av.at[b, half_rows(half)], a_r.at[b, half], f"a{half}" if isinstance(half, int) else "a")

    send_a(mine, 0, 0, X)
    send_a(mine, 1, 1, Y)
    send_a(mine, 1, 2, X)
    send_a(mine, 0, 3, Y)
    send_a(mine, 0, 4, C)
    send_a(mine, 1, 5, C)

    for n, q in ((1, pX), (2, pY), (3, pD)):
        got(wf.at[:, row(q, z, c)], wf_r.at[row(q, z, c)], f"w_plane{n}")
        got(ws.at[:, 2 * q + z], ws_r.at[2 * q + z])
        w_on(n, q, z, True)
    load_wo.wait()
    send(wov.at[me], wov.at[me], wo_s.at[0], wo_r.at[me], Z)

    for n, q in enumerate(planes):
        i, s = row(q, oz, c), 2 * q + oz
        got(wf.at[:, i], wf_r.at[i], f"w_z{n}")
        got(ws.at[:, s], ws_r.at[s])
        w_on(n, q, oz, False)
    for q in planes:
        for zz in (0, 1):
            got(wf.at[:, row(q, zz, oc)], wf_r.at[row(q, zz, oc)])

    @jax.named_scope("project")
    def project(b, half):
        rows = half_rows(half)
        a = av[b, rows, :]
        i = 4 * (b // 2) + 2 * z + b % 2
        cb, sb = coarse_ref[0, pl.ds(i, 1), :], coarse_ref[1, pl.ds(i, 1), :]
        cf, sf = fine_ref[0, rows, :], fine_ref[1, rows, :]
        cos = cb * cf - sb * sf
        sin = sb * cf + cb * sf

        def turned(t):
            t = t.astype(BF16).astype(F32)
            u, v = t[:, : HEAD // 2], t[:, HEAD // 2 :]
            return jnp.concatenate([u * cos - v * sin, v * cos + u * sin], -1).astype(BF16)

        kv_k[z, b, rows, :] = turned(_dot(a, wf[0].reshape(D, HEAD), 1, 0))
        kv_v[z, b, :, rows] = _dot(a, wf[1].reshape(D, HEAD), 1, 0).astype(BF16).T
        qv[b, rows, :] = turned(_dot(a, wf[2].reshape(D, HEAD), 1, 0))

    def kv_copies(b, half):
        rows = half_rows(half)
        return (rc(kv_k.at[z, b, rows, :], kv_k.at[z, b, rows, :], kv_s.at[b, half, 0], kv_r.at[b, half, 0], Z),
                rc(kv_v.at[z, b, :, rows], kv_v.at[z, b, :, rows], kv_s.at[b, half, 1], kv_r.at[b, half, 1], Z))

    def q_copy(b, half):
        rows = half_rows(half)
        return rc(qv.at[b, rows, :], qv.at[b + 2, rows, :], q_s.at[b - 6, half], q_r.at[b - 6, half], Z)

    def send_kv(b, half):
        for cp in kv_copies(b, half):
            cp.start()

    def on(b, half):
        @pl.when(b < 6)
        def _():
            send_kv(b, half)

        @pl.when((b >= 6) & (z == 1))
        def _():
            q_copy(b, half).start()

    def core(n):
        return c + n * (oc - c)

    def own_piece(q):
        def body(n, _):
            b, half = 2 * q + core(n // 2), n % 2
            project(b, half)
            on(b, half)

        lax.fori_loop(0, 4, body, None)

    def side_half(t, n):
        return 2 * (pX + n % 2 * (pY - pX)) + core(n // 2), (n % 2 + t) % 2

    hold = (p == 0) & (z == 1)

    def side_pieces(t):
        def body(n, _):
            b, half = side_half(t, n)
            project(b, half)
            if t == 0:
                on(b, half)
            else:
                pl.when(jnp.logical_not(hold))(lambda: on(b, half))

        lax.fori_loop(0, 4, body, None)

    for half in (0, 1):
        got_a(2 * p + oc, half)
    own_piece(p)

    bX, bY, bD = 2 * pX + c, 2 * pY + c, 2 * pD + c
    got_a(bX, 0)
    send_a(bX, 0, 6, Y)
    send_a(bX, 0, 7, C)
    got_a(bY, 1)
    send_a(bY, 1, 8, X)
    send_a(bY, 1, 9, C)
    got_a(2 * pX + oc, 0)
    got_a(2 * pY + oc, 1)
    side_pieces(0)

    iz = row(p, oz, c)
    got(wov.at[iz], wo_r.at[iz], "wo_z")
    i0, i1 = row(p, 0, c), row(p, 1, c)
    for n, (i, dev) in enumerate(((i0, X), (i1, Y), (i1, X), (i0, Y), (i0, C), (i1, C))):
        send(wov.at[i], wov.at[i], wo_s.at[1 + n], wo_r.at[i], dev)

    e = HEAD**-0.5 * LOG2E
    top_s[...] = jnp.full(top_s.shape, NEG, F32)
    mix_s[...] = jnp.zeros(mix_s.shape, F32)

    def tile(zz, kb, bq, masked):
        s = _dot(kv_k[zz, kb], qv[bq], 1, 1)
        if masked:
            ok = lax.broadcasted_iota(jnp.int32, s.shape, 1) >= lax.broadcasted_iota(jnp.int32, s.shape, 0)
            s = jnp.where(ok, s, HIDDEN)
        return s

    ones = jnp.ones((SUM, OWN), BF16)

    def attend(work):
        scores = [[tile(zz, kb, bq, masked) for zz, kb, masked in keys] for bq, keys in work]
        for (bq, keys), ss in zip(work, scores):
            old = top_s[bq]
            top = old
            for s in ss:
                top = jnp.maximum(top, s.max(axis=0, keepdims=True))
            top_s[bq] = top
            keep = jnp.exp2((old - top) * e)
            total = mix_s[bq] * keep
            for (zz, kb, _), s in zip(keys, ss):
                w = jnp.exp2((s - top) * e).astype(BF16)
                total = total + _dot(jnp.concatenate([kv_v[zz, kb], ones], axis=0), w, 1, 0)
            mix_s[bq] = total

    @jax.named_scope("pair")
    def pair(zz, kp, qp):
        keys = [(zz, 2 * kp, False), (zz, 2 * kp + 1, False)]
        attend([(2 * qp, keys), (2 * qp + 1, keys)])

    @jax.named_scope("diagonal")
    def diagonal(kp):
        attend([(2 * kp, [(z, 2 * kp, True)]), (2 * kp + 1, [(z, 2 * kp, False), (z, 2 * kp + 1, True)])])

    got_a(bX, 1)
    send_a(bX, 1, 10, C)
    got_a(bY, 0)
    send_a(bY, 0, 11, C)
    got_a(2 * pX + oc, 1)
    got_a(2 * pY + oc, 0)
    side_pieces(1)
    even = 1 - (x + y) % 2

    def near(n, _):
        diagonal(p * (n == 0) + pX * (n == 1) + pY * (n == 2))
        low = y * (n == 0) + 2 * x * (n == 1) + even * (n == 2)
        high = (y + 2) * (n == 0) + (2 * x + 1) * (n == 1) + (3 - even) * (n == 2)
        pair(z, low, high)

    lax.fori_loop(0, 3, near, None)

    for half in (0, 1):
        got_a(bD, half)
        send_a(bD, half, 12 + half, C)
    for half in (0, 1):
        got_a(2 * pD + oc, half)
    own_piece(pD)

    @pl.when(hold)
    def _():
        for n in range(4):
            send_kv(*side_half(1, n))

    diagonal(pD)

    def far(n, _):
        low = (1 - even) * (n == 0) + 2 * (1 - x) * (n == 1) + (1 - y) * (n == 2)
        high = (2 + even) * (n == 0) + (3 - 2 * x) * (n == 1) + (3 - y) * (n == 2)
        pair(z, low, high)

    lax.fori_loop(0, 3, far, None)

    for n, (i, dev) in enumerate(((row(pX, 0, c), Y), (row(pY, 1, c), X), (row(pX, 1, c), C), (row(pY, 0, c), C))):
        got(wov.at[i], wo_r.at[i], f"wo{n}")
        send(wov.at[i], wov.at[i], wo_s.at[7 + n], wo_r.at[i], dev)
        if n < 2:
            send(wov.at[i], wov.at[i], wo_s.at[11 + n], wo_r.at[i], C)

    cols = pl.ds(pl.multiple_of(head * HEAD, HEAD), HEAD)

    def o_copy(b):
        return rc(ov.at[b], og.at[:, cols], o_s.at[b], o_r.at[head], row(b // 2, z, b % 2))

    def finish(b, _):
        with jax.named_scope("finish"):
            mix = mix_s[b]
            ov[b] = (mix[:HEAD] * (1 / mix[HEAD : HEAD + 1])).T.astype(BF16)

        @pl.when(b != mine)
        def _():
            o_copy(b).start()

    def finish_pieces(first, last):
        lax.fori_loop(2 * first, 2 * last, finish, None)

    first, last = (3 - p) // 3, p // 3
    kp0, kp1 = p - 2 * last, first + 2 * last
    done0, done1 = first, 2 * ((3 - p) // 2) + p // 2 * (3 - p)

    def remote_piece(kp):
        for n in (0, 1):
            for half in (0, 1):
                rows = half_rows(half)
                got(kv_k.at[oz, 2 * kp + n, rows, :], kv_r.at[2 * kp + n, half, 0], "kv")
                got(kv_v.at[oz, 2 * kp + n, :, rows], kv_r.at[2 * kp + n, half, 1], "kv")
        lax.fori_loop(kp + 1 - z, 4, lambda qp, _: pair(oz, kp, qp), None)

    finish_pieces(0, oz)
    remote_piece(kp0)
    finish_pieces(oz, done0 + oz)

    def part_copies():
        return (rc(part.at[0], part.at[1], part_s.at[0], part_r.at[0], Z), rc(part_f.at[0], part_f.at[1], part_s.at[1], part_r.at[1], Z))

    @pl.when(z == 0)
    def _():
        for n in (0, 1):
            for half in (0, 1):
                got(qv.at[8 + n, half_rows(half), :], q_r.at[n, half], "q")
        pair(z, 3, 4)
        for n in (0, 1):
            mix = mix_s[8 + n]
            total = mix[HEAD : HEAD + 1]
            part[0, n] = (mix[:HEAD] * (1 / total)).astype(BF16)
            part_f[0, n] = jnp.concatenate([top_s[8 + n], total], axis=0)
        for cp in part_copies():
            cp.start()

    remote_piece(kp1)
    finish_pieces(done0 + oz, done1 + oz)
    remote_piece(3 - kp0 - kp1)
    finish_pieces(done1 + oz, 3)

    @pl.when(z == 1)
    def _():
        got(part.at[1], part_r.at[0], "part")
        got(part_f.at[1], part_r.at[1], "part")
        for n in (0, 1):
            old, came, count = top_s[6 + n], part_f[1, n, 0:1], part_f[1, n, 1:2]
            top = jnp.maximum(old, came)
            keep, add = jnp.exp2((old - top) * e), jnp.exp2((came - top) * e) * count
            mix = mix_s[6 + n]
            more = jnp.concatenate([part[1, n].astype(F32) * add, jnp.broadcast_to(add, (SUM, OWN))], axis=0)
            mix_s[6 + n] = mix * keep + more

    finish_pieces(3, 4)

    for n, i in enumerate((row(pD, 0, c), row(pD, 1, c))):
        got(wov.at[i], wo_r.at[i], f"wo_d{n}")
        send(wov.at[i], wov.at[i], wo_s.at[13 + n], wo_r.at[i], C)
    og[:, cols] = ov[mine]
    for k, q in enumerate(planes):
        for zz in (0, 1):
            got(wov.at[row(q, zz, oc)], wo_r.at[row(q, zz, oc)], "wo_c")
        for cc in (c, oc):
            if k or cc is oc:
                hd = 2 * q + cc
                got(og.at[:, pl.ds(pl.multiple_of(hd * HEAD, HEAD), HEAD)], o_r.at[hd], "og")
        heads = pl.ds(pl.multiple_of(q * 2 * HEAD, 2 * HEAD), 2 * HEAD)

        def out(n, _):
            cols = pl.ds(pl.multiple_of(n * 512, 512), 512)
            with jax.named_scope("out"):
                t = _dot(og[:, heads], wov[pl.ds(4 * q, 4), :, cols].reshape(2 * HEAD, 512), 1, 0)
                for m in range(2):
                    rows = pl.ds(m * HEAD, HEAD)
                    u = t[m * HEAD : (m + 1) * HEAD]
                    if k:
                        u = mix_s[2 * n + m, :HEAD, :] + u
                    if k < 3:
                        mix_s[2 * n + m, :HEAD, :] = u
                    else:
                        xv[rows, cols] = (xv[rows, cols].astype(F32) + u).astype(BF16)

        lax.fori_loop(0, D // 512, out, None)
    local(xv, y_h, 11).wait()

    for cp in sends:
        cp.wait_send()

    def kv_left(n, _):
        for cp in kv_copies(n // 2, n % 2):
            cp.wait_send()

    lax.fori_loop(0, 12, kv_left, None)

    def o_left(b, _):
        @pl.when(b != mine)
        def _():
            o_copy(b).wait_send()

    lax.fori_loop(0, 8, o_left, None)

    @pl.when(z == 1)
    def _():
        for n in (0, 1):
            for half in (0, 1):
                q_copy(6 + n, half).wait_send()

    @pl.when(z == 0)
    def _():
        for cp in part_copies():
            cp.wait_send()


def tables():
    half = HEAD // 2
    rate = (THETA ** (-np.arange(half, dtype=np.float64) / half))[None]
    fine = np.arange(OWN, dtype=np.float64)[:, None] * rate
    coarse = np.arange(16, dtype=np.float64)[:, None] * OWN * rate
    return (np.stack([np.cos(t), np.sin(t)]).astype(np.float32) for t in (fine, coarse))


def solution(mesh):
    def step(x, gain, wq, wk, wv, wo):
        fine, coarse = tables()
        anywhere, vmem = pl.BlockSpec(memory_space=pltpu.HBM), pl.BlockSpec(memory_space=pltpu.VMEM)
        dma = pltpu.SemaphoreType.DMA
        return pl.pallas_call(
            kernel,
            out_shape=jax.ShapeDtypeStruct((OWN, D), BF16),
            in_specs=[anywhere, vmem, anywhere, anywhere, anywhere, anywhere, vmem, vmem],
            out_specs=anywhere,
            scratch_shapes=[
                pltpu.VMEM((OWN, D), BF16),
                pltpu.VMEM((8, OWN, D), BF16),
                pltpu.VMEM((3, 128, D), BF16),
                pltpu.VMEM((3, 16, 128, HEAD), BF16),
                pltpu.VMEM((3, 8, 128, HEAD), BF16),
                pltpu.VMEM((16, 128, D), BF16),
                pltpu.VMEM((2, 8, OWN, HEAD), BF16),
                pltpu.VMEM((2, 8, HEAD, OWN), BF16),
                pltpu.VMEM((10, OWN, HEAD), BF16),
                pltpu.VMEM((8, OWN, HEAD), BF16),
                pltpu.VMEM((OWN, D), BF16),
                pltpu.VMEM((10, 1, OWN), F32),
                pltpu.VMEM((10, HEAD + SUM, OWN), F32),
                pltpu.VMEM((2, 2, HEAD, OWN), BF16),
                pltpu.VMEM((2, 2, 2, OWN), F32),
                dma((12,)), dma((22,)), dma((16,)), dma((8,)), dma((14,)), dma((8, 2)), dma((15,)), dma((16,)),
                dma((8, 2, 2)), dma((8, 2, 2)), dma((8,)), dma((8,)), dma((2, 2)), dma((2, 2)), dma((2,)), dma((2,)),
            ],
            compiler_params=pltpu.CompilerParams(collective_id=0, has_side_effects=True, vmem_limit_bytes=67043328),
            name="decoder_attention",
        )(x, gain, wq, wk, wv, wo, jnp.asarray(fine), jnp.asarray(coarse))

    tokens, whole = P(("dp", "sp"), None), P("sp", None)
    return jax.shard_map(
        step,
        mesh=mesh,
        in_specs=(tokens, P(None), whole, whole, whole, whole),
        out_specs=tokens,
        check_vma=False,
    )
```

```python
import functools

import jax
import jax.numpy as jnp
import numpy as np
from jax import lax
from jax.experimental import pallas as pl
from jax.experimental.pallas import tpu as pltpu
from jax.sharding import PartitionSpec as P

NEG = -1e30
HIDDEN = 2 * NEG
LOG2E = 1.4426950408889634
HEAD = 256
THETA = 10000
D = 2048
OWN = 512
HALF = 256
SUM = 8
F32, BF16 = jnp.float32, jnp.bfloat16
MESH = pl.DeviceIdType.MESH


def _dot(a, b, ca, cb):
    return lax.dot_general(a, b, (((ca,), (cb,)), ((), ())), preferred_element_type=F32)


def kernel(x_h, gain_h, wq_h, wk_h, wv_h, wo_h, fine_h, coarse_h, y_h,
           gain_ref, fine_ref, coarse_ref, xv, av, wi, wf, ws, wov, kv_k, kv_v, qv, ov, og, top_s, mix_s, part, part_f, orl,
           ld, w_s, wf_r, ws_r, a_s, a_r, wo_s, wo_r, kv_s, kv_r, o_s, o_r, q_s, q_r, part_s, part_r, wod_r, orl_s, orl_r, y_s):
    me = lax.axis_index("sp")
    x, y, z, c, p = me // 8, (me // 4) % 2, (me // 2) % 2, me % 2, me // 4
    X, Y, Z, C = me + 8 - 16 * x, me + 4 - 8 * y, me + 2 - 4 * z, me + 1 - 2 * c
    Dg = X + Y - me
    pX, pY, pD = X // 4, Y // 4, Dg // 4
    oc, oz = 1 - c, 1 - z
    head = 2 * p + c
    mine = 2 * p + c
    planes = (p, pX, pY, pD)

    def row(q, zz, cc):
        return 4 * q + 2 * zz + cc

    def rc(src, dst, ssem, rsem, dev):
        return pltpu.make_async_remote_copy(src_ref=src, dst_ref=dst, send_sem=ssem, recv_sem=rsem, device_id={"sp": dev}, device_id_type=MESH)

    def got(ref, sem, name="wait"):
        with jax.named_scope(name):
            pltpu.make_async_copy(ref, ref, sem).wait()

    def local(src, dst, n):
        cp = pltpu.make_async_copy(src, dst, ld.at[n])
        cp.start()
        return cp

    loads_w = [local(w, wi.at[n], n) for n, w in enumerate((wk_h, wv_h, wq_h))]
    here = pl.ds(pl.multiple_of(head * HEAD, HEAD), HEAD)
    other = pl.ds(pl.multiple_of((2 * p + oc) * HEAD, HEAD), HEAD)
    sme = 2 * p + z
    load_x = local(x_h, xv, 3)
    load_gain = local(gain_h, gain_ref, 11)
    load_tables = (local(fine_h, fine_ref, 12), local(coarse_h, coarse_ref, 13))
    load_wo = local(wo_h, wov.at[me], 4)
    loads_own = [local(w.at[:, here], wf.at[n, me], 5 + n) for n, w in enumerate((wk_h, wv_h, wq_h))]
    loads_own += [local(w.at[:, other], ws.at[n, sme], 8 + n) for n, w in enumerate((wk_h, wv_h, wq_h))]

    barrier = pltpu.get_barrier_semaphore()
    partners = (X, Y, Dg, X + C - me, Y + C - me, Dg + C - me, C, Z)
    for dev in partners:
        pl.semaphore_signal(barrier, inc=1, device_id={"sp": dev}, device_id_type=MESH)
    with jax.named_scope("barrier"):
        pl.semaphore_wait(barrier, len(partners))

    sends = []

    def send(src, dst, ssem, rsem, dev):
        cp = rc(src, dst, ssem, rsem, dev)
        cp.start()
        sends.append(cp)

    with jax.named_scope("load"):
        for cp in loads_w:
            cp.wait()
    for n, (dev, q) in enumerate(((X, pX), (Y, pY), (Dg, pD))):
        for m, (hd, dst, rs) in enumerate(((2 * q + c, wf.at[:, me], wf_r.at[me]), (2 * q + oc, ws.at[:, sme], ws_r.at[sme]))):
            cols = pl.ds(pl.multiple_of(hd * HEAD, HEAD), HEAD)
            send(wi.at[:, :, cols], dst, w_s.at[2 * n + m], rs, dev)

    def wf_on(n, q, zz):
        i = row(q, zz, c)
        send(wf.at[:, i], wf.at[:, i], w_s.at[6 + 2 * n], wf_r.at[i], Z)

    def ws_on(n, q, zz, on):
        i, s = row(q, zz, c), 2 * q + zz
        if on:
            send(ws.at[:, s], ws.at[:, s], w_s.at[7 + 2 * n], ws_r.at[s], Z)
        send(ws.at[:, s], wf.at[:, i], w_s.at[14 + n + (0 if on else 4)], wf_r.at[i], C)

    def got_wf(n, q, zz):
        got(wf.at[:, row(q, zz, c)], wf_r.at[row(q, zz, c)], f"wf{n}")

    def got_ws(n, q, zz):
        got(ws.at[:, 2 * q + zz], ws_r.at[2 * q + zz], f"ws{n}")

    for cp in loads_own:
        cp.wait()
    wf_on(0, p, z)
    ws_on(0, p, z, True)

    load_x.wait()
    load_gain.wait()

    @jax.named_scope("norm")
    def norm(n, _):
        rows = pl.ds(pl.multiple_of(n * 128, 128), 128)
        wide = xv[rows, :].astype(F32)
        scale = lax.rsqrt(jnp.mean(wide * wide, -1, keepdims=True) + 1e-6)
        av[mine, rows, :] = (wide * scale * gain_ref[...].reshape(1, D).astype(F32)).astype(BF16)

    lax.fori_loop(0, OWN // 128, norm, None)

    def half_rows(half):
        return pl.ds(half * HALF if isinstance(half, int) else pl.multiple_of(half * HALF, HALF), HALF)

    def send_a(b, half, n, dev):
        rows = half_rows(half)
        send(av.at[b, rows], av.at[b, rows], a_s.at[n], a_r.at[b, half], dev)

    def got_a(b, half):
        got(av.at[b, half_rows(half)], a_r.at[b, half], f"a{half}" if isinstance(half, int) else "a")

    send_a(mine, 0, 0, X)
    send_a(mine, 1, 1, Y)
    send_a(mine, 1, 2, X)
    send_a(mine, 0, 3, Y)
    send_a(mine, 0, 4, C)
    send_a(mine, 1, 5, C)

    for n, q in ((1, pX), (2, pY)):
        got_wf(n, q, z)
        wf_on(n, q, z)
    for n, q in ((1, pX), (2, pY)):
        got_ws(n, q, z)
        ws_on(n, q, z, True)
    got_wf(3, pD, z)
    wf_on(3, pD, z)
    got_ws(3, pD, z)
    ws_on(3, pD, z, True)
    load_wo.wait()
    send(wov.at[me], wov.at[me], wo_s.at[0], wo_r.at[me], Z)

    for n, q in enumerate(planes):
        got_wf(n, q, oz)
        got_ws(n, q, oz)
        ws_on(n, q, oz, False)
    for q in planes:
        for zz in (0, 1):
            got(wf.at[:, row(q, zz, oc)], wf_r.at[row(q, zz, oc)])

    @jax.named_scope("project")
    def project(b, half):
        rows = half_rows(half)
        a = av[b, rows, :]
        i = 4 * (b // 2) + 2 * z + b % 2
        cb, sb = coarse_ref[0, pl.ds(i, 1), :], coarse_ref[1, pl.ds(i, 1), :]
        cf, sf = fine_ref[0, rows, :], fine_ref[1, rows, :]
        cos = cb * cf - sb * sf
        sin = sb * cf + cb * sf

        def turned(t):
            t = t.astype(BF16).astype(F32)
            u, v = t[:, : HEAD // 2], t[:, HEAD // 2 :]
            return jnp.concatenate([u * cos - v * sin, v * cos + u * sin], -1).astype(BF16)

        kv_k[z, b, rows, :] = turned(_dot(a, wf[0].reshape(D, HEAD), 1, 0))
        kv_v[z, b, :, rows] = _dot(a, wf[1].reshape(D, HEAD), 1, 0).astype(BF16).T
        qv[b, rows, :] = turned(_dot(a, wf[2].reshape(D, HEAD), 1, 0))

    def kv_copies(b, half):
        rows = half_rows(half)
        return (rc(kv_k.at[z, b, rows, :], kv_k.at[z, b, rows, :], kv_s.at[b, half, 0], kv_r.at[b, half, 0], Z),
                rc(kv_v.at[z, b, :, rows], kv_v.at[z, b, :, rows], kv_s.at[b, half, 1], kv_r.at[b, half, 1], Z))

    def q_copy(b, half):
        rows = half_rows(half)
        return rc(qv.at[b, rows, :], qv.at[b + 2, rows, :], q_s.at[b - 6, half], q_r.at[b - 6, half], Z)

    def send_kv(b, half):
        for cp in kv_copies(b, half):
            cp.start()

    def on(b, half):
        @pl.when(b < 6)
        def _():
            send_kv(b, half)

        @pl.when((b >= 6) & (z == 1))
        def _():
            q_copy(b, half).start()

    def core(n):
        return c + n * (oc - c)

    def own_piece(q):
        def body(n, _):
            b, half = 2 * q + core(n // 2), n % 2
            project(b, half)
            on(b, half)

        lax.fori_loop(0, 4, body, None)

    def side_half(t, n):
        isy = n % 2 if t == 0 else 1 - n // 2
        return 2 * (pX + isy * (pY - pX)) + core(n // 2 if t == 0 else n % 2), (isy + t) % 2

    hold = (p == 0) & (z == 1)
    hold_y = p == 3

    def side_pieces(t):
        def body(n, _):
            b, half = side_half(t, n)
            project(b, half)
            if t == 0:
                on(b, half)
            else:
                @pl.when(jnp.logical_not(hold | (hold_y & (n < 2))))
                def _():
                    on(b, half)

        lax.fori_loop(0, 4, body, None)

    for cp in load_tables:
        cp.wait()
    for half in (0, 1):
        got_a(2 * p + oc, half)
    own_piece(p)

    bX, bY, bD = 2 * pX + c, 2 * pY + c, 2 * pD + c
    got_a(bX, 0)
    send_a(bX, 0, 6, Y)
    send_a(bX, 0, 7, C)
    got_a(bY, 1)
    send_a(bY, 1, 8, X)
    send_a(bY, 1, 9, C)
    got_a(2 * pX + oc, 0)
    got_a(2 * pY + oc, 1)
    side_pieces(0)

    iz = row(p, oz, c)
    got(wov.at[iz], wo_r.at[iz], "wo_z")
    for n, (i, dev) in enumerate(((me, X), (me, Y), (iz, X), (iz, Y), (me, C), (iz, C))):
        send(wov.at[i], wov.at[i], wo_s.at[1 + n], wo_r.at[i], dev)

    e = HEAD**-0.5 * LOG2E
    top_s[...] = jnp.full(top_s.shape, NEG, F32)
    mix_s[...] = jnp.zeros(mix_s.shape, F32)

    def tile(zz, kb, bq, masked):
        s = _dot(kv_k[zz, kb], qv[bq], 1, 1)
        if masked:
            ok = lax.broadcasted_iota(jnp.int32, s.shape, 1) >= lax.broadcasted_iota(jnp.int32, s.shape, 0)
            s = jnp.where(ok, s, HIDDEN)
        return s

    ones = jnp.ones((SUM, OWN), BF16)

    def attend(work):
        scores = [[tile(zz, kb, bq, masked) for zz, kb, masked in keys] for bq, keys in work]
        for (bq, keys), ss in zip(work, scores):
            old = top_s[bq]
            top = old
            for s in ss:
                top = jnp.maximum(top, s.max(axis=0, keepdims=True))
            top_s[bq] = top
            keep = jnp.exp2((old - top) * e)
            total = mix_s[bq] * keep
            for (zz, kb, _), s in zip(keys, ss):
                w = jnp.exp2((s - top) * e).astype(BF16)
                total = total + _dot(jnp.concatenate([kv_v[zz, kb], ones], axis=0), w, 1, 0)
            mix_s[bq] = total

    @jax.named_scope("pair")
    def pair(zz, kp, qp):
        keys = [(zz, 2 * kp, False), (zz, 2 * kp + 1, False)]
        attend([(2 * qp, keys), (2 * qp + 1, keys)])

    @jax.named_scope("diagonal")
    def diagonal(kp):
        attend([(2 * kp, [(z, 2 * kp, True)]), (2 * kp + 1, [(z, 2 * kp, False), (z, 2 * kp + 1, True)])])

    got_a(bX, 1)
    send_a(bX, 1, 10, C)
    got_a(bY, 0)
    send_a(bY, 0, 11, C)
    got_a(2 * pX + oc, 1)
    got_a(2 * pY + oc, 0)
    side_pieces(1)
    even = 1 - (x + y) % 2

    def near(n, _):
        diagonal(p * (n == 0) + pX * (n == 1) + pY * (n == 2))
        low = y * (n == 0) + 2 * x * (n == 1) + even * (n == 2)
        high = (y + 2) * (n == 0) + (2 * x + 1) * (n == 1) + (3 - even) * (n == 2)
        pair(z, low, high)

    lax.fori_loop(0, 3, near, None)

    for half in (0, 1):
        got_a(bD, half)
        send_a(bD, half, 12 + half, C)
    for half in (0, 1):
        got_a(2 * pD + oc, half)
    own_piece(pD)

    @pl.when(hold)
    def _():
        for n in range(4):
            send_kv(*side_half(1, n))

    @pl.when(hold_y)
    def _():
        for n in range(2):
            send_kv(*side_half(1, n))

    diagonal(pD)

    def far(n, _):
        low = (1 - even) * (n == 0) + 2 * (1 - x) * (n == 1) + (1 - y) * (n == 2)
        high = (2 + even) * (n == 0) + (3 - 2 * x) * (n == 1) + (3 - y) * (n == 2)
        pair(z, low, high)

    lax.fori_loop(0, 3, far, None)

    iX, iY, iD = row(pX, z, c), row(pY, z, c), row(pD, z, c)
    for n, (i, dev) in enumerate(((iX, Y), (iY, X))):
        got(wov.at[i], wo_r.at[i], f"wo{n}")
        rows = pl.ds(n * 64, 64)
        send(wov.at[i, rows], wov.at[i, rows], wo_s.at[7 + n], wod_r.at[n], dev)
        send(wov.at[i], wov.at[i], wo_s.at[9 + n], wo_r.at[i], C)

    def wo_rest():
        for n in (0, 1):
            got(wov.at[iD, pl.ds(n * 64, 64)], wod_r.at[n], f"wod{n}")
        send(wov.at[iD], wov.at[iD], wo_s.at[13], wo_r.at[iD], Z)
        send(wov.at[iD], wov.at[iD], wo_s.at[14], wo_r.at[iD], C)
        for n, i in enumerate((row(pX, oz, c), row(pY, oz, c))):
            got(wov.at[i], wo_r.at[i], f"wo_oz{n}")
            send(wov.at[i], wov.at[i], wo_s.at[11 + n], wo_r.at[i], C)

    cols = pl.ds(pl.multiple_of(head * HEAD, HEAD), HEAD)

    def o_copy(b):
        return rc(ov.at[b], og.at[:, cols], o_s.at[b], o_r.at[head], row(b // 2, z, b % 2))

    by_y = 2 * pD + 1

    def o_copy_by_y():
        return rc(ov.at[by_y], orl, o_s.at[by_y], orl_r, Y)

    def finish(b, _):
        with jax.named_scope("finish"):
            mix = mix_s[b]
            ov[b] = (mix[:HEAD] * (1 / mix[HEAD : HEAD + 1])).T.astype(BF16)

        @pl.when((b != mine) & (b != by_y))
        def _():
            o_copy(b).start()

        @pl.when(b == by_y)
        def _():
            o_copy_by_y().start()

    def finish_pieces(first, last):
        lax.fori_loop(2 * first, 2 * last, finish, None)

    first, last = (3 - p) // 3, p // 3
    kp0, kp1 = p - 2 * last, first
    done0, done1 = first, 2 - p // 2 * (3 - p)

    def got_kv(b):
        for half in (0, 1):
            rows = half_rows(half)
            got(kv_k.at[oz, b, rows, :], kv_r.at[b, half, 0], "kv")
            got(kv_v.at[oz, b, :, rows], kv_r.at[b, half, 1], "kv")

    def remote_piece(kp):
        got_kv(2 * kp)
        got_kv(2 * kp + 1)
        lax.fori_loop(kp + 1 - z, 4, lambda qp, _: pair(oz, kp, qp), None)

    def remote_blocks(kp):
        def body(n, _):
            b = 2 * kp + core(n)
            got_kv(b)

            def one(qp, _):
                with jax.named_scope("one"):
                    attend([(2 * qp, [(oz, b, False)]), (2 * qp + 1, [(oz, b, False)])])

            lax.fori_loop(kp + 1 - z, 4, one, None)

        lax.fori_loop(0, 2, body, None)

    finish_pieces(0, oz)
    remote_piece(kp0)
    finish_pieces(oz, done0 + oz)

    def part_copies():
        return (rc(part.at[0], part.at[1], part_s.at[0], part_r.at[0], Z), rc(part_f.at[0], part_f.at[1], part_s.at[1], part_r.at[1], Z))

    @pl.when(z == 0)
    def _():
        for n in (0, 1):
            for half in (0, 1):
                got(qv.at[8 + n, half_rows(half), :], q_r.at[n, half], "q")
        pair(z, 3, 4)
        for n in (0, 1):
            mix = mix_s[8 + n]
            total = mix[HEAD : HEAD + 1]
            part[0, n] = (mix[:HEAD] * (1 / total)).astype(BF16)
            part_f[0, n] = jnp.concatenate([top_s[8 + n], total], axis=0)
        for cp in part_copies():
            cp.start()

    remote_piece(kp1)
    finish_pieces(done0 + oz, done1 + oz)
    wo_rest()
    remote_blocks(3 - kp0 - kp1)
    finish_pieces(done1 + oz, 3)

    @pl.when(z == 1)
    def _():
        got(part.at[1], part_r.at[0], "part")
        got(part_f.at[1], part_r.at[1], "part")
        for n in (0, 1):
            old, came, count = top_s[6 + n], part_f[1, n, 0:1], part_f[1, n, 1:2]
            top = jnp.maximum(old, came)
            keep, add = jnp.exp2((old - top) * e), jnp.exp2((came - top) * e) * count
            mix = mix_s[6 + n]
            more = jnp.concatenate([part[1, n].astype(F32) * add, jnp.broadcast_to(add, (SUM, OWN))], axis=0)
            mix_s[6 + n] = mix * keep + more

    finish_pieces(3, 4)

    with jax.named_scope("relay"):
        got(orl, orl_r)
    from_y = pl.ds(pl.multiple_of((2 * pY + c) * HEAD, HEAD), HEAD)
    send(orl, og.at[:, from_y], orl_s, o_r.at[2 * pY + c], row(pX, z, 1))
    og[:, cols] = ov[mine]
    def y_copy(n):
        cols = pl.ds(pl.multiple_of(n * 512, 512), 512)
        return pltpu.make_async_copy(xv.at[:, cols], y_h.at[:, cols], y_s.at[n])

    for k, q in enumerate(planes):
        if k == 3:
            i = row(pD, oz, c)
            got(wov.at[i], wo_r.at[i], "wo_dz")
            send(wov.at[i], wov.at[i], wo_s.at[15], wo_r.at[i], C)
        for zz in (0, 1):
            got(wov.at[row(q, zz, oc)], wo_r.at[row(q, zz, oc)], "wo_c")
        for cc in (c, oc):
            if k or cc is oc:
                hd = 2 * q + cc
                got(og.at[:, pl.ds(pl.multiple_of(hd * HEAD, HEAD), HEAD)], o_r.at[hd], "og")
        heads = pl.ds(pl.multiple_of(q * 2 * HEAD, 2 * HEAD), 2 * HEAD)

        def out(n, _):
            cols = pl.ds(pl.multiple_of(n * 512, 512), 512)
            with jax.named_scope("out"):
                t = _dot(og[:, heads], wov[pl.ds(4 * q, 4), :, cols].reshape(2 * HEAD, 512), 1, 0)
                for m in range(2):
                    rows = pl.ds(m * HEAD, HEAD)
                    u = t[m * HEAD : (m + 1) * HEAD]
                    if k:
                        u = mix_s[2 * n + m, :HEAD, :] + u
                    if k < 3:
                        mix_s[2 * n + m, :HEAD, :] = u
                    else:
                        xv[rows, cols] = (xv[rows, cols].astype(F32) + u).astype(BF16)

            if k == 3:
                y_copy(n).start()

        lax.fori_loop(0, D // 512, out, None)

    with jax.named_scope("left"):
        for cp in sends:
            cp.wait_send()

    def kv_left(n, _):
        for cp in kv_copies(n // 2, n % 2):
            cp.wait_send()

    lax.fori_loop(0, 12, kv_left, None)

    def o_left(b, _):
        @pl.when(b != mine)
        def _():
            o_copy(b).wait_send()

    lax.fori_loop(0, 8, o_left, None)

    @pl.when(z == 1)
    def _():
        for n in (0, 1):
            for half in (0, 1):
                q_copy(6 + n, half).wait_send()

    @pl.when(z == 0)
    def _():
        for cp in part_copies():
            cp.wait_send()

    for n in range(D // 512):
        y_copy(n).wait()


def tables():
    half = HEAD // 2
    rate = (THETA ** (-np.arange(half, dtype=np.float64) / half))[None]
    fine = np.arange(OWN, dtype=np.float64)[:, None] * rate
    coarse = np.arange(16, dtype=np.float64)[:, None] * OWN * rate
    return (np.stack([np.cos(t), np.sin(t)]).astype(np.float32) for t in (fine, coarse))


def solution(mesh):
    def step(x, gain, wq, wk, wv, wo):
        fine, coarse = tables()
        anywhere = pl.BlockSpec(memory_space=pltpu.HBM)
        dma = pltpu.SemaphoreType.DMA
        return pl.pallas_call(
            kernel,
            out_shape=jax.ShapeDtypeStruct((OWN, D), BF16),
            in_specs=[anywhere] * 8,
            out_specs=anywhere,
            scratch_shapes=[
                pltpu.VMEM((D,), BF16),
                pltpu.VMEM((2, OWN, HEAD // 2), F32),
                pltpu.VMEM((2, 16, HEAD // 2), F32),
                pltpu.VMEM((OWN, D), BF16),
                pltpu.VMEM((8, OWN, D), BF16),
                pltpu.VMEM((3, 128, D), BF16),
                pltpu.VMEM((3, 16, 128, HEAD), BF16),
                pltpu.VMEM((3, 8, 128, HEAD), BF16),
                pltpu.VMEM((16, 128, D), BF16),
                pltpu.VMEM((2, 8, OWN, HEAD), BF16),
                pltpu.VMEM((2, 8, HEAD, OWN), BF16),
                pltpu.VMEM((10, OWN, HEAD), BF16),
                pltpu.VMEM((8, OWN, HEAD), BF16),
                pltpu.VMEM((OWN, D), BF16),
                pltpu.VMEM((10, 1, OWN), F32),
                pltpu.VMEM((10, HEAD + SUM, OWN), F32),
                pltpu.VMEM((2, 2, HEAD, OWN), BF16),
                pltpu.VMEM((2, 2, 2, OWN), F32),
                pltpu.VMEM((OWN, HEAD), BF16),
                dma((14,)), dma((22,)), dma((16,)), dma((8,)), dma((14,)), dma((8, 2)), dma((16,)), dma((16,)),
                dma((8, 2, 2)), dma((8, 2, 2)), dma((8,)), dma((8,)), dma((2, 2)), dma((2, 2)), dma((2,)), dma((2,)),
                dma((2,)), dma(()), dma(()), dma((4,)),
            ],
            compiler_params=pltpu.CompilerParams(collective_id=0, has_side_effects=True, vmem_limit_bytes=67043328),
            name="decoder_attention",
        )(x, gain, wq, wk, wv, wo, jnp.asarray(fine), jnp.asarray(coarse))

    tokens, whole = P(("dp", "sp"), None), P("sp", None)
    return jax.shard_map(
        step,
        mesh=mesh,
        in_specs=(tokens, P(None), whole, whole, whole, whole),
        out_specs=tokens,
        check_vma=False,
    )
```

```python
import functools

import jax
import jax.numpy as jnp
import numpy as np
from jax import lax
from jax.experimental import pallas as pl
from jax.experimental.pallas import tpu as pltpu
from jax.sharding import PartitionSpec as P

NEG = -1e30
HIDDEN = 2 * NEG
LOG2E = 1.4426950408889634
HEAD = 256
THETA = 10000
D = 2048
OWN = 512
HALF = 256
SUM = 8
F32, BF16 = jnp.float32, jnp.bfloat16
MESH = pl.DeviceIdType.MESH


def _dot(a, b, ca, cb):
    return lax.dot_general(a, b, (((ca,), (cb,)), ((), ())), preferred_element_type=F32)


def kernel(x_h, gain_h, wq_h, wk_h, wv_h, wo_h, fine_h, coarse_h, y_ref,
           gain_ref, fine_ref, coarse_ref, xv, av, wi, wf, ws, wov, kv_k, kv_v, qv, ov, og, top_s, mix_s, part, part_f, orl,
           ld, w_s, wf_r, ws_r, a_s, a_r, wo_s, wo_r, kv_s, kv_r, o_s, o_r, q_s, q_r, part_s, part_r, wod_r, orl_s, orl_r):
    me = lax.axis_index("sp")
    x, y, z, c, p = me // 8, (me // 4) % 2, (me // 2) % 2, me % 2, me // 4
    X, Y, Z, C = me + 8 - 16 * x, me + 4 - 8 * y, me + 2 - 4 * z, me + 1 - 2 * c
    Dg = X + Y - me
    pX, pY, pD = X // 4, Y // 4, Dg // 4
    oc, oz = 1 - c, 1 - z
    head = 2 * p + c
    mine = 2 * p + c
    planes = (p, pX, pY, pD)

    def row(q, zz, cc):
        return 4 * q + 2 * zz + cc

    def rc(src, dst, ssem, rsem, dev):
        return pltpu.make_async_remote_copy(src_ref=src, dst_ref=dst, send_sem=ssem, recv_sem=rsem, device_id={"sp": dev}, device_id_type=MESH)

    def got(ref, sem, name="wait"):
        with jax.named_scope(name):
            pltpu.make_async_copy(ref, ref, sem).wait()

    def local(src, dst, n):
        cp = pltpu.make_async_copy(src, dst, ld.at[n])
        cp.start()
        return cp

    loads_w = [local(w, wi.at[n], n) for n, w in enumerate((wk_h, wv_h, wq_h))]
    here = pl.ds(pl.multiple_of(head * HEAD, HEAD), HEAD)
    other = pl.ds(pl.multiple_of((2 * p + oc) * HEAD, HEAD), HEAD)
    sme = 2 * p + z
    load_x = local(x_h, xv, 3)
    load_gain = local(gain_h, gain_ref, 11)
    load_tables = (local(fine_h, fine_ref, 12), local(coarse_h, coarse_ref, 13))
    load_wo = local(wo_h, wov.at[me], 4)
    loads_own = [local(w.at[:, here], wf.at[n, me], 5 + n) for n, w in enumerate((wk_h, wv_h, wq_h))]
    loads_own += [local(w.at[:, other], ws.at[n, sme], 8 + n) for n, w in enumerate((wk_h, wv_h, wq_h))]

    barrier = pltpu.get_barrier_semaphore()
    partners = (X, Y, Dg, X + C - me, Y + C - me, Dg + C - me, C, Z)
    for dev in partners:
        pl.semaphore_signal(barrier, inc=1, device_id={"sp": dev}, device_id_type=MESH)
    with jax.named_scope("barrier"):
        pl.semaphore_wait(barrier, len(partners))

    sends = []

    def send(src, dst, ssem, rsem, dev):
        cp = rc(src, dst, ssem, rsem, dev)
        cp.start()
        sends.append(cp)

    with jax.named_scope("load"):
        for cp in loads_w:
            cp.wait()
    for n, (dev, q) in enumerate(((X, pX), (Y, pY), (Dg, pD))):
        for m, (hd, dst, rs) in enumerate(((2 * q + c, wf.at[:, me], wf_r.at[me]), (2 * q + oc, ws.at[:, sme], ws_r.at[sme]))):
            cols = pl.ds(pl.multiple_of(hd * HEAD, HEAD), HEAD)
            send(wi.at[:, :, cols], dst, w_s.at[2 * n + m], rs, dev)

    def wf_on(n, q, zz):
        i = row(q, zz, c)
        send(wf.at[:, i], wf.at[:, i], w_s.at[6 + 2 * n], wf_r.at[i], Z)

    def ws_on(n, q, zz, on):
        i, s = row(q, zz, c), 2 * q + zz
        if on:
            send(ws.at[:, s], ws.at[:, s], w_s.at[7 + 2 * n], ws_r.at[s], Z)
        send(ws.at[:, s], wf.at[:, i], w_s.at[14 + n + (0 if on else 4)], wf_r.at[i], C)

    def got_wf(n, q, zz):
        got(wf.at[:, row(q, zz, c)], wf_r.at[row(q, zz, c)], f"wf{n}")

    def got_ws(n, q, zz):
        got(ws.at[:, 2 * q + zz], ws_r.at[2 * q + zz], f"ws{n}")

    for cp in loads_own:
        cp.wait()
    wf_on(0, p, z)
    ws_on(0, p, z, True)

    load_x.wait()
    load_gain.wait()

    @jax.named_scope("norm")
    def norm(n, _):
        rows = pl.ds(pl.multiple_of(n * 128, 128), 128)
        wide = xv[rows, :].astype(F32)
        scale = lax.rsqrt(jnp.mean(wide * wide, -1, keepdims=True) + 1e-6)
        av[mine, rows, :] = (wide * scale * gain_ref[...].reshape(1, D).astype(F32)).astype(BF16)

    lax.fori_loop(0, OWN // 128, norm, None)

    def half_rows(half):
        return pl.ds(half * HALF if isinstance(half, int) else pl.multiple_of(half * HALF, HALF), HALF)

    def send_a(b, half, n, dev):
        rows = half_rows(half)
        send(av.at[b, rows], av.at[b, rows], a_s.at[n], a_r.at[b, half], dev)

    def got_a(b, half):
        got(av.at[b, half_rows(half)], a_r.at[b, half], f"a{half}" if isinstance(half, int) else "a")

    send_a(mine, 0, 0, X)
    send_a(mine, 1, 1, Y)
    send_a(mine, 1, 2, X)
    send_a(mine, 0, 3, Y)
    send_a(mine, 0, 4, C)
    send_a(mine, 1, 5, C)

    for n, q in ((1, pX), (2, pY)):
        got_wf(n, q, z)
        wf_on(n, q, z)
    for n, q in ((1, pX), (2, pY)):
        got_ws(n, q, z)
        ws_on(n, q, z, True)
    got_wf(3, pD, z)
    wf_on(3, pD, z)
    got_ws(3, pD, z)
    ws_on(3, pD, z, True)
    load_wo.wait()
    send(wov.at[me], wov.at[me], wo_s.at[0], wo_r.at[me], Z)

    for n, q in enumerate(planes):
        got_wf(n, q, oz)
        got_ws(n, q, oz)
        ws_on(n, q, oz, False)
    for q in planes:
        for zz in (0, 1):
            got(wf.at[:, row(q, zz, oc)], wf_r.at[row(q, zz, oc)])

    @jax.named_scope("project")
    def project(b, half):
        rows = half_rows(half)
        a = av[b, rows, :]
        i = 4 * (b // 2) + 2 * z + b % 2
        cb, sb = coarse_ref[0, pl.ds(i, 1), :], coarse_ref[1, pl.ds(i, 1), :]
        cf, sf = fine_ref[0, rows, :], fine_ref[1, rows, :]
        cos = cb * cf - sb * sf
        sin = sb * cf + cb * sf

        def turned(t):
            t = t.astype(BF16).astype(F32)
            u, v = t[:, : HEAD // 2], t[:, HEAD // 2 :]
            return jnp.concatenate([u * cos - v * sin, v * cos + u * sin], -1).astype(BF16)

        kv_k[z, b, rows, :] = turned(_dot(a, wf[0].reshape(D, HEAD), 1, 0))
        kv_v[z, b, :, rows] = _dot(a, wf[1].reshape(D, HEAD), 1, 0).astype(BF16).T
        qv[b, rows, :] = turned(_dot(a, wf[2].reshape(D, HEAD), 1, 0))

    def kv_copies(b, half):
        rows = half_rows(half)
        return (rc(kv_k.at[z, b, rows, :], kv_k.at[z, b, rows, :], kv_s.at[b, half, 0], kv_r.at[b, half, 0], Z),
                rc(kv_v.at[z, b, :, rows], kv_v.at[z, b, :, rows], kv_s.at[b, half, 1], kv_r.at[b, half, 1], Z))

    def q_copy(b, half):
        rows = half_rows(half)
        return rc(qv.at[b, rows, :], qv.at[b + 2, rows, :], q_s.at[b - 6, half], q_r.at[b - 6, half], Z)

    def send_kv(b, half):
        for cp in kv_copies(b, half):
            cp.start()

    def on(b, half):
        @pl.when(b < 6)
        def _():
            send_kv(b, half)

        @pl.when((b >= 6) & (z == 1))
        def _():
            q_copy(b, half).start()

    def core(n):
        return c + n * (oc - c)

    def own_piece(q):
        def body(n, _):
            b, half = 2 * q + core(n // 2), n % 2
            project(b, half)
            on(b, half)

        lax.fori_loop(0, 4, body, None)

    def side_half(t, n):
        isy = n % 2 if t == 0 else 1 - n // 2
        return 2 * (pX + isy * (pY - pX)) + core(n // 2 if t == 0 else n % 2), (isy + t) % 2

    hold = (p == 0) & (z == 1)
    hold_y = p == 3

    def side_pieces(t):
        def body(n, _):
            b, half = side_half(t, n)
            project(b, half)
            if t == 0:
                on(b, half)
            else:
                @pl.when(jnp.logical_not(hold | (hold_y & (n < 2))))
                def _():
                    on(b, half)

        lax.fori_loop(0, 4, body, None)

    for cp in load_tables:
        cp.wait()
    for half in (0, 1):
        got_a(2 * p + oc, half)
    own_piece(p)

    bX, bY, bD = 2 * pX + c, 2 * pY + c, 2 * pD + c
    got_a(bX, 0)
    send_a(bX, 0, 6, Y)
    send_a(bX, 0, 7, C)
    got_a(bY, 1)
    send_a(bY, 1, 8, X)
    send_a(bY, 1, 9, C)
    got_a(2 * pX + oc, 0)
    got_a(2 * pY + oc, 1)
    side_pieces(0)

    iz = row(p, oz, c)
    got(wov.at[iz], wo_r.at[iz], "wo_z")
    for n, (i, dev) in enumerate(((me, X), (me, Y), (iz, X), (iz, Y), (me, C), (iz, C))):
        send(wov.at[i], wov.at[i], wo_s.at[1 + n], wo_r.at[i], dev)

    e = HEAD**-0.5 * LOG2E
    top_s[...] = jnp.full(top_s.shape, NEG, F32)
    mix_s[...] = jnp.zeros(mix_s.shape, F32)

    def tile(zz, kb, bq, masked):
        s = _dot(kv_k[zz, kb], qv[bq], 1, 1)
        if masked:
            ok = lax.broadcasted_iota(jnp.int32, s.shape, 1) >= lax.broadcasted_iota(jnp.int32, s.shape, 0)
            s = jnp.where(ok, s, HIDDEN)
        return s

    ones = jnp.ones((SUM, OWN), BF16)

    def attend(work):
        scores = [[tile(zz, kb, bq, masked) for zz, kb, masked in keys] for bq, keys in work]
        for (bq, keys), ss in zip(work, scores):
            old = top_s[bq]
            top = old
            for s in ss:
                top = jnp.maximum(top, s.max(axis=0, keepdims=True))
            top_s[bq] = top
            keep = jnp.exp2((old - top) * e)
            total = mix_s[bq] * keep
            for (zz, kb, _), s in zip(keys, ss):
                w = jnp.exp2((s - top) * e).astype(BF16)
                total = total + _dot(jnp.concatenate([kv_v[zz, kb], ones], axis=0), w, 1, 0)
            mix_s[bq] = total

    @jax.named_scope("pair")
    def pair(zz, kp, qp):
        keys = [(zz, 2 * kp, False), (zz, 2 * kp + 1, False)]
        attend([(2 * qp, keys), (2 * qp + 1, keys)])

    @jax.named_scope("diagonal")
    def diagonal(kp):
        attend([(2 * kp, [(z, 2 * kp, True)]), (2 * kp + 1, [(z, 2 * kp, False), (z, 2 * kp + 1, True)])])

    got_a(bX, 1)
    send_a(bX, 1, 10, C)
    got_a(bY, 0)
    send_a(bY, 0, 11, C)
    got_a(2 * pX + oc, 1)
    got_a(2 * pY + oc, 0)
    side_pieces(1)
    even = 1 - (x + y) % 2

    def near(n, _):
        diagonal(p * (n == 0) + pX * (n == 1) + pY * (n == 2))
        low = y * (n == 0) + 2 * x * (n == 1) + even * (n == 2)
        high = (y + 2) * (n == 0) + (2 * x + 1) * (n == 1) + (3 - even) * (n == 2)
        pair(z, low, high)

    lax.fori_loop(0, 3, near, None)

    def part_copies():
        return (rc(part.at[0], part.at[1], part_s.at[0], part_r.at[0], Z), rc(part_f.at[0], part_f.at[1], part_s.at[1], part_r.at[1], Z))

    def send_part():
        for n in (0, 1):
            for half in (0, 1):
                got(qv.at[8 + n, half_rows(half), :], q_r.at[n, half], "q")
        pair(z, 3, 4)
        for n in (0, 1):
            mix = mix_s[8 + n]
            total = mix[HEAD : HEAD + 1]
            part[0, n] = (mix[:HEAD] * (1 / total)).astype(BF16)
            part_f[0, n] = jnp.concatenate([top_s[8 + n], total], axis=0)
        for cp in part_copies():
            cp.start()

    @pl.when((z == 0) & (p == 3))
    def _():
        send_part()

    for half in (0, 1):
        got_a(bD, half)
        send_a(bD, half, 12 + half, C)
    for half in (0, 1):
        got_a(2 * pD + oc, half)
    own_piece(pD)

    @pl.when(hold)
    def _():
        for n in range(4):
            send_kv(*side_half(1, n))

    @pl.when(hold_y)
    def _():
        for n in range(2):
            send_kv(*side_half(1, n))

    diagonal(pD)

    def far(n, _):
        low = (1 - even) * (n == 0) + 2 * (1 - x) * (n == 1) + (1 - y) * (n == 2)
        high = (2 + even) * (n == 0) + (3 - 2 * x) * (n == 1) + (3 - y) * (n == 2)
        pair(z, low, high)

    lax.fori_loop(0, 3, far, None)

    iX, iY, iD = row(pX, z, c), row(pY, z, c), row(pD, z, c)
    for n, (i, dev) in enumerate(((iX, Y), (iY, X))):
        got(wov.at[i], wo_r.at[i], f"wo{n}")
        rows = pl.ds(n * 64, 64)
        send(wov.at[i, rows], wov.at[i, rows], wo_s.at[7 + n], wod_r.at[n], dev)
        send(wov.at[i], wov.at[i], wo_s.at[9 + n], wo_r.at[i], C)

    def wo_rest():
        for n in (0, 1):
            got(wov.at[iD, pl.ds(n * 64, 64)], wod_r.at[n], f"wod{n}")
        send(wov.at[iD], wov.at[iD], wo_s.at[13], wo_r.at[iD], Z)
        send(wov.at[iD], wov.at[iD], wo_s.at[14], wo_r.at[iD], C)
        for n, i in enumerate((row(pX, oz, c), row(pY, oz, c))):
            got(wov.at[i], wo_r.at[i], f"wo_oz{n}")
            send(wov.at[i], wov.at[i], wo_s.at[11 + n], wo_r.at[i], C)

    cols = pl.ds(pl.multiple_of(head * HEAD, HEAD), HEAD)

    def o_copy(b):
        return rc(ov.at[b], og.at[:, cols], o_s.at[b], o_r.at[head], row(b // 2, z, b % 2))

    by_y = 2 * pD + 1

    def o_copy_by_y():
        return rc(ov.at[by_y], orl, o_s.at[by_y], orl_r, Y)

    def finish(b, _):
        with jax.named_scope("finish"):
            mix = mix_s[b]
            ov[b] = (mix[:HEAD] * (1 / mix[HEAD : HEAD + 1])).T.astype(BF16)

        @pl.when((b != mine) & (b != by_y))
        def _():
            o_copy(b).start()

        @pl.when(b == by_y)
        def _():
            o_copy_by_y().start()

    def finish_pieces(first, last):
        lax.fori_loop(2 * first, 2 * last, finish, None)

    first, last = (3 - p) // 3, p // 3
    kp0, kp1 = p - 2 * last, first
    done0, done1 = first, 2 - p // 2 * (3 - p)

    def got_kv(b):
        for half in (0, 1):
            rows = half_rows(half)
            got(kv_k.at[oz, b, rows, :], kv_r.at[b, half, 0], "kv")
            got(kv_v.at[oz, b, :, rows], kv_r.at[b, half, 1], "kv")

    def remote_piece(kp):
        got_kv(2 * kp)
        got_kv(2 * kp + 1)
        lax.fori_loop(kp + 1 - z, 4, lambda qp, _: pair(oz, kp, qp), None)

    def remote_blocks(kp):
        def body(n, _):
            b = 2 * kp + core(n)
            got_kv(b)

            def one(qp, _):
                with jax.named_scope("one"):
                    attend([(2 * qp, [(oz, b, False)]), (2 * qp + 1, [(oz, b, False)])])

            lax.fori_loop(kp + 1 - z, 4, one, None)

        lax.fori_loop(0, 2, body, None)

    finish_pieces(0, oz)
    remote_piece(kp0)
    finish_pieces(oz, done0 + oz)

    @pl.when((z == 0) & (p < 3))
    def _():
        send_part()

    remote_piece(kp1)
    finish_pieces(done0 + oz, done1 + oz)
    wo_rest()
    remote_blocks(3 - kp0 - kp1)
    finish_pieces(done1 + oz, 3)

    @pl.when(z == 1)
    def _():
        got(part.at[1], part_r.at[0], "part")
        got(part_f.at[1], part_r.at[1], "part")
        for n in (0, 1):
            old, came, count = top_s[6 + n], part_f[1, n, 0:1], part_f[1, n, 1:2]
            top = jnp.maximum(old, came)
            keep, add = jnp.exp2((old - top) * e), jnp.exp2((came - top) * e) * count
            mix = mix_s[6 + n]
            more = jnp.concatenate([part[1, n].astype(F32) * add, jnp.broadcast_to(add, (SUM, OWN))], axis=0)
            mix_s[6 + n] = mix * keep + more

    finish_pieces(3, 4)

    og[:, cols] = ov[mine]
    for k, q in enumerate(planes):
        if k == 1:
            got(orl, orl_r, "relay")
            from_y = pl.ds(pl.multiple_of((2 * pY + c) * HEAD, HEAD), HEAD)
            send(orl, og.at[:, from_y], orl_s, o_r.at[2 * pY + c], row(pX, z, 1))
        if k == 2:
            i = row(pD, oz, c)
            got(wov.at[i], wo_r.at[i], "wo_dz")
            send(wov.at[i], wov.at[i], wo_s.at[15], wo_r.at[i], C)
        for zz in (0, 1):
            got(wov.at[row(q, zz, oc)], wo_r.at[row(q, zz, oc)], "wo_c")
        for cc in (c, oc):
            if k or cc is oc:
                hd = 2 * q + cc
                got(og.at[:, pl.ds(pl.multiple_of(hd * HEAD, HEAD), HEAD)], o_r.at[hd], "og")
        heads = pl.ds(pl.multiple_of(q * 2 * HEAD, 2 * HEAD), 2 * HEAD)

        def out(n, _):
            cols = pl.ds(pl.multiple_of(n * 512, 512), 512)
            with jax.named_scope("out"):
                t = _dot(og[:, heads], wov[pl.ds(4 * q, 4), :, cols].reshape(2 * HEAD, 512), 1, 0)
                for m in range(2):
                    rows = pl.ds(m * HEAD, HEAD)
                    u = t[m * HEAD : (m + 1) * HEAD]
                    if k:
                        u = mix_s[2 * n + m, :HEAD, :] + u
                    if k < 3:
                        mix_s[2 * n + m, :HEAD, :] = u
                    else:
                        y_ref[rows, cols] = (xv[rows, cols].astype(F32) + u).astype(BF16)

        lax.fori_loop(0, D // 512, out, None)

    with jax.named_scope("left"):
        for cp in sends:
            cp.wait_send()

    def kv_left(n, _):
        for cp in kv_copies(n // 2, n % 2):
            cp.wait_send()

    lax.fori_loop(0, 12, kv_left, None)

    def o_left(b, _):
        @pl.when(b != mine)
        def _():
            o_copy(b).wait_send()

    lax.fori_loop(0, 8, o_left, None)

    @pl.when(z == 1)
    def _():
        for n in (0, 1):
            for half in (0, 1):
                q_copy(6 + n, half).wait_send()

    @pl.when(z == 0)
    def _():
        for cp in part_copies():
            cp.wait_send()


def tables():
    half = HEAD // 2
    rate = (THETA ** (-np.arange(half, dtype=np.float64) / half))[None]
    fine = np.arange(OWN, dtype=np.float64)[:, None] * rate
    coarse = np.arange(16, dtype=np.float64)[:, None] * OWN * rate
    return (np.stack([np.cos(t), np.sin(t)]).astype(np.float32) for t in (fine, coarse))


def solution(mesh):
    def step(x, gain, wq, wk, wv, wo):
        fine, coarse = tables()
        anywhere = pl.BlockSpec(memory_space=pltpu.HBM)
        dma = pltpu.SemaphoreType.DMA
        return pl.pallas_call(
            kernel,
            out_shape=pltpu.VMEM((OWN, D), BF16),
            in_specs=[anywhere] * 8,
            out_specs=pl.BlockSpec(memory_space=pltpu.VMEM),
            scratch_shapes=[
                pltpu.VMEM((D,), BF16),
                pltpu.VMEM((2, OWN, HEAD // 2), F32),
                pltpu.VMEM((2, 16, HEAD // 2), F32),
                pltpu.VMEM((OWN, D), BF16),
                pltpu.VMEM((8, OWN, D), BF16),
                pltpu.VMEM((3, 128, D), BF16),
                pltpu.VMEM((3, 16, 128, HEAD), BF16),
                pltpu.VMEM((3, 8, 128, HEAD), BF16),
                pltpu.VMEM((16, 128, D), BF16),
                pltpu.VMEM((2, 8, OWN, HEAD), BF16),
                pltpu.VMEM((2, 8, HEAD, OWN), BF16),
                pltpu.VMEM((10, OWN, HEAD), BF16),
                pltpu.VMEM((8, OWN, HEAD), BF16),
                pltpu.VMEM((OWN, D), BF16),
                pltpu.VMEM((10, 1, OWN), F32),
                pltpu.VMEM((10, HEAD + SUM, OWN), F32),
                pltpu.VMEM((2, 2, HEAD, OWN), BF16),
                pltpu.VMEM((2, 2, 2, OWN), F32),
                pltpu.VMEM((OWN, HEAD), BF16),
                dma((14,)), dma((22,)), dma((16,)), dma((8,)), dma((14,)), dma((8, 2)), dma((16,)), dma((16,)),
                dma((8, 2, 2)), dma((8, 2, 2)), dma((8,)), dma((8,)), dma((2, 2)), dma((2, 2)), dma((2,)), dma((2,)),
                dma((2,)), dma(()), dma(()),
            ],
            compiler_params=pltpu.CompilerParams(collective_id=0, has_side_effects=True, vmem_limit_bytes=61 * 2**20),
            name="decoder_attention",
        )(x, gain, wq, wk, wv, wo, jnp.asarray(fine), jnp.asarray(coarse))

    tokens, whole = P(("dp", "sp"), None), P("sp", None)
    return jax.shard_map(
        step,
        mesh=mesh,
        in_specs=(tokens, P(None), whole, whole, whole, whole),
        out_specs=tokens,
        check_vma=False,
    )
```

```python
import functools

import jax
import jax.numpy as jnp
import numpy as np
from jax import lax
from jax.experimental import pallas as pl
from jax.experimental.pallas import tpu as pltpu
from jax.sharding import PartitionSpec as P

NEG = -1e30
HIDDEN = 2 * NEG
LOG2E = 1.4426950408889634
HEAD = 256
THETA = 10000
D = 2048
OWN = 512
HALF = 256
SUM = 8
F32, BF16 = jnp.float32, jnp.bfloat16
MESH = pl.DeviceIdType.MESH


def _dot(a, b, ca, cb):
    return lax.dot_general(a, b, (((ca,), (cb,)), ((), ())), preferred_element_type=F32)


def kernel(x_h, gain_h, wq_h, wk_h, wv_h, wo_h, fine_h, coarse_h, y_ref,
           gain_ref, fine_ref, coarse_ref, xv, av, wi, wf, ws, wov, kv_k, kv_v, qv, ov, og, top_s, mix_s, part, part_f, orl,
           ld, w_s, wf_r, wfc_r, ws_r, a_s, a_r, ac_r, wo_s, wo_r, wod_r, woc_r, kv_s, kv_r, o_s, o_r, orl_r, q_s, q_r, part_s, part_r):
    me = lax.axis_index("sp")
    x, y, z, c, p = me // 8, (me // 4) % 2, (me // 2) % 2, me % 2, me // 4
    X, Y, Z, C = me + 8 - 16 * x, me + 4 - 8 * y, me + 2 - 4 * z, me + 1 - 2 * c
    Dg = X + Y - me
    pX, pY, pD = X // 4, Y // 4, Dg // 4
    oc, oz = 1 - c, 1 - z
    head = 2 * p + c
    mine = 2 * p + c
    planes = (p, pX, pY, pD)

    def row(q, zz, cc):
        return 4 * q + 2 * zz + cc

    def rc(src, dst, ssem, rsem, dev):
        return pltpu.make_async_remote_copy(src_ref=src, dst_ref=dst, send_sem=ssem, recv_sem=rsem, device_id={"sp": dev}, device_id_type=MESH)

    def got(ref, sem, name="wait"):
        with jax.named_scope(name):
            pltpu.make_async_copy(ref, ref, sem).wait()

    def local(src, dst, n):
        cp = pltpu.make_async_copy(src, dst, ld.at[n])
        cp.start()
        return cp

    loads = (wk_h, wv_h, wq_h)
    for n, w in enumerate(loads):
        local(w, wi.at[n], 0)
    here = pl.ds(pl.multiple_of(head * HEAD, HEAD), HEAD)
    other = pl.ds(pl.multiple_of((2 * p + oc) * HEAD, HEAD), HEAD)
    sme = 2 * p + z
    load_x = local(x_h, xv, 1)
    load_gain = local(gain_h, gain_ref, 2)
    load_tables = (local(fine_h, fine_ref, 3), local(coarse_h, coarse_ref, 4))
    load_wo = local(wo_h, wov.at[me], 5)
    for n, w in enumerate(loads):
        local(w.at[:, here], wf.at[n, me], 6)
        local(w.at[:, other], ws.at[n, sme], 7)

    barrier = pltpu.get_barrier_semaphore()
    partners = (X, Y, Dg, X + C - me, Y + C - me, Dg + C - me, C, Z)
    for dev in partners:
        pl.semaphore_signal(barrier, inc=1, device_id={"sp": dev}, device_id_type=MESH)
    with jax.named_scope("barrier"):
        pl.semaphore_wait(barrier, len(partners))

    def send(src, dst, ssem, rsem, dev):
        rc(src, dst, ssem, rsem, dev).start()

    got(wi, ld.at[0], "load")
    for dev, q in ((X, pX), (Y, pY), (Dg, pD)):
        for hd, dst, rs in ((2 * q + c, wf.at[:, me], wf_r.at[sme]), (2 * q + oc, ws.at[:, sme], ws_r.at[sme])):
            cols = pl.ds(pl.multiple_of(hd * HEAD, HEAD), HEAD)
            send(wi.at[:, :, cols], dst, w_s.at[1], rs, dev)

    def wf_on(q, zz):
        i = row(q, zz, c)
        send(wf.at[:, i], wf.at[:, i], w_s.at[0], wf_r.at[2 * q + zz], Z)

    def ws_on(q, zz, on):
        i, s = row(q, zz, c), 2 * q + zz
        if on:
            send(ws.at[:, s], ws.at[:, s], w_s.at[0], ws_r.at[s], Z)
        send(ws.at[:, s], wf.at[:, i], w_s.at[0], wfc_r, C)

    def got_wf(n, q, zz):
        got(wf.at[:, row(q, zz, c)], wf_r.at[2 * q + zz], f"wf{n}")

    def got_ws(n, q, zz):
        got(ws.at[:, 2 * q + zz], ws_r.at[2 * q + zz], f"ws{n}")

    got(wf.at[:, me], ld.at[6])
    got(ws.at[:, sme], ld.at[7])
    wf_on(p, z)
    ws_on(p, z, True)

    load_x.wait()
    load_gain.wait()

    @jax.named_scope("norm")
    def norm(n, _):
        rows = pl.ds(pl.multiple_of(n * 128, 128), 128)
        wide = xv[rows, :].astype(F32)
        scale = lax.rsqrt(jnp.mean(wide * wide, -1, keepdims=True) + 1e-6)
        av[mine, rows, :] = (wide * scale * gain_ref[...].reshape(1, D).astype(F32)).astype(BF16)

    lax.fori_loop(0, OWN // 128, norm, None)

    def half_rows(half):
        return pl.ds(half * HALF if isinstance(half, int) else pl.multiple_of(half * HALF, HALF), HALF)

    def send_a(b, half, place, dev):
        rows = half_rows(half)
        send(av.at[b, rows], av.at[b, rows], a_s, a_r.at[place, half], dev)

    def give_a(b, half, n):
        rows = half_rows(half)
        send(av.at[b, rows], av.at[b, rows], a_s, ac_r.at[n], C)

    def got_a(b, half, place):
        got(av.at[b, half_rows(half)], a_r.at[place, half], f"a{half}")

    def got_given(n):
        got(av.at[0], ac_r.at[n], "given")

    send_a(mine, 0, 1, X)
    send_a(mine, 1, 2, Y)
    send_a(mine, 1, 1, X)
    send_a(mine, 0, 2, Y)
    give_a(mine, 0, 0)
    give_a(mine, 1, 0)

    for n, q in ((1, pX), (2, pY)):
        got_wf(n, q, z)
        wf_on(q, z)
    for n, q in ((1, pX), (2, pY)):
        got_ws(n, q, z)
        ws_on(q, z, True)
    got_wf(3, pD, z)
    wf_on(pD, z)
    got_ws(3, pD, z)
    ws_on(pD, z, True)
    load_wo.wait()
    send(wov.at[me], wov.at[me], wo_s, wo_r.at[sme], Z)

    for n, q in enumerate(planes):
        got_wf(n, q, oz)
        got_ws(n, q, oz)
        ws_on(q, oz, False)
    got(wf.at[:, pl.ds(0, 8)], wfc_r, "wfc")

    @jax.named_scope("project")
    def project(b, half):
        rows = half_rows(half)
        a = av[b, rows, :]
        i = 4 * (b // 2) + 2 * z + b % 2
        cb, sb = coarse_ref[0, pl.ds(i, 1), :], coarse_ref[1, pl.ds(i, 1), :]
        cf, sf = fine_ref[0, rows, :], fine_ref[1, rows, :]
        cos = cb * cf - sb * sf
        sin = sb * cf + cb * sf

        def turned(t):
            t = t.astype(BF16).astype(F32)
            u, v = t[:, : HEAD // 2], t[:, HEAD // 2 :]
            return jnp.concatenate([u * cos - v * sin, v * cos + u * sin], -1).astype(BF16)

        kv_k[z, b, rows, :] = turned(_dot(a, wf[0].reshape(D, HEAD), 1, 0))
        kv_v[z, b, :, rows] = _dot(a, wf[1].reshape(D, HEAD), 1, 0).astype(BF16).T
        qv[b, rows, :] = turned(_dot(a, wf[2].reshape(D, HEAD), 1, 0))

    def kv_copies(b, half):
        rows = half_rows(half)
        return (rc(kv_k.at[z, b, rows, :], kv_k.at[z, b, rows, :], kv_s, kv_r.at[b, half], Z),
                rc(kv_v.at[z, b, :, rows], kv_v.at[z, b, :, rows], kv_s, kv_r.at[b, half], Z))

    def q_copy(b, half):
        rows = half_rows(half)
        return rc(qv.at[b, rows, :], qv.at[b + 2, rows, :], q_s, q_r, Z)

    def send_kv(b, half):
        for cp in kv_copies(b, half):
            cp.start()

    def on(b, half):
        @pl.when(b < 6)
        def _():
            send_kv(b, half)

        @pl.when((b >= 6) & (z == 1))
        def _():
            q_copy(b, half).start()

    def core(n):
        return c + n * (oc - c)

    def own_piece(q):
        def body(n, _):
            b, half = 2 * q + core(n // 2), n % 2
            project(b, half)
            on(b, half)

        lax.fori_loop(0, 4, body, None)

    def side_half(t, n):
        isy = n % 2 if t == 0 else 1 - n // 2
        return 2 * (pX + isy * (pY - pX)) + core(n // 2 if t == 0 else n % 2), (isy + t) % 2

    hold = (p == 0) & (z == 1)
    hold_y = p == 3

    def side_pieces(t):
        def body(n, _):
            b, half = side_half(t, n)
            project(b, half)
            if t == 0:
                on(b, half)
            else:
                @pl.when(jnp.logical_not(hold | (hold_y & (n < 2))))
                def _():
                    on(b, half)

        lax.fori_loop(0, 4, body, None)

    for cp in load_tables:
        cp.wait()
    got_given(0)
    own_piece(p)

    bX, bY, bD = 2 * pX + c, 2 * pY + c, 2 * pD + c
    got_a(bX, 0, 1)
    send_a(bX, 0, 3, Y)
    give_a(bX, 0, 1)
    got_a(bY, 1, 2)
    send_a(bY, 1, 3, X)
    give_a(bY, 1, 1)
    got_given(1)
    side_pieces(0)

    iz = row(p, oz, c)

    def give_wo(i, place):
        send(wov.at[i], wov.at[i], wo_s, woc_r.at[place], C)

    got(wov.at[iz], wo_r.at[2 * p + oz], "wo_z")
    for i, zz in ((me, z), (iz, oz)):
        for dev in (X, Y):
            send(wov.at[i], wov.at[i], wo_s, wo_r.at[2 * p + zz], dev)
        give_wo(i, 0)

    e = HEAD**-0.5 * LOG2E
    top_s[...] = jnp.full(top_s.shape, NEG, F32)
    mix_s[...] = jnp.zeros(mix_s.shape, F32)

    def tile(zz, kb, bq, masked, rows):
        s = _dot(kv_k[zz, kb, rows, :], qv[bq], 1, 1)
        if masked:
            ok = lax.broadcasted_iota(jnp.int32, s.shape, 1) >= lax.broadcasted_iota(jnp.int32, s.shape, 0)
            s = jnp.where(ok, s, HIDDEN)
        return s

    every = pl.ds(0, OWN)

    def attend(work, rows=every):
        scores = [[tile(zz, kb, bq, masked, rows) for zz, kb, masked in keys] for bq, keys in work]
        for (bq, keys), ss in zip(work, scores):
            old = top_s[bq]
            top = old
            for s in ss:
                top = jnp.maximum(top, s.max(axis=0, keepdims=True))
            top_s[bq] = top
            keep = jnp.exp2((old - top) * e)
            total = mix_s[bq] * keep
            for (zz, kb, _), s in zip(keys, ss):
                w = jnp.exp2((s - top) * e).astype(BF16)
                total = total + _dot(jnp.concatenate([kv_v[zz, kb, :, rows], jnp.ones((SUM, rows.size), BF16)], axis=0), w, 1, 0)
            mix_s[bq] = total

    @jax.named_scope("pair")
    def pair(zz, kp, qp):
        keys = [(zz, 2 * kp, False), (zz, 2 * kp + 1, False)]
        attend([(2 * qp, keys), (2 * qp + 1, keys)])

    @jax.named_scope("diagonal")
    def diagonal(kp):
        attend([(2 * kp, [(z, 2 * kp, True)]), (2 * kp + 1, [(z, 2 * kp, False), (z, 2 * kp + 1, True)])])

    got_a(bX, 1, 1)
    give_a(bX, 1, 2)
    got_a(bY, 0, 2)
    give_a(bY, 0, 2)
    got_given(2)
    side_pieces(1)
    even = 1 - (x + y) % 2

    def near(n, _):
        diagonal(p * (n == 0) + pX * (n == 1) + pY * (n == 2))
        low = y * (n == 0) + 2 * x * (n == 1) + even * (n == 2)
        high = (y + 2) * (n == 0) + (2 * x + 1) * (n == 1) + (3 - even) * (n == 2)
        pair(z, low, high)

    lax.fori_loop(0, 3, near, None)

    def part_copies():
        return (rc(part.at[0], part.at[1], part_s.at[0], part_r.at[0], Z), rc(part_f.at[0], part_f.at[1], part_s.at[1], part_r.at[1], Z))

    def send_part():
        got(qv.at[pl.ds(8, 2)], q_r, "q")
        pair(z, 3, 4)
        for n in (0, 1):
            mix = mix_s[8 + n]
            total = mix[HEAD : HEAD + 1]
            part[0, n] = (mix[:HEAD] * (1 / total)).astype(BF16)
            part_f[0, n] = jnp.concatenate([top_s[8 + n], total], axis=0)
        for cp in part_copies():
            cp.start()

    @pl.when((z == 0) & (p == 3))
    def _():
        send_part()

    for half in (0, 1):
        got_a(bD, half, 3)
        give_a(bD, half, 3)
    got_given(3)
    own_piece(pD)

    @pl.when(hold)
    def _():
        for n in range(4):
            send_kv(*side_half(1, n))

    @pl.when(hold_y)
    def _():
        for n in range(2):
            send_kv(*side_half(1, n))

    diagonal(pD)

    def far(n, _):
        low = (1 - even) * (n == 0) + 2 * (1 - x) * (n == 1) + (1 - y) * (n == 2)
        high = (2 + even) * (n == 0) + (3 - 2 * x) * (n == 1) + (3 - y) * (n == 2)
        pair(z, low, high)

    lax.fori_loop(0, 3, far, None)

    iX, iY, iD = row(pX, z, c), row(pY, z, c), row(pD, z, c)
    for n, (i, q, dev) in enumerate(((iX, pX, Y), (iY, pY, X))):
        got(wov.at[i], wo_r.at[2 * q + z], f"wo{n}")
        rows = pl.ds(n * 64, 64)
        send(wov.at[i, rows], wov.at[i, rows], wo_s, wod_r.at[n], dev)
        give_wo(i, 1 + n)

    def wo_rest():
        for n in (0, 1):
            got(wov.at[iD, pl.ds(n * 64, 64)], wod_r.at[n], f"wod{n}")
        send(wov.at[iD], wov.at[iD], wo_s, wo_r.at[2 * pD + z], Z)
        give_wo(iD, 3)
        for n, q in enumerate((pX, pY)):
            i = row(q, oz, c)
            got(wov.at[i], wo_r.at[2 * q + oz], f"wo_oz{n}")
            give_wo(i, 1 + n)

    cols = pl.ds(pl.multiple_of(head * HEAD, HEAD), HEAD)

    def o_copy(b):
        place = 2 * ((b // 2 % 2 + y) % 2) + (b // 4 + x) % 2
        return rc(ov.at[b], og.at[:, cols], o_s, o_r.at[place], row(b // 2, z, b % 2))

    by_y = 2 * pD + 1

    def o_copy_by_y():
        return rc(ov.at[by_y], orl, o_s, orl_r, Y)

    def finish(b, _):
        with jax.named_scope("finish"):
            mix = mix_s[b]
            ov[b] = (mix[:HEAD] * (1 / mix[HEAD : HEAD + 1])).T.astype(BF16)

        @pl.when((b != mine) & (b != by_y))
        def _():
            o_copy(b).start()

        @pl.when(b == by_y)
        def _():
            o_copy_by_y().start()

    def finish_pieces(first, last):
        lax.fori_loop(2 * first, 2 * last, finish, None)

    first, last = (3 - p) // 3, p // 3
    kp0, kp1 = p - 2 * last, first
    done0, done1 = first, 2 - p // 2 * (3 - p)

    def got_kv(b, half):
        got(kv_k.at[oz, b], kv_r.at[b, half], "kv")

    def remote_piece(kp):
        for n in (0, 1):
            for half in (0, 1):
                got_kv(2 * kp + n, half)
        lax.fori_loop(kp + 1 - z, 4, lambda qp, _: pair(oz, kp, qp), None)

    def last_piece(kp):
        block = 2 * kp + core(0)
        got_kv(block, 0)
        got_kv(block, 1)

        def first(n, _):
            with jax.named_scope("one"):
                attend([(2 * (3 - n) + m, [(oz, block, False)]) for m in (0, 1)])

        lax.fori_loop(0, 3 - kp + z, first, None)
        block2 = 2 * kp + core(1)
        for half in (0, 1):
            got_kv(block2, half)

            def second(n, _):
                with jax.named_scope("half"):
                    attend([(2 * (3 - n) + m, [(oz, block2, False)]) for m in (0, 1)], half_rows(half))
                if half:
                    @pl.when((n > 0) | (z == 0))
                    def _():
                        finish_pieces(3 - n, 4 - n)

            lax.fori_loop(0, 3 - kp + z, second, None)

    finish_pieces(0, oz)
    remote_piece(kp0)
    finish_pieces(oz, done0 + oz)

    @pl.when((z == 0) & (p < 3))
    def _():
        send_part()

    remote_piece(kp1)
    finish_pieces(done0 + oz, done1 + oz)
    wo_rest()
    last_piece(3 - kp0 - kp1)

    @pl.when(z == 1)
    def _():
        got(part.at[1], part_r.at[0], "part")
        got(part_f.at[1], part_r.at[1], "part")
        for n in (0, 1):
            old, came, count = top_s[6 + n], part_f[1, n, 0:1], part_f[1, n, 1:2]
            top = jnp.maximum(old, came)
            keep, add = jnp.exp2((old - top) * e), jnp.exp2((came - top) * e) * count
            mix = mix_s[6 + n]
            more = jnp.concatenate([part[1, n].astype(F32) * add, jnp.broadcast_to(add, (SUM, OWN))], axis=0)
            mix_s[6 + n] = mix * keep + more

        finish_pieces(3, 4)

    og[:, cols] = ov[mine]
    for k, q in enumerate(planes):
        heads = pl.ds(pl.multiple_of(q * 2 * HEAD, 2 * HEAD), 2 * HEAD)
        if k == 1:
            got(orl, orl_r, "relay")
            from_y = pl.ds(pl.multiple_of((2 * pY + c) * HEAD, HEAD), HEAD)
            send(orl, og.at[:, from_y], o_s, o_r.at[3], row(pX, z, 1))
            i = row(pD, oz, c)
            got(wov.at[i], wo_r.at[2 * pD + oz], "wo_dz")
            give_wo(i, 3)
        got(wov.at[pl.ds(0, 2)], woc_r.at[k], "wo_c")
        got(og.at[:, heads] if k else orl, o_r.at[k], "og")

        def out(n, _):
            cols = pl.ds(pl.multiple_of(n * 512, 512), 512)
            with jax.named_scope("out"):
                t = _dot(og[:, heads], wov[pl.ds(4 * q, 4), :, cols].reshape(2 * HEAD, 512), 1, 0)
                for m in range(2):
                    rows = pl.ds(m * HEAD, HEAD)
                    u = t[m * HEAD : (m + 1) * HEAD]
                    if k:
                        u = mix_s[2 * n + m, :HEAD, :] + u
                    if k < 3:
                        mix_s[2 * n + m, :HEAD, :] = u
                    else:
                        y_ref[rows, cols] = (xv[rows, cols].astype(F32) + u).astype(BF16)

        lax.fori_loop(0, D // 512, out, None)

    got(wf, w_s.at[0])
    got(ws.at[:, pl.ds(0, 6)], w_s.at[1])
    got(av.at[pl.ds(0, 7)], a_s)
    got(wov.at[pl.ds(0, 15)], wo_s)
    got(kv_k.at[:, pl.ds(0, 6)], kv_s)
    got(ov, o_s)

    @pl.when(z == 1)
    def _():
        got(qv.at[pl.ds(0, 2)], q_s)

    @pl.when(z == 0)
    def _():
        for cp in part_copies():
            cp.wait_send()


def tables():
    half = HEAD // 2
    rate = (THETA ** (-np.arange(half, dtype=np.float64) / half))[None]
    fine = np.arange(OWN, dtype=np.float64)[:, None] * rate
    coarse = np.arange(16, dtype=np.float64)[:, None] * OWN * rate
    return (np.stack([np.cos(t), np.sin(t)]).astype(np.float32) for t in (fine, coarse))


def solution(mesh):
    def step(x, gain, wq, wk, wv, wo):
        fine, coarse = tables()
        anywhere = pl.BlockSpec(memory_space=pltpu.HBM)
        dma = pltpu.SemaphoreType.DMA
        return pl.pallas_call(
            kernel,
            out_shape=pltpu.VMEM((OWN, D), BF16),
            in_specs=[anywhere] * 8,
            out_specs=pl.BlockSpec(memory_space=pltpu.VMEM),
            scratch_shapes=[
                pltpu.VMEM((D,), BF16),
                pltpu.VMEM((2, OWN, HEAD // 2), F32),
                pltpu.VMEM((2, 16, HEAD // 2), F32),
                pltpu.VMEM((OWN, D), BF16),
                pltpu.VMEM((8, OWN, D), BF16),
                pltpu.VMEM((3, 128, D), BF16),
                pltpu.VMEM((3, 16, 128, HEAD), BF16),
                pltpu.VMEM((3, 8, 128, HEAD), BF16),
                pltpu.VMEM((16, 128, D), BF16),
                pltpu.VMEM((2, 8, OWN, HEAD), BF16),
                pltpu.VMEM((2, 8, HEAD, OWN), BF16),
                pltpu.VMEM((10, OWN, HEAD), BF16),
                pltpu.VMEM((8, OWN, HEAD), BF16),
                pltpu.VMEM((OWN, D), BF16),
                pltpu.VMEM((10, 1, OWN), F32),
                pltpu.VMEM((10, HEAD + SUM, OWN), F32),
                pltpu.VMEM((2, 2, HEAD, OWN), BF16),
                pltpu.VMEM((2, 2, 2, OWN), F32),
                pltpu.VMEM((OWN, HEAD), BF16),
                dma((8,)),
                dma((2,)), dma((8,)), dma(()), dma((8,)),
                dma(()), dma((4, 2)), dma((4,)),
                dma(()), dma((8,)), dma((2,)), dma((4,)),
                dma(()), dma((8, 2)), dma(()), dma((4,)), dma(()),
                dma(()), dma(()), dma((2,)), dma((2,)),
            ],
            compiler_params=pltpu.CompilerParams(collective_id=0, has_side_effects=True, vmem_limit_bytes=61 * 2**20),
            name="decoder_attention",
        )(x, gain, wq, wk, wv, wo, jnp.asarray(fine), jnp.asarray(coarse))

    tokens, whole = P(("dp", "sp"), None), P("sp", None)
    return jax.shard_map(
        step,
        mesh=mesh,
        in_specs=(tokens, P(None), whole, whole, whole, whole),
        out_specs=tokens,
        check_vma=False,
    )
```

```python
import functools

import jax
import jax.numpy as jnp
import numpy as np
from jax import lax
from jax.experimental import pallas as pl
from jax.experimental.pallas import tpu as pltpu
from jax.sharding import PartitionSpec as P

NEG = -1e30
HIDDEN = 2 * NEG
LOG2E = 1.4426950408889634
HEAD = 256
THETA = 10000
D = 2048
OWN = 512
HALF = 256
SUM = 8
F32, BF16 = jnp.float32, jnp.bfloat16
MESH = pl.DeviceIdType.MESH


def _dot(a, b, ca, cb):
    return lax.dot_general(a, b, (((ca,), (cb,)), ((), ())), preferred_element_type=F32)


def kernel(x_h, gain_h, wq_h, wk_h, wv_h, wo_h, fine_h, coarse_h, y_ref,
           gain_ref, fine_ref, coarse_ref, av, wi, wf, ws, wov, kv_k, kv_v, qv, og, top_s, mix_s, part, part_f, orl,
           ld, w_s, wf_r, wfc_r, ws_r, a_s, a_r, ac_r, wo_s, wo_r, wod_r, woc_r, kv_s, kv_r, o_s, o_r, orl_r, q_s, q_r, part_s, part_r):
    me = lax.axis_index("sp")
    x, y, z, c, p = me // 8, (me // 4) % 2, (me // 2) % 2, me % 2, me // 4
    X, Y, Z, C = me + 8 - 16 * x, me + 4 - 8 * y, me + 2 - 4 * z, me + 1 - 2 * c
    Dg = X + Y - me
    pX, pY, pD = X // 4, Y // 4, Dg // 4
    oc, oz = 1 - c, 1 - z
    head = 2 * p + c
    mine = 2 * p + c
    planes = (p, pX, pY, pD)

    def row(q, zz, cc):
        return 4 * q + 2 * zz + cc

    def rc(src, dst, ssem, rsem, dev):
        return pltpu.make_async_remote_copy(src_ref=src, dst_ref=dst, send_sem=ssem, recv_sem=rsem, device_id={"sp": dev}, device_id_type=MESH)

    def got(ref, sem, name="wait"):
        with jax.named_scope(name):
            pltpu.make_async_copy(ref, ref, sem).wait()

    def local(src, dst, n):
        cp = pltpu.make_async_copy(src, dst, ld.at[n])
        cp.start()
        return cp

    loads = (wk_h, wv_h, wq_h)
    for n, w in enumerate(loads):
        local(w, wi.at[n], 0)
    here = pl.ds(pl.multiple_of(head * HEAD, HEAD), HEAD)
    other = pl.ds(pl.multiple_of((2 * p + oc) * HEAD, HEAD), HEAD)
    sme = 2 * p + z
    load_x = local(x_h, y_ref, 1)
    load_gain = local(gain_h, gain_ref, 2)
    load_tables = (local(fine_h, fine_ref, 3), local(coarse_h, coarse_ref, 4))
    load_wo = local(wo_h, wov.at[me], 5)
    for n, w in enumerate(loads):
        local(w.at[:, here], wf.at[n, me], 6)
        local(w.at[:, other], ws.at[n, sme], 7)

    barrier = pltpu.get_barrier_semaphore()
    partners = (X, Y, Dg, X + C - me, Y + C - me, Dg + C - me, C, Z)
    for dev in partners:
        pl.semaphore_signal(barrier, inc=1, device_id={"sp": dev}, device_id_type=MESH)
    with jax.named_scope("barrier"):
        pl.semaphore_wait(barrier, len(partners))

    def send(src, dst, ssem, rsem, dev):
        rc(src, dst, ssem, rsem, dev).start()

    got(wi, ld.at[0], "load")
    for dev, q in ((X, pX), (Y, pY), (Dg, pD)):
        for hd, dst, rs in ((2 * q + c, wf.at[:, me], wf_r.at[sme]), (2 * q + oc, ws.at[:, sme], ws_r.at[sme])):
            cols = pl.ds(pl.multiple_of(hd * HEAD, HEAD), HEAD)
            send(wi.at[:, :, cols], dst, w_s.at[1], rs, dev)

    def wf_on(q, zz):
        i = row(q, zz, c)
        send(wf.at[:, i], wf.at[:, i], w_s.at[0], wf_r.at[2 * q + zz], Z)

    def ws_on(q, zz, on):
        i, s = row(q, zz, c), 2 * q + zz
        if on:
            send(ws.at[:, s], ws.at[:, s], w_s.at[0], ws_r.at[s], Z)
        send(ws.at[:, s], wf.at[:, i], w_s.at[0], wfc_r, C)

    def got_wf(n, q, zz):
        got(wf.at[:, row(q, zz, c)], wf_r.at[2 * q + zz], f"wf{n}")

    def got_ws(n, q, zz):
        got(ws.at[:, 2 * q + zz], ws_r.at[2 * q + zz], f"ws{n}")

    got(wf.at[:, me], ld.at[6])
    got(ws.at[:, sme], ld.at[7])
    wf_on(p, z)
    ws_on(p, z, True)

    load_x.wait()
    load_gain.wait()

    @jax.named_scope("norm")
    def norm(n, _):
        rows = pl.ds(pl.multiple_of(n * 128, 128), 128)
        wide = y_ref[rows, :].astype(F32)
        scale = lax.rsqrt(jnp.mean(wide * wide, -1, keepdims=True) + 1e-6)
        av[mine, rows, :] = (wide * scale * gain_ref[...].reshape(1, D).astype(F32)).astype(BF16)

    lax.fori_loop(0, OWN // 128, norm, None)

    def half_rows(half):
        return pl.ds(half * HALF if isinstance(half, int) else pl.multiple_of(half * HALF, HALF), HALF)

    def send_a(b, half, place, dev):
        rows = half_rows(half)
        send(av.at[b, rows], av.at[b, rows], a_s, a_r.at[place, half], dev)

    def give_a(b, half, n):
        rows = half_rows(half)
        send(av.at[b, rows], av.at[b, rows], a_s, ac_r.at[n], C)

    def got_a(b, half, place):
        got(av.at[b, half_rows(half)], a_r.at[place, half], f"a{half}")

    def got_given(n):
        got(av.at[0], ac_r.at[n], "given")

    send_a(mine, 0, 1, X)
    send_a(mine, 1, 2, Y)
    send_a(mine, 1, 1, X)
    send_a(mine, 0, 2, Y)
    give_a(mine, 0, 0)
    give_a(mine, 1, 0)

    for n, q in ((1, pX), (2, pY)):
        got_wf(n, q, z)
        wf_on(q, z)
    for n, q in ((1, pX), (2, pY)):
        got_ws(n, q, z)
        ws_on(q, z, True)
    got_wf(3, pD, z)
    wf_on(pD, z)
    got_ws(3, pD, z)
    ws_on(pD, z, True)
    load_wo.wait()
    send(wov.at[me], wov.at[me], wo_s, wo_r.at[sme], Z)

    for n, q in enumerate(planes):
        got_wf(n, q, oz)
        got_ws(n, q, oz)
        ws_on(q, oz, False)
    got(wf.at[:, pl.ds(0, 8)], wfc_r, "wfc")

    @jax.named_scope("project")
    def project(b, half):
        rows = half_rows(half)
        a = av[b, rows, :]
        i = 4 * (b // 2) + 2 * z + b % 2
        cb, sb = coarse_ref[0, pl.ds(i, 1), :], coarse_ref[1, pl.ds(i, 1), :]
        cf, sf = fine_ref[0, rows, :], fine_ref[1, rows, :]
        cos = cb * cf - sb * sf
        sin = sb * cf + cb * sf

        def turned(t):
            t = t.astype(BF16).astype(F32)
            u, v = t[:, : HEAD // 2], t[:, HEAD // 2 :]
            return jnp.concatenate([u * cos - v * sin, v * cos + u * sin], -1).astype(BF16)

        kv_k[z, b, rows, :] = turned(_dot(a, wf[0].reshape(D, HEAD), 1, 0))
        kv_v[z, b, :, rows] = _dot(a, wf[1].reshape(D, HEAD), 1, 0).astype(BF16).T
        qv[b, rows, :] = turned(_dot(a, wf[2].reshape(D, HEAD), 1, 0))

    def kv_copies(b, half):
        rows = half_rows(half)
        return (rc(kv_k.at[z, b, rows, :], kv_k.at[z, b, rows, :], kv_s, kv_r.at[b, half], Z),
                rc(kv_v.at[z, b, :, rows], kv_v.at[z, b, :, rows], kv_s, kv_r.at[b, half], Z))

    def q_copy(b, half):
        rows = half_rows(half)
        return rc(qv.at[b, rows, :], qv.at[b + 2, rows, :], q_s, q_r, Z)

    def send_kv(b, half):
        for cp in kv_copies(b, half):
            cp.start()

    def on(b, half):
        @pl.when(b < 6)
        def _():
            send_kv(b, half)

        @pl.when((b >= 6) & (z == 1))
        def _():
            q_copy(b, half).start()

    def core(n):
        return c + n * (oc - c)

    def own_piece(q):
        def body(n, _):
            b, half = 2 * q + core(n // 2), n % 2
            project(b, half)
            on(b, half)

        lax.fori_loop(0, 4, body, None)

    def side_half(t, n):
        isy = n % 2 if t == 0 else 1 - n // 2
        return 2 * (pX + isy * (pY - pX)) + core(n // 2 if t == 0 else n % 2), (isy + t) % 2

    hold = (p == 0) & (z == 1)
    hold_y = p == 3

    def side_pieces(t):
        def body(n, _):
            b, half = side_half(t, n)
            project(b, half)
            if t == 0:
                on(b, half)
            else:
                @pl.when(jnp.logical_not(hold | (hold_y & (n < 2))))
                def _():
                    on(b, half)

        lax.fori_loop(0, 4, body, None)

    for cp in load_tables:
        cp.wait()
    got_given(0)
    own_piece(p)

    bX, bY, bD = 2 * pX + c, 2 * pY + c, 2 * pD + c
    got_a(bX, 0, 1)
    send_a(bX, 0, 3, Y)
    give_a(bX, 0, 1)
    got_a(bY, 1, 2)
    send_a(bY, 1, 3, X)
    give_a(bY, 1, 1)
    got_given(1)
    side_pieces(0)

    iz = row(p, oz, c)

    def give_wo(i, place):
        send(wov.at[i], wov.at[i], wo_s, woc_r.at[place], C)

    got(wov.at[iz], wo_r.at[2 * p + oz], "wo_z")
    for i, zz in ((me, z), (iz, oz)):
        for dev in (X, Y):
            send(wov.at[i], wov.at[i], wo_s, wo_r.at[2 * p + zz], dev)
        give_wo(i, 0)

    e = HEAD**-0.5 * LOG2E
    top_s[...] = jnp.full(top_s.shape, NEG, F32)
    mix_s[...] = jnp.zeros(mix_s.shape, F32)

    def tile(zz, kb, bq, masked, rows):
        s = _dot(kv_k[zz, kb, rows, :], qv[bq], 1, 1)
        if masked:
            ok = lax.broadcasted_iota(jnp.int32, s.shape, 1) >= lax.broadcasted_iota(jnp.int32, s.shape, 0)
            s = jnp.where(ok, s, HIDDEN)
        return s

    every = pl.ds(0, OWN)

    def attend(work, rows=every):
        scores = [[tile(zz, kb, bq, masked, rows) for zz, kb, masked in keys] for bq, keys in work]
        for (bq, keys), ss in zip(work, scores):
            old = top_s[bq]
            top = old
            for s in ss:
                top = jnp.maximum(top, s.max(axis=0, keepdims=True))
            top_s[bq] = top
            keep = jnp.exp2((old - top) * e)
            total = mix_s[bq] * keep
            for (zz, kb, _), s in zip(keys, ss):
                w = jnp.exp2((s - top) * e).astype(BF16)
                total = total + _dot(jnp.concatenate([kv_v[zz, kb, :, rows], jnp.ones((SUM, rows.size), BF16)], axis=0), w, 1, 0)
            mix_s[bq] = total

    @jax.named_scope("pair")
    def pair(zz, kp, qp):
        keys = [(zz, 2 * kp, False), (zz, 2 * kp + 1, False)]
        attend([(2 * qp, keys), (2 * qp + 1, keys)])

    @jax.named_scope("diagonal")
    def diagonal(kp):
        attend([(2 * kp, [(z, 2 * kp, True)]), (2 * kp + 1, [(z, 2 * kp, False), (z, 2 * kp + 1, True)])])

    diagonal(p)

    got_a(bX, 1, 1)
    give_a(bX, 1, 2)
    got_a(bY, 0, 2)
    give_a(bY, 0, 2)
    got_given(2)
    side_pieces(1)
    even = 1 - (x + y) % 2

    def near(n, _):
        @pl.when(n > 0)
        def _():
            diagonal(pX * (n == 1) + pY * (n == 2))

        low = y * (n == 0) + 2 * x * (n == 1) + even * (n == 2)
        high = (y + 2) * (n == 0) + (2 * x + 1) * (n == 1) + (3 - even) * (n == 2)
        pair(z, low, high)

    lax.fori_loop(0, 3, near, None)

    def part_copies():
        return (rc(part.at[0], part.at[1], part_s.at[0], part_r.at[0], Z), rc(part_f.at[0], part_f.at[1], part_s.at[1], part_r.at[1], Z))

    def send_part():
        got(qv.at[pl.ds(8, 2)], q_r, "q")
        pair(z, 3, 4)
        for n in (0, 1):
            mix = mix_s[8 + n]
            total = mix[HEAD : HEAD + 1]
            part[0, n] = (mix[:HEAD] * (1 / total)).astype(BF16)
            part_f[0, n] = jnp.concatenate([top_s[8 + n], total], axis=0)
        for cp in part_copies():
            cp.start()

    @pl.when((z == 0) & (p == 3))
    def _():
        send_part()

    def got_kv(b, half):
        got(kv_k.at[oz, b], kv_r.at[b, half], "kv")

    def got_piece(kp):
        for n in (0, 1):
            for half in (0, 1):
                got_kv(2 * kp + n, half)

    def near_remote(n, _):
        qp = p * (n == 0) + pX * (n == 1) + pY * (n == 2)
        pl.when(qp >= p + oz)(lambda: pair(oz, p, qp))

    @pl.when(p < 3)
    def _():
        got_piece(p)
        lax.fori_loop(0, 3, near_remote, None)

    for half in (0, 1):
        got_a(bD, half, 3)
        give_a(bD, half, 3)
    got_given(3)
    own_piece(pD)

    @pl.when(hold)
    def _():
        for n in range(4):
            send_kv(*side_half(1, n))

    @pl.when(hold_y)
    def _():
        for n in range(2):
            send_kv(*side_half(1, n))

    diagonal(pD)

    def far(n, _):
        low = (1 - even) * (n == 0) + 2 * (1 - x) * (n == 1) + (1 - y) * (n == 2)
        high = (2 + even) * (n == 0) + (3 - 2 * x) * (n == 1) + (3 - y) * (n == 2)
        pair(z, low, high)

    lax.fori_loop(0, 3, far, None)

    iX, iY, iD = row(pX, z, c), row(pY, z, c), row(pD, z, c)
    for n, (i, q, dev) in enumerate(((iX, pX, Y), (iY, pY, X))):
        got(wov.at[i], wo_r.at[2 * q + z], f"wo{n}")
        rows = pl.ds(n * 64, 64)
        send(wov.at[i, rows], wov.at[i, rows], wo_s, wod_r.at[n], dev)
        give_wo(i, 1 + n)

    def wo_rest():
        for n in (0, 1):
            got(wov.at[iD, pl.ds(n * 64, 64)], wod_r.at[n], f"wod{n}")
        send(wov.at[iD], wov.at[iD], wo_s, wo_r.at[2 * pD + z], Z)
        give_wo(iD, 3)
        for n, q in enumerate((pX, pY)):
            i = row(q, oz, c)
            got(wov.at[i], wo_r.at[2 * q + oz], f"wo_oz{n}")
            give_wo(i, 1 + n)

    cols = pl.ds(pl.multiple_of(head * HEAD, HEAD), HEAD)

    def o_copy(b):
        place = 2 * ((b // 2 % 2 + y) % 2) + (b // 4 + x) % 2
        return rc(qv.at[b], og.at[:, cols], o_s, o_r.at[place], row(b // 2, z, b % 2))

    by_y = 2 * pD + 1

    def o_copy_by_y():
        return rc(qv.at[by_y], orl, o_s, orl_r, Y)

    def finish(b, _):
        with jax.named_scope("finish"):
            mix = mix_s[b]
            qv[b] = (mix[:HEAD] * (1 / mix[HEAD : HEAD + 1])).T.astype(BF16)

        @pl.when((b != mine) & (b != by_y))
        def _():
            o_copy(b).start()

        @pl.when(b == by_y)
        def _():
            o_copy_by_y().start()

    def finish_pieces(first, last):
        lax.fori_loop(2 * first, 2 * last, finish, None)

    first, last = (3 - p) // 3, p // 3
    kp0, kp1 = p - 2 * last, first
    done0, done1 = first, 2 - p // 2 * (3 - p)

    def remote_piece(kp, done):
        got_piece(kp)

        def body(qp, _):
            pair(oz, kp, qp)
            pl.when(qp < done)(lambda: finish_pieces(qp, qp + 1))

        lax.fori_loop(kp + oz, 4, body, None)

    def remote_blocks(kp, done):
        for n in (0, 1):
            block = 2 * kp + core(n)
            got_kv(block, 0)
            got_kv(block, 1)

            def body(qp, _):
                with jax.named_scope("one"):
                    attend([(2 * qp + m, [(oz, block, False)]) for m in (0, 1)])
                if n:
                    pl.when(qp < done)(lambda: finish_pieces(qp, qp + 1))

            lax.fori_loop(kp + oz, 4, body, None)

    def last_piece(kp):
        block = 2 * kp + core(0)
        got_kv(block, 0)
        got_kv(block, 1)

        def first(n, _):
            with jax.named_scope("one"):
                attend([(2 * (3 - n) + m, [(oz, block, False)]) for m in (0, 1)])

        lax.fori_loop(0, 3 - kp + z, first, None)
        block2 = 2 * kp + core(1)
        for half in (0, 1):
            got_kv(block2, half)

            def second(n, _):
                with jax.named_scope("half"):
                    attend([(2 * (3 - n) + m, [(oz, block2, False)]) for m in (0, 1)], half_rows(half))
                if half:
                    @pl.when((n > 0) | (z == 0))
                    def _():
                        finish_pieces(3 - n, 4 - n)

            lax.fori_loop(0, 3 - kp + z, second, None)

    finish_pieces(0, oz)

    @pl.when(last == 0)
    def _():
        pl.when(pD >= p + oz)(lambda: pair(oz, p, pD))
        finish_pieces(oz, done0 + oz)

    @pl.when(last == 1)
    def _():
        remote_piece(kp0, 0)

    @pl.when((z == 0) & (p < 3))
    def _():
        send_part()


    @pl.when(last == 0)
    def _():
        remote_piece(kp1, done1 + oz)

    @pl.when(last == 1)
    def _():
        remote_blocks(kp1, done1 + oz)

    wo_rest()
    last_piece(3 - kp0 - kp1)

    @pl.when(z == 1)
    def _():
        got(qv.at[pl.ds(0, 2)], q_s, "q_left")
        got(part.at[1], part_r.at[0], "part")
        got(part_f.at[1], part_r.at[1], "part")
        for n in (0, 1):
            old, came, count = top_s[6 + n], part_f[1, n, 0:1], part_f[1, n, 1:2]
            top = jnp.maximum(old, came)
            keep, add = jnp.exp2((old - top) * e), jnp.exp2((came - top) * e) * count
            mix = mix_s[6 + n]
            more = jnp.concatenate([part[1, n].astype(F32) * add, jnp.broadcast_to(add, (SUM, OWN))], axis=0)
            mix_s[6 + n] = mix * keep + more

        finish_pieces(3, 4)

    og[:, cols] = qv[mine]
    for k, q in enumerate(planes):
        heads = pl.ds(pl.multiple_of(q * 2 * HEAD, 2 * HEAD), 2 * HEAD)
        if k == 1:
            got(orl, orl_r, "relay")
            from_y = pl.ds(pl.multiple_of((2 * pY + c) * HEAD, HEAD), HEAD)
            send(orl, og.at[:, from_y], o_s, o_r.at[3], row(pX, z, 1))
            i = row(pD, oz, c)
            got(wov.at[i], wo_r.at[2 * pD + oz], "wo_dz")
            give_wo(i, 3)
        got(wov.at[pl.ds(0, 2)], woc_r.at[k], "wo_c")
        got(og.at[:, heads] if k else orl, o_r.at[k], "og")

        def out(n, _):
            cols = pl.ds(pl.multiple_of(n * 512, 512), 512)
            with jax.named_scope("out"):
                t = _dot(og[:, heads], wov[pl.ds(4 * q, 4), :, cols].reshape(2 * HEAD, 512), 1, 0)
                for m in range(2):
                    rows = pl.ds(m * HEAD, HEAD)
                    u = t[m * HEAD : (m + 1) * HEAD]
                    if k:
                        u = mix_s[2 * n + m, :HEAD, :] + u
                    if k < 3:
                        mix_s[2 * n + m, :HEAD, :] = u
                    else:
                        y_ref[rows, cols] = (y_ref[rows, cols].astype(F32) + u).astype(BF16)

        lax.fori_loop(0, D // 512, out, None)

    got(wf, w_s.at[0])
    got(ws.at[:, pl.ds(0, 6)], w_s.at[1])
    got(av.at[pl.ds(0, 7)], a_s)
    got(wov.at[pl.ds(0, 15)], wo_s)
    got(kv_k.at[:, pl.ds(0, 6)], kv_s)
    got(qv.at[pl.ds(0, 8)], o_s)

    @pl.when(z == 0)
    def _():
        for cp in part_copies():
            cp.wait_send()


def tables():
    half = HEAD // 2
    rate = (THETA ** (-np.arange(half, dtype=np.float64) / half))[None]
    fine = np.arange(OWN, dtype=np.float64)[:, None] * rate
    coarse = np.arange(16, dtype=np.float64)[:, None] * OWN * rate
    return (np.stack([np.cos(t), np.sin(t)]).astype(np.float32) for t in (fine, coarse))


def solution(mesh):
    def step(x, gain, wq, wk, wv, wo):
        fine, coarse = tables()
        anywhere = pl.BlockSpec(memory_space=pltpu.HBM)
        dma = pltpu.SemaphoreType.DMA
        return pl.pallas_call(
            kernel,
            out_shape=pltpu.VMEM((OWN, D), BF16),
            in_specs=[anywhere] * 8,
            out_specs=pl.BlockSpec(memory_space=pltpu.VMEM),
            scratch_shapes=[
                pltpu.VMEM((D,), BF16),
                pltpu.VMEM((2, OWN, HEAD // 2), F32),
                pltpu.VMEM((2, 16, HEAD // 2), F32),
                pltpu.VMEM((8, OWN, D), BF16),
                pltpu.VMEM((3, 128, D), BF16),
                pltpu.VMEM((3, 16, 128, HEAD), BF16),
                pltpu.VMEM((3, 8, 128, HEAD), BF16),
                pltpu.VMEM((16, 128, D), BF16),
                pltpu.VMEM((2, 8, OWN, HEAD), BF16),
                pltpu.VMEM((2, 8, HEAD, OWN), BF16),
                pltpu.VMEM((10, OWN, HEAD), BF16),
                pltpu.VMEM((OWN, D), BF16),
                pltpu.VMEM((10, 1, OWN), F32),
                pltpu.VMEM((10, HEAD + SUM, OWN), F32),
                pltpu.VMEM((2, 2, HEAD, OWN), BF16),
                pltpu.VMEM((2, 2, 2, OWN), F32),
                pltpu.VMEM((OWN, HEAD), BF16),
                dma((8,)),
                dma((2,)), dma((8,)), dma(()), dma((8,)),
                dma(()), dma((4, 2)), dma((4,)),
                dma(()), dma((8,)), dma((2,)), dma((4,)),
                dma(()), dma((8, 2)), dma(()), dma((4,)), dma(()),
                dma(()), dma(()), dma((2,)), dma((2,)),
            ],
            compiler_params=pltpu.CompilerParams(collective_id=0, has_side_effects=True, vmem_limit_bytes=61 * 2**20),
            name="decoder_attention",
        )(x, gain, wq, wk, wv, wo, jnp.asarray(fine), jnp.asarray(coarse))

    tokens, whole = P(("dp", "sp"), None), P("sp", None)
    return jax.shard_map(
        step,
        mesh=mesh,
        in_specs=(tokens, P(None), whole, whole, whole, whole),
        out_specs=tokens,
        check_vma=False,
    )
```

```python
import functools

import jax
import jax.numpy as jnp
import numpy as np
from jax import lax
from jax.experimental import pallas as pl
from jax.experimental.pallas import tpu as pltpu
from jax.sharding import PartitionSpec as P

NEG = -1e30
HIDDEN = 2 * NEG
LOG2E = 1.4426950408889634
HEAD = 256
THETA = 10000
D = 2048
OWN = 512
HALF = 256
SUM = 8
F32, BF16 = jnp.float32, jnp.bfloat16
MESH = pl.DeviceIdType.MESH


def _dot(a, b, ca, cb):
    return lax.dot_general(a, b, (((ca,), (cb,)), ((), ())), preferred_element_type=F32)


def kernel(x_h, gain_h, wq_h, wk_h, wv_h, wo_h, fine_h, coarse_h, y_ref,
           gain_ref, fine_ref, coarse_ref, av, wi, wf, ws, wov, kv_k, kv_v, qv, og, top_s, mix_s, part, part_f, orl,
           ld, w_s, wf_r, wfc_r, ws_r, a_s, a_r, ac_r, wo_s, wo_r, wod_r, woc_r, kv_s, kv_r, o_s, o_r, orl_s, orl_r, q_s, q_r, part_s, part_r):
    me = lax.axis_index("sp")
    x, y, z, c, p = me // 8, (me // 4) % 2, (me // 2) % 2, me % 2, me // 4
    X, Y, Z, C = me + 8 - 16 * x, me + 4 - 8 * y, me + 2 - 4 * z, me + 1 - 2 * c
    Dg = X + Y - me
    pX, pY, pD = X // 4, Y // 4, Dg // 4
    oc, oz = 1 - c, 1 - z
    head = 2 * p + c
    mine = 2 * p + c
    planes = (p, pX, pY, pD)

    def row(q, zz, cc):
        return 4 * q + 2 * zz + cc

    def rc(src, dst, ssem, rsem, dev):
        return pltpu.make_async_remote_copy(src_ref=src, dst_ref=dst, send_sem=ssem, recv_sem=rsem, device_id={"sp": dev}, device_id_type=MESH)

    def got(ref, sem, name="wait"):
        with jax.named_scope(name):
            pltpu.make_async_copy(ref, ref, sem).wait()

    def local(src, dst, n):
        cp = pltpu.make_async_copy(src, dst, ld.at[n])
        cp.start()
        return cp

    loads = (wk_h, wv_h, wq_h)
    for n, w in enumerate(loads):
        local(w, wi.at[n], 0)
    here = pl.ds(pl.multiple_of(head * HEAD, HEAD), HEAD)
    other = pl.ds(pl.multiple_of((2 * p + oc) * HEAD, HEAD), HEAD)
    sme = 2 * p + z
    load_x = local(x_h, y_ref, 1)
    load_gain = local(gain_h, gain_ref, 2)
    load_tables = (local(fine_h, fine_ref, 3), local(coarse_h, coarse_ref, 4))
    load_wo = local(wo_h, wov.at[me], 5)
    for n, w in enumerate(loads):
        local(w.at[:, here], wf.at[n, me], 6)
        local(w.at[:, other], ws.at[n, sme], 7)

    barrier = pltpu.get_barrier_semaphore()
    partners = (X, Y, Dg, X + C - me, Y + C - me, Dg + C - me, C, Z)
    for dev in partners:
        pl.semaphore_signal(barrier, inc=1, device_id={"sp": dev}, device_id_type=MESH)
    with jax.named_scope("barrier"):
        pl.semaphore_wait(barrier, len(partners))

    def send(src, dst, ssem, rsem, dev):
        rc(src, dst, ssem, rsem, dev).start()

    got(wi, ld.at[0], "load")
    for dev, q in ((X, pX), (Y, pY), (Dg, pD)):
        for hd, dst, rs in ((2 * q + c, wf.at[:, me], wf_r.at[sme]), (2 * q + oc, ws.at[:, sme], ws_r.at[sme])):
            cols = pl.ds(pl.multiple_of(hd * HEAD, HEAD), HEAD)
            send(wi.at[:, :, cols], dst, w_s.at[1], rs, dev)

    def wf_on(q, zz):
        i = row(q, zz, c)
        send(wf.at[:, i], wf.at[:, i], w_s.at[0], wf_r.at[2 * q + zz], Z)

    def ws_on(q, zz, on):
        i, s = row(q, zz, c), 2 * q + zz
        if on:
            send(ws.at[:, s], ws.at[:, s], w_s.at[0], ws_r.at[s], Z)
        send(ws.at[:, s], wf.at[:, i], w_s.at[0], wfc_r, C)

    def got_wf(n, q, zz):
        got(wf.at[:, row(q, zz, c)], wf_r.at[2 * q + zz], f"wf{n}")

    def got_ws(n, q, zz):
        got(ws.at[:, 2 * q + zz], ws_r.at[2 * q + zz], f"ws{n}")

    got(wf.at[:, me], ld.at[6])
    got(ws.at[:, sme], ld.at[7])
    wf_on(p, z)
    ws_on(p, z, True)

    load_x.wait()
    load_gain.wait()

    @jax.named_scope("norm")
    def norm(n, _):
        rows = pl.ds(pl.multiple_of(n * 128, 128), 128)
        wide = y_ref[rows, :].astype(F32)
        scale = lax.rsqrt(jnp.mean(wide * wide, -1, keepdims=True) + 1e-6)
        av[mine, rows, :] = (wide * scale * gain_ref[...].reshape(1, D).astype(F32)).astype(BF16)

    lax.fori_loop(0, OWN // 128, norm, None)

    def half_rows(half):
        return pl.ds(half * HALF if isinstance(half, int) else pl.multiple_of(half * HALF, HALF), HALF)

    def send_a(b, half, place, dev):
        rows = half_rows(half)
        send(av.at[b, rows], av.at[b, rows], a_s, a_r.at[place, half], dev)

    def give_a(b, half, n):
        rows = half_rows(half)
        send(av.at[b, rows], av.at[b, rows], a_s, ac_r.at[n], C)

    def got_a(b, half, place):
        got(av.at[b, half_rows(half)], a_r.at[place, half], f"a{half}")

    def got_given(n):
        got(av.at[0], ac_r.at[n], "given")

    send_a(mine, 0, 1, X)
    send_a(mine, 1, 2, Y)
    send_a(mine, 1, 1, X)
    send_a(mine, 0, 2, Y)
    give_a(mine, 0, 0)
    give_a(mine, 1, 0)

    for n, q in ((1, pX), (2, pY)):
        got_wf(n, q, z)
        wf_on(q, z)
    for n, q in ((1, pX), (2, pY)):
        got_ws(n, q, z)
        ws_on(q, z, True)
    got_wf(3, pD, z)
    wf_on(pD, z)
    got_ws(3, pD, z)
    ws_on(pD, z, True)
    load_wo.wait()
    send(wov.at[me], wov.at[me], wo_s, wo_r.at[sme], Z)

    for n, q in enumerate(planes):
        got_wf(n, q, oz)
        got_ws(n, q, oz)
        ws_on(q, oz, False)
    got(wf.at[:, pl.ds(0, 8)], wfc_r, "wfc")

    @jax.named_scope("project")
    def project(b, half):
        rows = half_rows(half)
        a = av[b, rows, :]
        i = 4 * (b // 2) + 2 * z + b % 2
        cb, sb = coarse_ref[0, pl.ds(i, 1), :], coarse_ref[1, pl.ds(i, 1), :]
        cf, sf = fine_ref[0, rows, :], fine_ref[1, rows, :]
        cos = cb * cf - sb * sf
        sin = sb * cf + cb * sf

        def turned(t):
            t = t.astype(BF16).astype(F32)
            u, v = t[:, : HEAD // 2], t[:, HEAD // 2 :]
            return jnp.concatenate([u * cos - v * sin, v * cos + u * sin], -1).astype(BF16)

        kv_k[z, b, rows, :] = turned(_dot(a, wf[0].reshape(D, HEAD), 1, 0))
        kv_v[z, b, :, rows] = _dot(a, wf[1].reshape(D, HEAD), 1, 0).astype(BF16).T
        qv[b, rows, :] = turned(_dot(a, wf[2].reshape(D, HEAD), 1, 0))

    def kv_copies(b, half):
        rows = half_rows(half)
        return (rc(kv_k.at[z, b, rows, :], kv_k.at[z, b, rows, :], kv_s, kv_r.at[b, half], Z),
                rc(kv_v.at[z, b, :, rows], kv_v.at[z, b, :, rows], kv_s, kv_r.at[b, half], Z))

    def q_copy(b, half):
        rows = half_rows(half)
        return rc(qv.at[b, rows, :], qv.at[b + 2, rows, :], q_s, q_r, Z)

    def send_kv(b, half):
        for cp in kv_copies(b, half):
            cp.start()

    def on(b, half):
        @pl.when(b < 6)
        def _():
            send_kv(b, half)

        @pl.when((b >= 6) & (z == 1))
        def _():
            q_copy(b, half).start()

    def core(n):
        return c + n * (oc - c)

    def own_piece(q):
        def body(n, _):
            b, half = 2 * q + core(n // 2), n % 2
            project(b, half)
            on(b, half)

        lax.fori_loop(0, 4, body, None)

    def side_half(t, n):
        isy = n % 2 if t == 0 else 1 - n // 2
        return 2 * (pX + isy * (pY - pX)) + core(n // 2 if t == 0 else n % 2), (isy + t) % 2

    hold = (p == 0) & (z == 1)
    hold_y = p == 3

    def side_pieces(t):
        def body(n, _):
            b, half = side_half(t, n)
            project(b, half)
            if t == 0:
                on(b, half)
            else:
                @pl.when(jnp.logical_not(hold | (hold_y & (n < 2))))
                def _():
                    on(b, half)

        lax.fori_loop(0, 4, body, None)

    for cp in load_tables:
        cp.wait()
    got_given(0)
    own_piece(p)

    bX, bY, bD = 2 * pX + c, 2 * pY + c, 2 * pD + c
    got_a(bX, 0, 1)
    send_a(bX, 0, 3, Y)
    give_a(bX, 0, 1)
    got_a(bY, 1, 2)
    send_a(bY, 1, 3, X)
    give_a(bY, 1, 1)
    got_given(1)
    side_pieces(0)

    iz = row(p, oz, c)

    def give_wo(i, place):
        send(wov.at[i], wov.at[i], wo_s, woc_r.at[place], C)

    got(wov.at[iz], wo_r.at[2 * p + oz], "wo_z")
    for i, zz in ((me, z), (iz, oz)):
        for dev in (X, Y):
            send(wov.at[i], wov.at[i], wo_s, wo_r.at[2 * p + zz], dev)
        give_wo(i, 0)

    e = HEAD**-0.5 * LOG2E
    top_s[...] = jnp.full(top_s.shape, NEG, F32)
    mix_s[...] = jnp.zeros(mix_s.shape, F32)

    def tile(zz, kb, bq, masked, rows):
        s = _dot(kv_k[zz, kb, rows, :], qv[bq], 1, 1)
        if masked:
            ok = lax.broadcasted_iota(jnp.int32, s.shape, 1) >= lax.broadcasted_iota(jnp.int32, s.shape, 0)
            s = jnp.where(ok, s, HIDDEN)
        return s

    every = pl.ds(0, OWN)

    def attend(work, rows=every):
        scores = [[tile(zz, kb, bq, masked, rows) for zz, kb, masked in keys] for bq, keys in work]
        for (bq, keys), ss in zip(work, scores):
            old = top_s[bq]
            top = old
            for s in ss:
                top = jnp.maximum(top, s.max(axis=0, keepdims=True))
            top_s[bq] = top
            keep = jnp.exp2((old - top) * e)
            total = mix_s[bq] * keep
            for (zz, kb, _), s in zip(keys, ss):
                w = jnp.exp2((s - top) * e).astype(BF16)
                total = total + _dot(jnp.concatenate([kv_v[zz, kb, :, rows], jnp.ones((SUM, rows.size), BF16)], axis=0), w, 1, 0)
            mix_s[bq] = total

    @jax.named_scope("pair")
    def pair(zz, kp, qp):
        keys = [(zz, 2 * kp, False), (zz, 2 * kp + 1, False)]
        attend([(2 * qp, keys), (2 * qp + 1, keys)])

    @jax.named_scope("diagonal")
    def diagonal(kp):
        attend([(2 * kp, [(z, 2 * kp, True)]), (2 * kp + 1, [(z, 2 * kp, False), (z, 2 * kp + 1, True)])])

    diagonal(p)

    got_a(bX, 1, 1)
    give_a(bX, 1, 2)
    got_a(bY, 0, 2)
    give_a(bY, 0, 2)
    got_given(2)
    side_pieces(1)
    even = 1 - (x + y) % 2

    def near(n, _):
        @pl.when(n > 0)
        def _():
            diagonal(pX * (n == 1) + pY * (n == 2))

        low = y * (n == 0) + 2 * x * (n == 1) + even * (n == 2)
        high = (y + 2) * (n == 0) + (2 * x + 1) * (n == 1) + (3 - even) * (n == 2)
        pair(z, low, high)

    lax.fori_loop(0, 3, near, None)

    def part_copies():
        return (rc(part.at[0], part.at[1], part_s.at[0], part_r.at[0], Z), rc(part_f.at[0], part_f.at[1], part_s.at[1], part_r.at[1], Z))

    def send_part():
        got(qv.at[pl.ds(8, 2)], q_r, "q")
        pair(z, 3, 4)
        for n in (0, 1):
            mix = mix_s[8 + n]
            total = mix[HEAD : HEAD + 1]
            part[0, n] = (mix[:HEAD] * (1 / total)).astype(BF16)
            part_f[0, n] = jnp.concatenate([top_s[8 + n], total], axis=0)
        for cp in part_copies():
            cp.start()

    @pl.when((z == 0) & (p == 3))
    def _():
        send_part()

    def got_kv(b, half):
        got(kv_k.at[oz, b], kv_r.at[b, half], "kv")

    def got_piece(kp):
        for n in (0, 1):
            for half in (0, 1):
                got_kv(2 * kp + n, half)

    def near_remote(n, _):
        qp = p * (n == 0) + pX * (n == 1) + pY * (n == 2)
        pl.when(qp >= p + oz)(lambda: pair(oz, p, qp))

    @pl.when(p < 3)
    def _():
        got_piece(p)
        lax.fori_loop(0, 3, near_remote, None)

    for half in (0, 1):
        got_a(bD, half, 3)
        give_a(bD, half, 3)
    got_given(3)
    own_piece(pD)

    @pl.when(hold)
    def _():
        for n in range(4):
            send_kv(*side_half(1, n))

    @pl.when(hold_y)
    def _():
        for n in range(2):
            send_kv(*side_half(1, n))

    diagonal(pD)

    def far(n, _):
        low = (1 - even) * (n == 0) + 2 * (1 - x) * (n == 1) + (1 - y) * (n == 2)
        high = (2 + even) * (n == 0) + (3 - 2 * x) * (n == 1) + (3 - y) * (n == 2)
        pair(z, low, high)

    lax.fori_loop(0, 3, far, None)

    iX, iY, iD = row(pX, z, c), row(pY, z, c), row(pD, z, c)
    for n, (i, q, dev) in enumerate(((iX, pX, Y), (iY, pY, X))):
        got(wov.at[i], wo_r.at[2 * q + z], f"wo{n}")
        rows = pl.ds(n * 64, 64)
        send(wov.at[i, rows], wov.at[i, rows], wo_s, wod_r.at[n], dev)
        give_wo(i, 1 + n)

    def wo_rest():
        for n in (0, 1):
            got(wov.at[iD, pl.ds(n * 64, 64)], wod_r.at[n], f"wod{n}")
        send(wov.at[iD], wov.at[iD], wo_s, wo_r.at[2 * pD + z], Z)
        give_wo(iD, 3)
        for n, q in enumerate((pX, pY)):
            i = row(q, oz, c)
            got(wov.at[i], wo_r.at[2 * q + oz], f"wo_oz{n}")
            give_wo(i, 1 + n)

    cols = pl.ds(pl.multiple_of(head * HEAD, HEAD), HEAD)

    def o_copy(b, rows):
        place = 2 * ((b // 2 % 2 + y) % 2) + (b // 4 + x) % 2
        return rc(qv.at[b, rows], og.at[rows, cols], o_s, o_r.at[place], row(b // 2, z, b % 2))

    by_y = (2 * pD + 1) * (1 - x) - x

    def finish(b, _):
        with jax.named_scope("finish"):
            mix = mix_s[b]
            qv[b] = (mix[:HEAD] * (1 / mix[HEAD : HEAD + 1])).T.astype(BF16)

        @pl.when((b != mine) & (b != by_y))
        def _():
            o_copy(b, every).start()

        @pl.when(b == by_y)
        def _():
            o_copy(b, half_rows(0)).start()
            send(qv.at[b, half_rows(1)], orl, o_s, orl_r, Y)

    def finish_pieces(first, last):
        lax.fori_loop(2 * first, 2 * last, finish, None)

    first, last = (3 - p) // 3, p // 3
    kp0, kp1 = p - 2 * last, first
    done0, done1 = first, 2 - p // 2 * (3 - p)

    def remote_piece(kp, done):
        got_piece(kp)

        def body(qp, _):
            pair(oz, kp, qp)
            pl.when(qp < done)(lambda: finish_pieces(qp, qp + 1))

        lax.fori_loop(kp + oz, 4, body, None)

    def remote_blocks(kp, done):
        for n in (0, 1):
            block = 2 * kp + core(n)
            got_kv(block, 0)
            got_kv(block, 1)

            def body(qp, _):
                with jax.named_scope("one"):
                    attend([(2 * qp + m, [(oz, block, False)]) for m in (0, 1)])
                if n:
                    pl.when(qp < done)(lambda: finish_pieces(qp, qp + 1))

            lax.fori_loop(kp + oz, 4, body, None)

    def last_piece(kp):
        block = 2 * kp + core(0)
        got_kv(block, 0)
        got_kv(block, 1)

        def piece(n):
            return z * (kp + oz + n) + oz * (3 - n)

        def first(n, _):
            with jax.named_scope("one"):
                attend([(2 * piece(n) + m, [(oz, block, False)]) for m in (0, 1)])

        lax.fori_loop(0, 4 - kp - oz, first, None)
        wo_rest()
        block2 = 2 * kp + core(1)
        for k in (0, 1):
            half = k + last * (1 - 2 * k)
            got_kv(block2, half)

            def second(n, _):
                qp = piece(n)
                with jax.named_scope("half"):
                    attend([(2 * qp + m, [(oz, block2, False)]) for m in (0, 1)], half_rows(half))
                if k:
                    @pl.when((qp < 3) | (z == 0))
                    def _():
                        finish_pieces(qp, qp + 1)

            lax.fori_loop(0, 4 - kp - oz, second, None)

    finish_pieces(0, oz)

    @pl.when(last == 0)
    def _():
        pl.when(pD >= p + oz)(lambda: pair(oz, p, pD))
        finish_pieces(oz, done0 + oz)

    @pl.when(last == 1)
    def _():
        remote_piece(kp0, 0)

    @pl.when((z == 0) & (p < 3))
    def _():
        send_part()


    @pl.when(last == 0)
    def _():
        remote_piece(kp1, done1 + oz)

    @pl.when(last == 1)
    def _():
        remote_blocks(kp1, done1 + oz)

    last_piece(3 - kp0 - kp1)

    @pl.when(z == 1)
    def _():
        got(qv.at[pl.ds(0, 2)], q_s, "q_left")
        got(part.at[1], part_r.at[0], "part")
        got(part_f.at[1], part_r.at[1], "part")
        for n in (0, 1):
            old, came, count = top_s[6 + n], part_f[1, n, 0:1], part_f[1, n, 1:2]
            top = jnp.maximum(old, came)
            keep, add = jnp.exp2((old - top) * e), jnp.exp2((came - top) * e) * count
            mix = mix_s[6 + n]
            more = jnp.concatenate([part[1, n].astype(F32) * add, jnp.broadcast_to(add, (SUM, OWN))], axis=0)
            mix_s[6 + n] = mix * keep + more

        finish_pieces(3, 4)

    og[:, cols] = qv[mine]
    def relay():
        from_y = pl.ds(pl.multiple_of((2 * pY + c) * HEAD, HEAD), HEAD)
        return rc(orl, og.at[half_rows(1), from_y], orl_s, o_r.at[3], row(pX, z, 1))

    for k, q in enumerate(planes):
        heads = pl.ds(pl.multiple_of(q * 2 * HEAD, 2 * HEAD), 2 * HEAD)
        if k == 1:
            @pl.when(x == 0)
            def _():
                got(orl, orl_r, "relay")
                relay().start()

            i = row(pD, oz, c)
            got(wov.at[i], wo_r.at[2 * pD + oz], "wo_dz")
            give_wo(i, 3)
        got(wov.at[pl.ds(0, 2)], woc_r.at[k], "wo_c")
        got(og.at[:, heads] if k else qv.at[0], o_r.at[k], "og")

        def out(n, _):
            cols = pl.ds(pl.multiple_of(n * 512, 512), 512)
            with jax.named_scope("out"):
                t = _dot(og[:, heads], wov[pl.ds(4 * q, 4), :, cols].reshape(2 * HEAD, 512), 1, 0)
                for m in range(2):
                    rows = pl.ds(m * HEAD, HEAD)
                    u = t[m * HEAD : (m + 1) * HEAD]
                    if k:
                        u = mix_s[2 * n + m, :HEAD, :] + u
                    if k < 3:
                        mix_s[2 * n + m, :HEAD, :] = u
                    else:
                        y_ref[rows, cols] = (y_ref[rows, cols].astype(F32) + u).astype(BF16)

        lax.fori_loop(0, D // 512, out, None)

    got(wf, w_s.at[0])
    got(ws.at[:, pl.ds(0, 6)], w_s.at[1])
    got(av.at[pl.ds(0, 7)], a_s)
    got(wov.at[pl.ds(0, 15)], wo_s)
    got(kv_k.at[:, pl.ds(0, 6)], kv_s)
    got(qv.at[pl.ds(0, 7)], o_s)
    pl.when(x == 0)(lambda: relay().wait_send())

    @pl.when(z == 0)
    def _():
        for cp in part_copies():
            cp.wait_send()


def tables():
    half = HEAD // 2
    rate = (THETA ** (-np.arange(half, dtype=np.float64) / half))[None]
    fine = np.arange(OWN, dtype=np.float64)[:, None] * rate
    coarse = np.arange(16, dtype=np.float64)[:, None] * OWN * rate
    return (np.stack([np.cos(t), np.sin(t)]).astype(np.float32) for t in (fine, coarse))


def solution(mesh):
    def step(x, gain, wq, wk, wv, wo):
        fine, coarse = tables()
        anywhere = pl.BlockSpec(memory_space=pltpu.HBM)
        dma = pltpu.SemaphoreType.DMA
        return pl.pallas_call(
            kernel,
            out_shape=pltpu.VMEM((OWN, D), BF16),
            in_specs=[anywhere] * 8,
            out_specs=pl.BlockSpec(memory_space=pltpu.VMEM),
            scratch_shapes=[
                pltpu.VMEM((D,), BF16),
                pltpu.VMEM((2, OWN, HEAD // 2), F32),
                pltpu.VMEM((2, 16, HEAD // 2), F32),
                pltpu.VMEM((8, OWN, D), BF16),
                pltpu.VMEM((3, 128, D), BF16),
                pltpu.VMEM((3, 16, 128, HEAD), BF16),
                pltpu.VMEM((3, 8, 128, HEAD), BF16),
                pltpu.VMEM((16, 128, D), BF16),
                pltpu.VMEM((2, 8, OWN, HEAD), BF16),
                pltpu.VMEM((2, 8, HEAD, OWN), BF16),
                pltpu.VMEM((10, OWN, HEAD), BF16),
                pltpu.VMEM((OWN, D), BF16),
                pltpu.VMEM((10, 1, OWN), F32),
                pltpu.VMEM((10, HEAD + SUM, OWN), F32),
                pltpu.VMEM((2, 2, HEAD, OWN), BF16),
                pltpu.VMEM((2, 2, 2, OWN), F32),
                pltpu.VMEM((HALF, HEAD), BF16),
                dma((8,)),
                dma((2,)), dma((8,)), dma(()), dma((8,)),
                dma(()), dma((4, 2)), dma((4,)),
                dma(()), dma((8,)), dma((2,)), dma((4,)),
                dma(()), dma((8, 2)), dma(()), dma((4,)), dma(()), dma(()),
                dma(()), dma(()), dma((2,)), dma((2,)),
            ],
            compiler_params=pltpu.CompilerParams(collective_id=0, has_side_effects=True, vmem_limit_bytes=61 * 2**20),
            name="decoder_attention",
        )(x, gain, wq, wk, wv, wo, jnp.asarray(fine), jnp.asarray(coarse))

    tokens, whole = P(("dp", "sp"), None), P("sp", None)
    return jax.shard_map(
        step,
        mesh=mesh,
        in_specs=(tokens, P(None), whole, whole, whole, whole),
        out_specs=tokens,
        check_vma=False,
    )
```

```python
import functools

import jax
import jax.numpy as jnp
import numpy as np
from jax import lax
from jax.experimental import pallas as pl
from jax.experimental.pallas import tpu as pltpu
from jax.sharding import PartitionSpec as P

NEG = -1e30
HIDDEN = 2 * NEG
LOG2E = 1.4426950408889634
HEAD = 256
THETA = 10000
D = 2048
OWN = 512
HALF = 256
SUM = 8
F32, BF16 = jnp.float32, jnp.bfloat16
MESH = pl.DeviceIdType.MESH


def _dot(a, b, ca, cb):
    return lax.dot_general(a, b, (((ca,), (cb,)), ((), ())), preferred_element_type=F32)


def kernel(x_h, gain_h, wq_h, wk_h, wv_h, wo_h, fine_h, coarse_h, y_ref,
           gain_ref, fine_ref, coarse_ref, av, wi, wf, ws, wov, kv_k, kv_v, qv, og, top_s, mix_s, part, part_f, orl,
           ld, w_s, wf_r, wfc_r, ws_r, a_s, a_r, ac_r, wo_s, wo_r, wod_r, woc_r, kv_s, kv_r, o_s, o_r, orl_s, orl_r, q_s, q_r, part_s, part_r):
    me = lax.axis_index("sp")
    x, y, z, c, p = me // 8, (me // 4) % 2, (me // 2) % 2, me % 2, me // 4
    X, Y, Z, C = me + 8 - 16 * x, me + 4 - 8 * y, me + 2 - 4 * z, me + 1 - 2 * c
    Dg = X + Y - me
    pX, pY, pD = X // 4, Y // 4, Dg // 4
    oc, oz = 1 - c, 1 - z
    head = 2 * p + c
    mine = 2 * p + c
    planes = (p, pX, pY, pD)

    def row(q, zz, cc):
        return 4 * q + 2 * zz + cc

    def rc(src, dst, ssem, rsem, dev):
        return pltpu.make_async_remote_copy(src_ref=src, dst_ref=dst, send_sem=ssem, recv_sem=rsem, device_id={"sp": dev}, device_id_type=MESH)

    def got(ref, sem, name="wait"):
        with jax.named_scope(name):
            pltpu.make_async_copy(ref, ref, sem).wait()

    def local(src, dst, n):
        cp = pltpu.make_async_copy(src, dst, ld.at[n])
        cp.start()
        return cp

    loads = (wk_h, wv_h, wq_h)
    for n, w in enumerate(loads):
        local(w, wi.at[n], 0)
    here = pl.ds(pl.multiple_of(head * HEAD, HEAD), HEAD)
    other = pl.ds(pl.multiple_of((2 * p + oc) * HEAD, HEAD), HEAD)
    sme = 2 * p + z
    load_x = local(x_h, y_ref, 1)
    load_gain = local(gain_h, gain_ref, 2)
    load_tables = (local(fine_h, fine_ref, 3), local(coarse_h, coarse_ref, 4))
    load_wo = local(wo_h, wov.at[me], 5)
    for n, w in enumerate(loads):
        local(w.at[:, here], wf.at[n, me], 6)
        local(w.at[:, other], ws.at[n, sme], 7)

    barrier = pltpu.get_barrier_semaphore()
    partners = (X, Y, Dg, X + C - me, Y + C - me, Dg + C - me, C, Z)
    for dev in partners:
        pl.semaphore_signal(barrier, inc=1, device_id={"sp": dev}, device_id_type=MESH)
    with jax.named_scope("barrier"):
        pl.semaphore_wait(barrier, len(partners))

    def send(src, dst, ssem, rsem, dev):
        rc(src, dst, ssem, rsem, dev).start()

    got(wi, ld.at[0], "load")
    for dev, q in ((X, pX), (Y, pY), (Dg, pD)):
        for hd, dst, rs in ((2 * q + c, wf.at[:, me], wf_r.at[sme]), (2 * q + oc, ws.at[:, sme], ws_r.at[sme])):
            cols = pl.ds(pl.multiple_of(hd * HEAD, HEAD), HEAD)
            send(wi.at[:, :, cols], dst, w_s.at[1], rs, dev)

    def wf_on(q, zz):
        i = row(q, zz, c)
        send(wf.at[:, i], wf.at[:, i], w_s.at[0], wf_r.at[2 * q + zz], Z)

    def ws_on(q, zz, on):
        i, s = row(q, zz, c), 2 * q + zz
        if on:
            send(ws.at[:, s], ws.at[:, s], w_s.at[0], ws_r.at[s], Z)
        send(ws.at[:, s], wf.at[:, i], w_s.at[0], wfc_r, C)

    def got_wf(n, q, zz):
        got(wf.at[:, row(q, zz, c)], wf_r.at[2 * q + zz], f"wf{n}")

    def got_ws(n, q, zz):
        got(ws.at[:, 2 * q + zz], ws_r.at[2 * q + zz], f"ws{n}")

    got(wf.at[:, me], ld.at[6])
    got(ws.at[:, sme], ld.at[7])
    wf_on(p, z)
    ws_on(p, z, True)

    load_x.wait()
    load_gain.wait()

    @jax.named_scope("norm")
    def norm(n, _):
        rows = pl.ds(pl.multiple_of(n * 128, 128), 128)
        wide = y_ref[rows, :].astype(F32)
        scale = lax.rsqrt(jnp.mean(wide * wide, -1, keepdims=True) + 1e-6)
        av[mine, rows, :] = (wide * scale * gain_ref[...].reshape(1, D).astype(F32)).astype(BF16)

    lax.fori_loop(0, OWN // 128, norm, None)

    def half_rows(half):
        return pl.ds(half * HALF if isinstance(half, int) else pl.multiple_of(half * HALF, HALF), HALF)

    def send_a(b, half, place, dev):
        rows = half_rows(half)
        send(av.at[b, rows], av.at[b, rows], a_s, a_r.at[place, half], dev)

    def give_a(b, half, n):
        rows = half_rows(half)
        send(av.at[b, rows], av.at[b, rows], a_s, ac_r.at[n], C)

    def got_a(b, half, place):
        got(av.at[b, half_rows(half)], a_r.at[place, half], f"a{half}")

    def got_given(n):
        got(av.at[0], ac_r.at[n], "given")

    send_a(mine, 0, 1, X)
    send_a(mine, 1, 2, Y)
    send_a(mine, 1, 1, X)
    send_a(mine, 0, 2, Y)
    give_a(mine, 0, 0)
    give_a(mine, 1, 0)

    for n, q in ((1, pX), (2, pY)):
        got_wf(n, q, z)
        wf_on(q, z)
    for n, q in ((1, pX), (2, pY)):
        got_ws(n, q, z)
        ws_on(q, z, True)
    got_wf(3, pD, z)
    wf_on(pD, z)
    got_ws(3, pD, z)
    ws_on(pD, z, True)
    load_wo.wait()
    send(wov.at[me], wov.at[me], wo_s, wo_r.at[sme], Z)

    for n, q in enumerate(planes):
        got_wf(n, q, oz)
        got_ws(n, q, oz)
        ws_on(q, oz, False)
    got(wf.at[:, pl.ds(0, 8)], wfc_r, "wfc")

    @jax.named_scope("project")
    def project(b, half):
        rows = half_rows(half)
        a = av[b, rows, :]
        i = 4 * (b // 2) + 2 * z + b % 2
        cb, sb = coarse_ref[0, pl.ds(i, 1), :], coarse_ref[1, pl.ds(i, 1), :]
        cf, sf = fine_ref[0, rows, :], fine_ref[1, rows, :]
        cos = cb * cf - sb * sf
        sin = sb * cf + cb * sf

        def turned(t):
            t = t.astype(BF16).astype(F32)
            u, v = t[:, : HEAD // 2], t[:, HEAD // 2 :]
            return jnp.concatenate([u * cos - v * sin, v * cos + u * sin], -1).astype(BF16)

        kv_k[z, b, rows, :] = turned(_dot(a, wf[0].reshape(D, HEAD), 1, 0))
        kv_v[z, b, :, rows] = _dot(a, wf[1].reshape(D, HEAD), 1, 0).astype(BF16).T
        qv[b, rows, :] = turned(_dot(a, wf[2].reshape(D, HEAD), 1, 0))

    def kv_copies(b, half):
        rows = half_rows(half)
        return (rc(kv_k.at[z, b, rows, :], kv_k.at[z, b, rows, :], kv_s, kv_r.at[b, half], Z),
                rc(kv_v.at[z, b, :, rows], kv_v.at[z, b, :, rows], kv_s, kv_r.at[b, half], Z))

    def q_copy(b, half):
        rows = half_rows(half)
        return rc(qv.at[b, rows, :], qv.at[b + 2, rows, :], q_s, q_r, Z)

    def send_kv(b, half):
        for cp in kv_copies(b, half):
            cp.start()

    def on(b, half):
        @pl.when(b < 6)
        def _():
            send_kv(b, half)

        @pl.when((b >= 6) & (z == 1))
        def _():
            q_copy(b, half).start()

    def core(n):
        return c + n * (oc - c)

    def own_piece(q):
        def body(n, _):
            b, half = 2 * q + core(n // 2), n % 2
            project(b, half)
            on(b, half)

        lax.fori_loop(0, 4, body, None)

    def side_half(t, n):
        isy = n % 2 if t == 0 else 1 - n // 2
        return 2 * (pX + isy * (pY - pX)) + core(n // 2 if t == 0 else n % 2), (isy + t) % 2

    hold = (p == 0) & (z == 1)
    hold_y = p == 3

    def side_pieces(t):
        def body(n, _):
            b, half = side_half(t, n)
            project(b, half)
            if t == 0:
                on(b, half)
            else:
                @pl.when(jnp.logical_not(hold | (hold_y & (n < 2))))
                def _():
                    on(b, half)

        lax.fori_loop(0, 4, body, None)

    for cp in load_tables:
        cp.wait()
    got_given(0)
    own_piece(p)

    bX, bY, bD = 2 * pX + c, 2 * pY + c, 2 * pD + c
    got_a(bX, 0, 1)
    send_a(bX, 0, 3, Y)
    give_a(bX, 0, 1)
    got_a(bY, 1, 2)
    send_a(bY, 1, 3, X)
    give_a(bY, 1, 1)
    got_given(1)
    side_pieces(0)

    iz = row(p, oz, c)

    def give_wo(i, place):
        send(wov.at[i], wov.at[i], wo_s, woc_r.at[place], C)

    got(wov.at[iz], wo_r.at[2 * p + oz], "wo_z")
    for i, zz in ((me, z), (iz, oz)):
        for dev in (X, Y):
            send(wov.at[i], wov.at[i], wo_s, wo_r.at[2 * p + zz], dev)
        give_wo(i, 0)

    e = HEAD**-0.5 * LOG2E
    top_s[...] = jnp.full(top_s.shape, NEG, F32)
    mix_s[...] = jnp.zeros(mix_s.shape, F32)

    def tile(zz, kb, bq, masked, rows):
        s = _dot(kv_k[zz, kb, rows, :], qv[bq], 1, 1)
        if masked:
            ok = lax.broadcasted_iota(jnp.int32, s.shape, 1) >= lax.broadcasted_iota(jnp.int32, s.shape, 0)
            s = jnp.where(ok, s, HIDDEN)
        return s

    every = pl.ds(0, OWN)

    def attend(work, rows=every):
        scores = [[tile(zz, kb, bq, masked, rows) for zz, kb, masked in keys] for bq, keys in work]
        for (bq, keys), ss in zip(work, scores):
            old = top_s[bq]
            top = old
            for s in ss:
                top = jnp.maximum(top, s.max(axis=0, keepdims=True))
            top_s[bq] = top
            keep = jnp.exp2((old - top) * e)
            total = mix_s[bq] * keep
            for (zz, kb, _), s in zip(keys, ss):
                w = jnp.exp2((s - top) * e).astype(BF16)
                total = total + _dot(jnp.concatenate([kv_v[zz, kb, :, rows], jnp.ones((SUM, rows.size), BF16)], axis=0), w, 1, 0)
            mix_s[bq] = total

    @jax.named_scope("pair")
    def pair(zz, kp, qp):
        keys = [(zz, 2 * kp, False), (zz, 2 * kp + 1, False)]
        attend([(2 * qp, keys), (2 * qp + 1, keys)])

    @jax.named_scope("diagonal")
    def diagonal(kp):
        attend([(2 * kp, [(z, 2 * kp, True)]), (2 * kp + 1, [(z, 2 * kp, False), (z, 2 * kp + 1, True)])])

    diagonal(p)

    got_a(bX, 1, 1)
    give_a(bX, 1, 2)
    got_a(bY, 0, 2)
    give_a(bY, 0, 2)
    got_given(2)
    side_pieces(1)
    even = 1 - (x + y) % 2

    def near(n, _):
        @pl.when(n > 0)
        def _():
            diagonal(pX * (n == 1) + pY * (n == 2))

        low = y * (n == 0) + 2 * x * (n == 1) + even * (n == 2)
        high = (y + 2) * (n == 0) + (2 * x + 1) * (n == 1) + (3 - even) * (n == 2)
        pair(z, low, high)

    lax.fori_loop(0, 3, near, None)

    def part_copies():
        return (rc(part.at[0], part.at[1], part_s.at[0], part_r.at[0], Z), rc(part_f.at[0], part_f.at[1], part_s.at[1], part_r.at[1], Z))

    def send_part():
        got(qv.at[pl.ds(8, 2)], q_r, "q")
        pair(z, 3, 4)
        for n in (0, 1):
            mix = mix_s[8 + n]
            total = mix[HEAD : HEAD + 1]
            part[0, n] = (mix[:HEAD] * (1 / total)).astype(BF16)
            part_f[0, n] = jnp.concatenate([top_s[8 + n], total], axis=0)
        for cp in part_copies():
            cp.start()

    @pl.when((z == 0) & (p == 3))
    def _():
        send_part()

    def got_kv(b, half):
        got(kv_k.at[oz, b], kv_r.at[b, half], "kv")

    def got_piece(kp):
        for n in (0, 1):
            for half in (0, 1):
                got_kv(2 * kp + n, half)

    def near_remote(n, _):
        qp = p * (n == 0) + pX * (n == 1) + pY * (n == 2)
        pl.when(qp >= p + oz)(lambda: pair(oz, p, qp))

    @pl.when(p < 3)
    def _():
        got_piece(p)
        lax.fori_loop(0, 3, near_remote, None)

    for half in (0, 1):
        got_a(bD, half, 3)
        give_a(bD, half, 3)
    got_given(3)
    own_piece(pD)

    @pl.when(hold)
    def _():
        for n in range(4):
            send_kv(*side_half(1, n))

    @pl.when(hold_y)
    def _():
        for n in range(2):
            send_kv(*side_half(1, n))

    diagonal(pD)

    def far(n, _):
        low = (1 - even) * (n == 0) + 2 * (1 - x) * (n == 1) + (1 - y) * (n == 2)
        high = (2 + even) * (n == 0) + (3 - 2 * x) * (n == 1) + (3 - y) * (n == 2)
        pair(z, low, high)

    lax.fori_loop(0, 3, far, None)

    iX, iY, iD = row(pX, z, c), row(pY, z, c), row(pD, z, c)
    for n, (i, q, dev) in enumerate(((iX, pX, Y), (iY, pY, X))):
        got(wov.at[i], wo_r.at[2 * q + z], f"wo{n}")
        rows = pl.ds(n * 64, 64)
        send(wov.at[i, rows], wov.at[i, rows], wo_s, wod_r.at[n], dev)
        give_wo(i, 1 + n)

    def wo_rest():
        for n in (0, 1):
            got(wov.at[iD, pl.ds(n * 64, 64)], wod_r.at[n], f"wod{n}")
        send(wov.at[iD], wov.at[iD], wo_s, wo_r.at[2 * pD + z], Z)
        give_wo(iD, 3)
        for n, q in enumerate((pX, pY)):
            i = row(q, oz, c)
            got(wov.at[i], wo_r.at[2 * q + oz], f"wo_oz{n}")
            give_wo(i, 1 + n)

    cols = pl.ds(pl.multiple_of(head * HEAD, HEAD), HEAD)

    def o_copy(b):
        place = 2 * ((b // 2 % 2 + y) % 2) + (b // 4 + x) % 2
        return rc(qv.at[b], og.at[:, cols], o_s, o_r.at[place], row(b // 2, z, b % 2))

    by_y = (2 * pD + 1) * (1 - x) - x

    def finish(n, _):
        b = n + 1 - 2 * (n % 2)
        with jax.named_scope("finish"):
            mix = mix_s[b]
            qv[b] = (mix[:HEAD] * (1 / mix[HEAD : HEAD + 1])).T.astype(BF16)

        @pl.when((b != mine) & (b != by_y))
        def _():
            o_copy(b).start()

        @pl.when(b == by_y)
        def _():
            send(qv.at[b], orl, o_s, orl_r, Y)

    def finish_pieces(first, last):
        lax.fori_loop(2 * first, 2 * last, finish, None)

    first, last = (3 - p) // 3, p // 3
    kp0, kp1 = p - 2 * last, first
    done0, done1 = first, 2 - p // 2 * (3 - p)

    def remote_piece(kp, done):
        got_piece(kp)

        def body(qp, _):
            pair(oz, kp, qp)
            pl.when(qp < done)(lambda: finish_pieces(qp, qp + 1))

        lax.fori_loop(kp + oz, 4, body, None)

    def remote_blocks(kp, done):
        for n in (0, 1):
            block = 2 * kp + core(n)
            got_kv(block, 0)
            got_kv(block, 1)

            def body(qp, _):
                with jax.named_scope("one"):
                    attend([(2 * qp + m, [(oz, block, False)]) for m in (0, 1)])
                if n:
                    pl.when(qp < done)(lambda: finish_pieces(qp, qp + 1))

            lax.fori_loop(kp + oz, 4, body, None)

    def last_piece(kp):
        block = 2 * kp + core(0)
        got_kv(block, 0)
        got_kv(block, 1)

        def piece(n):
            return z * (kp + oz + n) + oz * (3 - n)

        def first(n, _):
            with jax.named_scope("one"):
                attend([(2 * piece(n) + m, [(oz, block, False)]) for m in (0, 1)])

        lax.fori_loop(0, 4 - kp - oz, first, None)
        wo_rest()
        block2 = 2 * kp + core(1)
        for k in (0, 1):
            half = k + last * (1 - 2 * k)
            got_kv(block2, half)

            def second(n, _):
                qp = piece(n)
                with jax.named_scope("half"):
                    attend([(2 * qp + m, [(oz, block2, False)]) for m in (0, 1)], half_rows(half))
                if k:
                    @pl.when((qp < 3) | (z == 0))
                    def _():
                        finish_pieces(qp, qp + 1)

            lax.fori_loop(0, 4 - kp - oz, second, None)

    finish_pieces(0, oz)

    @pl.when(last == 0)
    def _():
        pl.when(pD >= p + oz)(lambda: pair(oz, p, pD))
        finish_pieces(oz, done0 + oz)

    @pl.when(last == 1)
    def _():
        remote_piece(kp0, 0)

    @pl.when((z == 0) & (p < 3))
    def _():
        send_part()


    @pl.when(last == 0)
    def _():
        remote_piece(kp1, done1 + oz)

    @pl.when(last == 1)
    def _():
        remote_blocks(kp1, done1 + oz)

    last_piece(3 - kp0 - kp1)

    @pl.when(z == 1)
    def _():
        got(qv.at[pl.ds(0, 2)], q_s, "q_left")
        got(part.at[1], part_r.at[0], "part")
        got(part_f.at[1], part_r.at[1], "part")
        for n in (0, 1):
            old, came, count = top_s[6 + n], part_f[1, n, 0:1], part_f[1, n, 1:2]
            top = jnp.maximum(old, came)
            keep, add = jnp.exp2((old - top) * e), jnp.exp2((came - top) * e) * count
            mix = mix_s[6 + n]
            more = jnp.concatenate([part[1, n].astype(F32) * add, jnp.broadcast_to(add, (SUM, OWN))], axis=0)
            mix_s[6 + n] = mix * keep + more

        finish_pieces(3, 4)

    og[:, cols] = qv[mine]
    def relay():
        from_y = pl.ds(pl.multiple_of((2 * pY + c) * HEAD, HEAD), HEAD)
        return rc(orl, og.at[:, from_y], orl_s, o_r.at[3], row(pX, z, 1))

    def heads(q):
        return pl.ds(pl.multiple_of(q * 2 * HEAD, 2 * HEAD), 2 * HEAD)

    def ready(k):
        got(wov.at[pl.ds(0, 2)], woc_r.at[k], "wo_c")
        got(og.at[:, heads(planes[k])] if k else qv.at[0], o_r.at[k], f"og{k}")

    for ks in ((0,), (1,), (2, 3)):
        if ks == (1,):
            @pl.when(x == 0)
            def _():
                got(orl, orl_r, "relay")
                relay().start()

            i = row(pD, oz, c)
            got(wov.at[i], wo_r.at[2 * pD + oz], "wo_dz")
            give_wo(i, 3)
        for k in ks:
            ready(k)

        def out(n, _):
            cols = pl.ds(pl.multiple_of(n * 512, 512), 512)
            with jax.named_scope("out"):
                t = sum(_dot(og[:, heads(planes[k])], wov[pl.ds(4 * planes[k], 4), :, cols].reshape(2 * HEAD, 512), 1, 0) for k in ks)
                for m in range(2):
                    rows = pl.ds(m * HEAD, HEAD)
                    u = t[m * HEAD : (m + 1) * HEAD]
                    if ks != (0,):
                        u = mix_s[2 * n + m, :HEAD, :] + u
                    if 3 in ks:
                        y_ref[rows, cols] = (y_ref[rows, cols].astype(F32) + u).astype(BF16)
                    else:
                        mix_s[2 * n + m, :HEAD, :] = u

        lax.fori_loop(0, D // 512, out, None)

    got(wf, w_s.at[0])
    got(ws.at[:, pl.ds(0, 6)], w_s.at[1])
    got(av.at[pl.ds(0, 7)], a_s)
    got(wov.at[pl.ds(0, 15)], wo_s)
    got(kv_k.at[:, pl.ds(0, 6)], kv_s)
    got(qv.at[pl.ds(0, 7)], o_s)
    pl.when(x == 0)(lambda: relay().wait_send())

    @pl.when(z == 0)
    def _():
        for cp in part_copies():
            cp.wait_send()


def tables():
    half = HEAD // 2
    rate = (THETA ** (-np.arange(half, dtype=np.float64) / half))[None]
    fine = np.arange(OWN, dtype=np.float64)[:, None] * rate
    coarse = np.arange(16, dtype=np.float64)[:, None] * OWN * rate
    return (np.stack([np.cos(t), np.sin(t)]).astype(np.float32) for t in (fine, coarse))


def solution(mesh):
    def step(x, gain, wq, wk, wv, wo):
        fine, coarse = tables()
        anywhere = pl.BlockSpec(memory_space=pltpu.HBM)
        dma = pltpu.SemaphoreType.DMA
        return pl.pallas_call(
            kernel,
            out_shape=pltpu.VMEM((OWN, D), BF16),
            in_specs=[anywhere] * 8,
            out_specs=pl.BlockSpec(memory_space=pltpu.VMEM),
            scratch_shapes=[
                pltpu.VMEM((D,), BF16),
                pltpu.VMEM((2, OWN, HEAD // 2), F32),
                pltpu.VMEM((2, 16, HEAD // 2), F32),
                pltpu.VMEM((8, OWN, D), BF16),
                pltpu.VMEM((3, 128, D), BF16),
                pltpu.VMEM((3, 16, 128, HEAD), BF16),
                pltpu.VMEM((3, 8, 128, HEAD), BF16),
                pltpu.VMEM((16, 128, D), BF16),
                pltpu.VMEM((2, 8, OWN, HEAD), BF16),
                pltpu.VMEM((2, 8, HEAD, OWN), BF16),
                pltpu.VMEM((10, OWN, HEAD), BF16),
                pltpu.VMEM((OWN, D), BF16),
                pltpu.VMEM((10, 1, OWN), F32),
                pltpu.VMEM((10, HEAD + SUM, OWN), F32),
                pltpu.VMEM((2, 2, HEAD, OWN), BF16),
                pltpu.VMEM((2, 2, 2, OWN), F32),
                pltpu.VMEM((OWN, HEAD), BF16),
                dma((8,)),
                dma((2,)), dma((8,)), dma(()), dma((8,)),
                dma(()), dma((4, 2)), dma((4,)),
                dma(()), dma((8,)), dma((2,)), dma((4,)),
                dma(()), dma((8, 2)), dma(()), dma((4,)), dma(()), dma(()),
                dma(()), dma(()), dma((2,)), dma((2,)),
            ],
            compiler_params=pltpu.CompilerParams(collective_id=0, has_side_effects=True, vmem_limit_bytes=61 * 2**20),
            name="decoder_attention",
        )(x, gain, wq, wk, wv, wo, jnp.asarray(fine), jnp.asarray(coarse))

    tokens, whole = P(("dp", "sp"), None), P("sp", None)
    return jax.shard_map(
        step,
        mesh=mesh,
        in_specs=(tokens, P(None), whole, whole, whole, whole),
        out_specs=tokens,
        check_vma=False,
    )
```

```python
import functools

import jax
import jax.numpy as jnp
import numpy as np
from jax import lax
from jax.experimental import pallas as pl
from jax.experimental.pallas import tpu as pltpu
from jax.sharding import PartitionSpec as P

NEG = -1e30
HIDDEN = 2 * NEG
LOG2E = 1.4426950408889634
HEAD = 256
THETA = 10000
D = 2048
OWN = 512
HALF = 256
SUM = 8
F32, BF16 = jnp.float32, jnp.bfloat16
MESH = pl.DeviceIdType.MESH


def _dot(a, b, ca, cb):
    return lax.dot_general(a, b, (((ca,), (cb,)), ((), ())), preferred_element_type=F32)


def kernel(x_h, gain_h, wq_h, wk_h, wv_h, wo_h, fine_h, coarse_h, y_ref,
           gain_ref, fine_ref, coarse_ref, av, wi, wf, ws, wov, kv_k, kv_v, qv, og, top_s, mix_s, part, part_f, orl,
           ld, w_s, wf_r, wfc_r, ws_r, a_s, a_r, ac_r, wo_s, wo_r, wod_r, woc_r, kv_s, kv_r, o_s, o_r, orl_s, orl_r, q_s, q_r, part_s, part_r):
    me = lax.axis_index("sp")
    x, y, z, c, p = me // 8, (me // 4) % 2, (me // 2) % 2, me % 2, me // 4
    X, Y, Z, C = me + 8 - 16 * x, me + 4 - 8 * y, me + 2 - 4 * z, me + 1 - 2 * c
    Dg = X + Y - me
    pX, pY, pD = X // 4, Y // 4, Dg // 4
    oc, oz = 1 - c, 1 - z
    head = 2 * p + c
    mine = 2 * p + c
    planes = (p, pX, pY, pD)

    def row(q, zz, cc):
        return 4 * q + 2 * zz + cc

    def rc(src, dst, ssem, rsem, dev):
        return pltpu.make_async_remote_copy(src_ref=src, dst_ref=dst, send_sem=ssem, recv_sem=rsem, device_id={"sp": dev}, device_id_type=MESH)

    def got(ref, sem, name="wait"):
        with jax.named_scope(name):
            pltpu.make_async_copy(ref, ref, sem).wait()

    def local(src, dst, n):
        cp = pltpu.make_async_copy(src, dst, ld.at[n])
        cp.start()
        return cp

    loads = (wk_h, wv_h, wq_h)
    for n, w in enumerate(loads):
        local(w, wi.at[n], 0)
    here = pl.ds(pl.multiple_of(head * HEAD, HEAD), HEAD)
    other = pl.ds(pl.multiple_of((2 * p + oc) * HEAD, HEAD), HEAD)
    sme = 2 * p + z
    load_x = local(x_h, y_ref, 1)
    load_gain = local(gain_h, gain_ref, 2)
    load_tables = (local(fine_h, fine_ref, 3), local(coarse_h, coarse_ref, 4))
    load_wo = local(wo_h, wov.at[me], 5)
    for n, w in enumerate(loads):
        local(w.at[:, here], wf.at[n, me], 6)
        local(w.at[:, other], ws.at[n, sme], 7)

    barrier = pltpu.get_barrier_semaphore()
    partners = (X, Y, Dg, X + C - me, Y + C - me, Dg + C - me, C, Z)
    for dev in partners:
        pl.semaphore_signal(barrier, inc=1, device_id={"sp": dev}, device_id_type=MESH)
    with jax.named_scope("barrier"):
        pl.semaphore_wait(barrier, len(partners))

    def send(src, dst, ssem, rsem, dev):
        rc(src, dst, ssem, rsem, dev).start()

    got(wi, ld.at[0], "load")
    for dev, q in ((X, pX), (Y, pY), (Dg, pD)):
        for hd, dst, rs in ((2 * q + c, wf.at[:, me], wf_r.at[sme]), (2 * q + oc, ws.at[:, sme], ws_r.at[sme])):
            cols = pl.ds(pl.multiple_of(hd * HEAD, HEAD), HEAD)
            send(wi.at[:, :, cols], dst, w_s.at[1], rs, dev)

    def wf_on(q, zz):
        i = row(q, zz, c)
        send(wf.at[:, i], wf.at[:, i], w_s.at[0], wf_r.at[2 * q + zz], Z)

    def ws_on(q, zz, on):
        i, s = row(q, zz, c), 2 * q + zz
        if on:
            send(ws.at[:, s], ws.at[:, s], w_s.at[0], ws_r.at[s], Z)
        send(ws.at[:, s], wf.at[:, i], w_s.at[0], wfc_r, C)

    def got_wf(n, q, zz):
        got(wf.at[:, row(q, zz, c)], wf_r.at[2 * q + zz], f"wf{n}")

    def got_ws(n, q, zz):
        got(ws.at[:, 2 * q + zz], ws_r.at[2 * q + zz], f"ws{n}")

    got(wf.at[:, me], ld.at[6])
    got(ws.at[:, sme], ld.at[7])
    wf_on(p, z)
    ws_on(p, z, True)

    load_x.wait()
    load_gain.wait()

    @jax.named_scope("norm")
    def norm(n, _):
        rows = pl.ds(pl.multiple_of(n * 128, 128), 128)
        wide = y_ref[rows, :].astype(F32)
        scale = lax.rsqrt(jnp.mean(wide * wide, -1, keepdims=True) + 1e-6)
        av[mine, rows, :] = (wide * scale * gain_ref[...].reshape(1, D).astype(F32)).astype(BF16)

    lax.fori_loop(0, OWN // 128, norm, None)

    def half_rows(half):
        return pl.ds(half * HALF if isinstance(half, int) else pl.multiple_of(half * HALF, HALF), HALF)

    def send_a(b, half, place, dev):
        rows = half_rows(half)
        send(av.at[b, rows], av.at[b, rows], a_s, a_r.at[place, half], dev)

    def give_a(b, half, n):
        rows = half_rows(half)
        send(av.at[b, rows], av.at[b, rows], a_s, ac_r.at[n], C)

    def got_a(b, half, place):
        got(av.at[b, half_rows(half)], a_r.at[place, half], f"a{half}")

    def got_given(n):
        got(av.at[0], ac_r.at[n], "given")

    send_a(mine, 0, 1, X)
    send_a(mine, 1, 2, Y)
    send_a(mine, 1, 1, X)
    send_a(mine, 0, 2, Y)
    give_a(mine, 0, 0)
    give_a(mine, 1, 0)

    for n, q in ((1, pX), (2, pY)):
        got_wf(n, q, z)
        wf_on(q, z)
    for n, q in ((1, pX), (2, pY)):
        got_ws(n, q, z)
        ws_on(q, z, True)
    got_wf(3, pD, z)
    wf_on(pD, z)
    got_ws(3, pD, z)
    ws_on(pD, z, True)
    load_wo.wait()
    send(wov.at[me], wov.at[me], wo_s, wo_r.at[sme], Z)

    for n, q in enumerate(planes):
        got_wf(n, q, oz)
        got_ws(n, q, oz)
        ws_on(q, oz, False)
    got(wf.at[:, pl.ds(0, 8)], wfc_r, "wfc")

    @jax.named_scope("project")
    def project(b, half):
        rows = half_rows(half)
        a = av[b, rows, :]
        i = 4 * (b // 2) + 2 * z + b % 2
        cb, sb = coarse_ref[0, pl.ds(i, 1), :], coarse_ref[1, pl.ds(i, 1), :]
        cf, sf = fine_ref[0, rows, :], fine_ref[1, rows, :]
        cos = cb * cf - sb * sf
        sin = sb * cf + cb * sf

        def turned(t):
            t = t.astype(BF16).astype(F32)
            u, v = t[:, : HEAD // 2], t[:, HEAD // 2 :]
            return jnp.concatenate([u * cos - v * sin, v * cos + u * sin], -1).astype(BF16)

        kv_k[z, b, rows, :] = turned(_dot(a, wf[0].reshape(D, HEAD), 1, 0))
        kv_v[z, b, :, rows] = _dot(a, wf[1].reshape(D, HEAD), 1, 0).astype(BF16).T
        qv[b, rows, :] = turned(_dot(a, wf[2].reshape(D, HEAD), 1, 0))

    def kv_copies(b, half):
        rows = half_rows(half)
        return (rc(kv_k.at[z, b, rows, :], kv_k.at[z, b, rows, :], kv_s, kv_r.at[b, half], Z),
                rc(kv_v.at[z, b, :, rows], kv_v.at[z, b, :, rows], kv_s, kv_r.at[b, half], Z))

    def q_copy(b, half):
        rows = half_rows(half)
        return rc(qv.at[b, rows, :], qv.at[b + 2, rows, :], q_s, q_r, Z)

    def send_kv(b, half):
        for cp in kv_copies(b, half):
            cp.start()

    def on(b, half):
        @pl.when(b < 6)
        def _():
            send_kv(b, half)

        @pl.when((b >= 6) & (z == 1))
        def _():
            q_copy(b, half).start()

    def core(n):
        return c + n * (oc - c)

    def own_piece(q):
        def body(n, _):
            b, half = 2 * q + core(n // 2), n % 2
            project(b, half)
            on(b, half)

        lax.fori_loop(0, 4, body, None)

    def side_half(t, n):
        isy = n % 2 if t == 0 else 1 - n // 2
        return 2 * (pX + isy * (pY - pX)) + core(n // 2 if t == 0 else n % 2), (isy + t) % 2

    hold = (p == 0) & (z == 1)
    hold_y = p == 3

    def side_pieces(t):
        def body(n, _):
            b, half = side_half(t, n)
            project(b, half)
            if t == 0:
                on(b, half)
            else:
                @pl.when(jnp.logical_not(hold | (hold_y & (n < 2))))
                def _():
                    on(b, half)

        lax.fori_loop(0, 4, body, None)

    for cp in load_tables:
        cp.wait()
    got_given(0)
    own_piece(p)

    bX, bY, bD = 2 * pX + c, 2 * pY + c, 2 * pD + c
    got_a(bX, 0, 1)
    send_a(bX, 0, 3, Y)
    give_a(bX, 0, 1)
    got_a(bY, 1, 2)
    send_a(bY, 1, 3, X)
    give_a(bY, 1, 1)
    got_given(1)
    side_pieces(0)

    iz = row(p, oz, c)

    def give_wo(i, place):
        send(wov.at[i], wov.at[i], wo_s, woc_r.at[place], C)

    got(wov.at[iz], wo_r.at[2 * p + oz], "wo_z")
    for i, zz in ((me, z), (iz, oz)):
        for dev in (X, Y):
            send(wov.at[i], wov.at[i], wo_s, wo_r.at[2 * p + zz], dev)
        give_wo(i, 0)

    e = HEAD**-0.5 * LOG2E
    top_s[...] = jnp.full(top_s.shape, NEG, F32)
    mix_s[...] = jnp.zeros(mix_s.shape, F32)

    def tile(zz, kb, bq, masked, rows):
        s = _dot(kv_k[zz, kb, rows, :], qv[bq], 1, 1)
        if masked:
            ok = lax.broadcasted_iota(jnp.int32, s.shape, 1) >= lax.broadcasted_iota(jnp.int32, s.shape, 0)
            s = jnp.where(ok, s, HIDDEN)
        return s

    every = pl.ds(0, OWN)

    def attend(work, rows=every):
        scores = [[tile(zz, kb, bq, masked, rows) for zz, kb, masked in keys] for bq, keys in work]
        for (bq, keys), ss in zip(work, scores):
            old = top_s[bq]
            top = old
            for s in ss:
                top = jnp.maximum(top, s.max(axis=0, keepdims=True))
            top_s[bq] = top
            keep = jnp.exp2((old - top) * e)
            total = mix_s[bq] * keep
            for (zz, kb, _), s in zip(keys, ss):
                w = jnp.exp2((s - top) * e).astype(BF16)
                total = total + _dot(jnp.concatenate([kv_v[zz, kb, :, rows], jnp.ones((SUM, rows.size), BF16)], axis=0), w, 1, 0)
            mix_s[bq] = total

    @jax.named_scope("pair")
    def pair(zz, kp, qp):
        keys = [(zz, 2 * kp, False), (zz, 2 * kp + 1, False)]
        attend([(2 * qp, keys), (2 * qp + 1, keys)])

    @jax.named_scope("diagonal")
    def diagonal(kp):
        attend([(2 * kp, [(z, 2 * kp, True)]), (2 * kp + 1, [(z, 2 * kp, False), (z, 2 * kp + 1, True)])])

    diagonal(p)

    got_a(bX, 1, 1)
    give_a(bX, 1, 2)
    got_a(bY, 0, 2)
    give_a(bY, 0, 2)
    got_given(2)
    side_pieces(1)
    even = 1 - (x + y) % 2

    def near(n, _):
        @pl.when(n > 0)
        def _():
            diagonal(pX * (n == 1) + pY * (n == 2))

        low = y * (n == 0) + 2 * x * (n == 1) + even * (n == 2)
        high = (y + 2) * (n == 0) + (2 * x + 1) * (n == 1) + (3 - even) * (n == 2)
        pair(z, low, high)

    lax.fori_loop(0, 3, near, None)

    def part_copies():
        return (rc(part.at[0], part.at[1], part_s.at[0], part_r.at[0], Z), rc(part_f.at[0], part_f.at[1], part_s.at[1], part_r.at[1], Z))

    def send_part():
        got(qv.at[pl.ds(8, 2)], q_r, "q")
        pair(z, 3, 4)
        for n in (0, 1):
            mix = mix_s[8 + n]
            total = mix[HEAD : HEAD + 1]
            part[0, n] = (mix[:HEAD] * (1 / total)).astype(BF16)
            part_f[0, n] = jnp.concatenate([top_s[8 + n], total], axis=0)
        for cp in part_copies():
            cp.start()

    @pl.when((z == 0) & (p == 3))
    def _():
        send_part()

    def got_kv(b, half):
        got(kv_k.at[oz, b], kv_r.at[b, half], "kv")

    def got_piece(kp):
        for n in (0, 1):
            for half in (0, 1):
                got_kv(2 * kp + n, half)

    def near_remote(n, _):
        qp = p * (n == 0) + pX * (n == 1) + pY * (n == 2)
        pl.when(qp >= p + oz)(lambda: pair(oz, p, qp))

    @pl.when(p < 3)
    def _():
        got_piece(p)
        lax.fori_loop(0, 3, near_remote, None)

    for half in (0, 1):
        got_a(bD, half, 3)
        give_a(bD, half, 3)
    got_given(3)
    own_piece(pD)

    @pl.when(hold)
    def _():
        for n in range(4):
            send_kv(*side_half(1, n))

    @pl.when(hold_y)
    def _():
        for n in range(2):
            send_kv(*side_half(1, n))

    diagonal(pD)

    def far(n, _):
        low = (1 - even) * (n == 0) + 2 * (1 - x) * (n == 1) + (1 - y) * (n == 2)
        high = (2 + even) * (n == 0) + (3 - 2 * x) * (n == 1) + (3 - y) * (n == 2)
        pair(z, low, high)

    lax.fori_loop(0, 3, far, None)

    iX, iY, iD = row(pX, z, c), row(pY, z, c), row(pD, z, c)
    for n, (i, q, dev) in enumerate(((iX, pX, Y), (iY, pY, X))):
        got(wov.at[i], wo_r.at[2 * q + z], f"wo{n}")
        rows = pl.ds(n * 64, 64)
        send(wov.at[i, rows], wov.at[i, rows], wo_s, wod_r.at[n], dev)
        give_wo(i, 1 + n)

    def wo_rest():
        for n in (0, 1):
            got(wov.at[iD, pl.ds(n * 64, 64)], wod_r.at[n], f"wod{n}")
        send(wov.at[iD], wov.at[iD], wo_s, wo_r.at[2 * pD + z], Z)
        give_wo(iD, 3)
        for n, q in enumerate((pX, pY)):
            i = row(q, oz, c)
            got(wov.at[i], wo_r.at[2 * q + oz], f"wo_oz{n}")
            give_wo(i, 1 + n)

    cols = pl.ds(pl.multiple_of(head * HEAD, HEAD), HEAD)

    def o_copy(b):
        place = 2 * ((b // 2 % 2 + y) % 2) + (b // 4 + x) % 2
        return rc(qv.at[b], og.at[:, cols], o_s, o_r.at[place], row(b // 2, z, b % 2))

    by_y = 2 * pD + 1

    def finish(n, _):
        b = n + 1 - 2 * (n % 2)
        with jax.named_scope("finish"):
            mix = mix_s[b]
            qv[b] = (mix[:HEAD] * (1 / mix[HEAD : HEAD + 1])).T.astype(BF16)

        @pl.when((b != mine) & (b != by_y))
        def _():
            o_copy(b).start()

        @pl.when(b == by_y)
        def _():
            send(qv.at[b], orl, o_s, orl_r, Y)

    def finish_pieces(first, last):
        lax.fori_loop(2 * first, 2 * last, finish, None)

    first, last = (3 - p) // 3, p // 3
    kp0, kp1 = p - 2 * last, first
    done0, done1 = first, 2 - p // 2 * (3 - p)

    def remote_piece(kp, done):
        got_piece(kp)

        def body(qp, _):
            pair(oz, kp, qp)
            pl.when(qp < done)(lambda: finish_pieces(qp, qp + 1))

        lax.fori_loop(kp + oz, 4, body, None)

    def remote_blocks(kp, done):
        for n in (0, 1):
            block = 2 * kp + core(n)
            got_kv(block, 0)
            got_kv(block, 1)

            def body(qp, _):
                with jax.named_scope("one"):
                    attend([(2 * qp + m, [(oz, block, False)]) for m in (0, 1)])
                if n:
                    pl.when(qp < done)(lambda: finish_pieces(qp, qp + 1))

            lax.fori_loop(kp + oz, 4, body, None)

    def last_piece(kp):
        block = 2 * kp + core(0)
        got_kv(block, 0)
        got_kv(block, 1)

        def piece(n):
            return z * (kp + oz + n) + oz * (3 - n)

        def first(n, _):
            with jax.named_scope("one"):
                attend([(2 * piece(n) + m, [(oz, block, False)]) for m in (0, 1)])

        lax.fori_loop(0, 4 - kp - oz, first, None)
        wo_rest()
        block2 = 2 * kp + core(1)
        for k in (0, 1):
            half = k + last * (1 - 2 * k)
            got_kv(block2, half)

            def second(n, _):
                qp = piece(n)
                with jax.named_scope("half"):
                    attend([(2 * qp + m, [(oz, block2, False)]) for m in (0, 1)], half_rows(half))
                if k:
                    @pl.when((qp < 3) | (z == 0))
                    def _():
                        finish_pieces(qp, qp + 1)

            lax.fori_loop(0, 4 - kp - oz, second, None)

    finish_pieces(0, oz)

    @pl.when(last == 0)
    def _():
        pl.when(pD >= p + oz)(lambda: pair(oz, p, pD))
        finish_pieces(oz, done0 + oz)

    @pl.when(last == 1)
    def _():
        remote_piece(kp0, 0)

    @pl.when((z == 0) & (p < 3))
    def _():
        send_part()


    @pl.when(last == 0)
    def _():
        remote_piece(kp1, done1 + oz)

    @pl.when(last == 1)
    def _():
        remote_blocks(kp1, done1 + oz)

    last_piece(3 - kp0 - kp1)

    @pl.when(z == 1)
    def _():
        got(qv.at[pl.ds(0, 2)], q_s, "q_left")
        got(part.at[1], part_r.at[0], "part")
        got(part_f.at[1], part_r.at[1], "part")
        for n in (0, 1):
            old, came, count = top_s[6 + n], part_f[1, n, 0:1], part_f[1, n, 1:2]
            top = jnp.maximum(old, came)
            keep, add = jnp.exp2((old - top) * e), jnp.exp2((came - top) * e) * count
            mix = mix_s[6 + n]
            more = jnp.concatenate([part[1, n].astype(F32) * add, jnp.broadcast_to(add, (SUM, OWN))], axis=0)
            mix_s[6 + n] = mix * keep + more

        finish_pieces(3, 4)

    og[:, cols] = qv[mine]
    def relay():
        from_y = pl.ds(pl.multiple_of((2 * pY + c) * HEAD, HEAD), HEAD)
        return rc(orl, og.at[:, from_y], orl_s, o_r.at[3], row(pX, z, 1))

    def heads(q):
        return pl.ds(pl.multiple_of(q * 2 * HEAD, 2 * HEAD), 2 * HEAD)

    def ready(k):
        got(wov.at[pl.ds(0, 2)], woc_r.at[k], "wo_c")
        got(og.at[:, heads(planes[k])] if k else qv.at[0], o_r.at[k], f"og{k}")

    for ks in ((0,), (1,), (2, 3)):
        if ks == (1,):
            got(orl, orl_r, "relay")
            relay().start()
            i = row(pD, oz, c)
            got(wov.at[i], wo_r.at[2 * pD + oz], "wo_dz")
            give_wo(i, 3)
        for k in ks:
            ready(k)

        def out(n, _):
            cols = pl.ds(pl.multiple_of(n * 512, 512), 512)
            with jax.named_scope("out"):
                t = sum(_dot(og[:, heads(planes[k])], wov[pl.ds(4 * planes[k], 4), :, cols].reshape(2 * HEAD, 512), 1, 0) for k in ks)
                for m in range(2):
                    rows = pl.ds(m * HEAD, HEAD)
                    u = t[m * HEAD : (m + 1) * HEAD]
                    if ks != (0,):
                        u = mix_s[2 * n + m, :HEAD, :] + u
                    if 3 in ks:
                        y_ref[rows, cols] = (y_ref[rows, cols].astype(F32) + u).astype(BF16)
                    else:
                        mix_s[2 * n + m, :HEAD, :] = u

        lax.fori_loop(0, D // 512, out, None)

    got(wf, w_s.at[0])
    got(ws.at[:, pl.ds(0, 6)], w_s.at[1])
    got(av.at[pl.ds(0, 7)], a_s)
    got(wov.at[pl.ds(0, 15)], wo_s)
    got(kv_k.at[:, pl.ds(0, 6)], kv_s)
    got(qv.at[pl.ds(0, 7)], o_s)
    relay().wait_send()

    @pl.when(z == 0)
    def _():
        for cp in part_copies():
            cp.wait_send()


def tables():
    half = HEAD // 2
    rate = (THETA ** (-np.arange(half, dtype=np.float64) / half))[None]
    fine = np.arange(OWN, dtype=np.float64)[:, None] * rate
    coarse = np.arange(16, dtype=np.float64)[:, None] * OWN * rate
    return (np.stack([np.cos(t), np.sin(t)]).astype(np.float32) for t in (fine, coarse))


def solution(mesh):
    def step(x, gain, wq, wk, wv, wo):
        fine, coarse = tables()
        anywhere = pl.BlockSpec(memory_space=pltpu.HBM)
        dma = pltpu.SemaphoreType.DMA
        return pl.pallas_call(
            kernel,
            out_shape=pltpu.VMEM((OWN, D), BF16),
            in_specs=[anywhere] * 8,
            out_specs=pl.BlockSpec(memory_space=pltpu.VMEM),
            scratch_shapes=[
                pltpu.VMEM((D,), BF16),
                pltpu.VMEM((2, OWN, HEAD // 2), F32),
                pltpu.VMEM((2, 16, HEAD // 2), F32),
                pltpu.VMEM((8, OWN, D), BF16),
                pltpu.VMEM((3, 128, D), BF16),
                pltpu.VMEM((3, 16, 128, HEAD), BF16),
                pltpu.VMEM((3, 8, 128, HEAD), BF16),
                pltpu.VMEM((16, 128, D), BF16),
                pltpu.VMEM((2, 8, OWN, HEAD), BF16),
                pltpu.VMEM((2, 8, HEAD, OWN), BF16),
                pltpu.VMEM((10, OWN, HEAD), BF16),
                pltpu.VMEM((OWN, D), BF16),
                pltpu.VMEM((10, 1, OWN), F32),
                pltpu.VMEM((10, HEAD + SUM, OWN), F32),
                pltpu.VMEM((2, 2, HEAD, OWN), BF16),
                pltpu.VMEM((2, 2, 2, OWN), F32),
                pltpu.VMEM((OWN, HEAD), BF16),
                dma((8,)),
                dma((2,)), dma((8,)), dma(()), dma((8,)),
                dma(()), dma((4, 2)), dma((4,)),
                dma(()), dma((8,)), dma((2,)), dma((4,)),
                dma(()), dma((8, 2)), dma(()), dma((4,)), dma(()), dma(()),
                dma(()), dma(()), dma((2,)), dma((2,)),
            ],
            compiler_params=pltpu.CompilerParams(collective_id=0, has_side_effects=True, vmem_limit_bytes=61 * 2**20),
            name="decoder_attention",
        )(x, gain, wq, wk, wv, wo, jnp.asarray(fine), jnp.asarray(coarse))

    tokens, whole = P(("dp", "sp"), None), P("sp", None)
    return jax.shard_map(
        step,
        mesh=mesh,
        in_specs=(tokens, P(None), whole, whole, whole, whole),
        out_specs=tokens,
        check_vma=False,
    )
```

```python
import functools

import jax
import jax.numpy as jnp
import numpy as np
from jax import lax
from jax.experimental import pallas as pl
from jax.experimental.pallas import tpu as pltpu
from jax.sharding import PartitionSpec as P

NEG = -1e30
HIDDEN = 2 * NEG
LOG2E = 1.4426950408889634
HEAD = 256
THETA = 10000
D = 2048
OWN = 512
HALF = 256
SUM = 8
F32, BF16 = jnp.float32, jnp.bfloat16
MESH = pl.DeviceIdType.MESH


def _dot(a, b, ca, cb):
    return lax.dot_general(a, b, (((ca,), (cb,)), ((), ())), preferred_element_type=F32)


def kernel(x_h, gain_h, wq_h, wk_h, wv_h, wo_h, fine_h, coarse_h, y_ref,
           gain_ref, fine_ref, coarse_ref, av, wi, wf, ws, wov, kv_k, kv_v, qv, og, top_s, mix_s, part, part_f, orl,
           ld, w_s, wf_r, wfc_r, ws_r, a_s, a_r, ac_r, wo_s, wo_r, wod_r, woc_r, kv_s, kv_r, o_s, o_r, orl_s, orl_r, q_s, q_r, part_s, part_r):
    me = lax.axis_index("sp")
    x, y, z, c, p = me // 8, (me // 4) % 2, (me // 2) % 2, me % 2, me // 4
    X, Y, Z, C = me + 8 - 16 * x, me + 4 - 8 * y, me + 2 - 4 * z, me + 1 - 2 * c
    Dg = X + Y - me
    pX, pY, pD = X // 4, Y // 4, Dg // 4
    oc, oz = 1 - c, 1 - z
    head = 2 * p + c
    mine = 2 * p + c
    planes = (p, pX, pY, pD)

    def row(q, zz, cc):
        return 4 * q + 2 * zz + cc

    def rc(src, dst, ssem, rsem, dev):
        return pltpu.make_async_remote_copy(src_ref=src, dst_ref=dst, send_sem=ssem, recv_sem=rsem, device_id={"sp": dev}, device_id_type=MESH)

    def got(ref, sem, name="wait"):
        with jax.named_scope(name):
            pltpu.make_async_copy(ref, ref, sem).wait()

    def local(src, dst, n):
        cp = pltpu.make_async_copy(src, dst, ld.at[n])
        cp.start()
        return cp

    loads = (wk_h, wv_h, wq_h)
    for n, w in enumerate(loads):
        local(w, wi.at[n], 0)
    here = pl.ds(pl.multiple_of(head * HEAD, HEAD), HEAD)
    other = pl.ds(pl.multiple_of((2 * p + oc) * HEAD, HEAD), HEAD)
    sme = 2 * p + z
    load_x = local(x_h, y_ref, 1)
    load_gain = local(gain_h, gain_ref, 2)
    load_tables = (local(fine_h, fine_ref, 3), local(coarse_h, coarse_ref, 4))
    load_wo = local(wo_h, wov.at[me], 5)
    for n, w in enumerate(loads):
        local(w.at[:, here], wf.at[n, me], 6)
        local(w.at[:, other], ws.at[n, sme], 7)

    barrier = pltpu.get_barrier_semaphore()
    partners = (X, Y, Dg, X + C - me, Y + C - me, Dg + C - me, C, Z)
    for dev in partners:
        pl.semaphore_signal(barrier, inc=1, device_id={"sp": dev}, device_id_type=MESH)
    with jax.named_scope("barrier"):
        pl.semaphore_wait(barrier, len(partners))

    def send(src, dst, ssem, rsem, dev):
        rc(src, dst, ssem, rsem, dev).start()

    got(wi, ld.at[0], "load")
    for dev, q in ((X, pX), (Y, pY), (Dg, pD)):
        for hd, dst, rs in ((2 * q + c, wf.at[:, me], wf_r.at[sme]), (2 * q + oc, ws.at[:, sme], ws_r.at[sme])):
            cols = pl.ds(pl.multiple_of(hd * HEAD, HEAD), HEAD)
            send(wi.at[:, :, cols], dst, w_s.at[1], rs, dev)

    def wf_on(q, zz):
        i = row(q, zz, c)
        send(wf.at[:, i], wf.at[:, i], w_s.at[0], wf_r.at[2 * q + zz], Z)

    def ws_on(q, zz, on):
        i, s = row(q, zz, c), 2 * q + zz
        if on:
            send(ws.at[:, s], ws.at[:, s], w_s.at[0], ws_r.at[s], Z)
        send(ws.at[:, s], wf.at[:, i], w_s.at[0], wfc_r, C)

    def got_wf(n, q, zz):
        got(wf.at[:, row(q, zz, c)], wf_r.at[2 * q + zz], f"wf{n}")

    def got_ws(n, q, zz):
        got(ws.at[:, 2 * q + zz], ws_r.at[2 * q + zz], f"ws{n}")

    got(wf.at[:, me], ld.at[6])
    got(ws.at[:, sme], ld.at[7])
    wf_on(p, z)
    ws_on(p, z, True)

    load_x.wait()
    load_gain.wait()

    @jax.named_scope("norm")
    def norm(n, _):
        rows = pl.ds(pl.multiple_of(n * 128, 128), 128)
        wide = y_ref[rows, :].astype(F32)
        scale = lax.rsqrt(jnp.mean(wide * wide, -1, keepdims=True) + 1e-6)
        av[mine, rows, :] = (wide * scale * gain_ref[...].reshape(1, D).astype(F32)).astype(BF16)

    lax.fori_loop(0, OWN // 128, norm, None)

    def half_rows(half):
        return pl.ds(half * HALF if isinstance(half, int) else pl.multiple_of(half * HALF, HALF), HALF)

    def send_a(b, half, place, dev):
        rows = half_rows(half)
        send(av.at[b, rows], av.at[b, rows], a_s, a_r.at[place, half], dev)

    def give_a(b, half, n):
        rows = half_rows(half)
        send(av.at[b, rows], av.at[b, rows], a_s, ac_r.at[n], C)

    def got_a(b, half, place):
        got(av.at[b, half_rows(half)], a_r.at[place, half], f"a{half}")

    def got_given(n):
        got(av.at[0], ac_r.at[n], "given")

    send_a(mine, 0, 1, X)
    send_a(mine, 1, 2, Y)
    send_a(mine, 1, 1, X)
    send_a(mine, 0, 2, Y)
    give_a(mine, 0, 0)
    give_a(mine, 1, 0)

    for n, q in ((1, pX), (2, pY)):
        got_wf(n, q, z)
        wf_on(q, z)
    for n, q in ((1, pX), (2, pY)):
        got_ws(n, q, z)
        ws_on(q, z, True)
    got_wf(3, pD, z)
    wf_on(pD, z)
    got_ws(3, pD, z)
    ws_on(pD, z, True)
    load_wo.wait()
    send(wov.at[me], wov.at[me], wo_s, wo_r.at[sme], Z)

    for n, q in enumerate(planes):
        got_wf(n, q, oz)
        got_ws(n, q, oz)
        ws_on(q, oz, False)
    got(wf.at[:, pl.ds(0, 8)], wfc_r, "wfc")

    @jax.named_scope("project")
    def project(b, half):
        rows = half_rows(half)
        a = av[b, rows, :]
        i = 4 * (b // 2) + 2 * z + b % 2
        cb, sb = coarse_ref[0, pl.ds(i, 1), :], coarse_ref[1, pl.ds(i, 1), :]
        cf, sf = fine_ref[0, rows, :], fine_ref[1, rows, :]
        cos = cb * cf - sb * sf
        sin = sb * cf + cb * sf

        def turned(t):
            t = t.astype(BF16).astype(F32)
            u, v = t[:, : HEAD // 2], t[:, HEAD // 2 :]
            return jnp.concatenate([u * cos - v * sin, v * cos + u * sin], -1).astype(BF16)

        kv_k[z, b, rows, :] = turned(_dot(a, wf[0].reshape(D, HEAD), 1, 0))
        kv_v[z, b, :, rows] = _dot(a, wf[1].reshape(D, HEAD), 1, 0).astype(BF16).T
        qv[b, rows, :] = turned(_dot(a, wf[2].reshape(D, HEAD), 1, 0))

    def kv_copies(b, half):
        rows = half_rows(half)
        return (rc(kv_k.at[z, b, rows, :], kv_k.at[z, b, rows, :], kv_s, kv_r.at[b, half], Z),
                rc(kv_v.at[z, b, :, rows], kv_v.at[z, b, :, rows], kv_s, kv_r.at[b, half], Z))

    def q_copy(b, half):
        rows = half_rows(half)
        return rc(qv.at[b, rows, :], qv.at[b + 2, rows, :], q_s, q_r, Z)

    def send_kv(b, half):
        for cp in kv_copies(b, half):
            cp.start()

    def on(b, half):
        @pl.when(b < 6)
        def _():
            send_kv(b, half)

        @pl.when((b >= 6) & (z == 1))
        def _():
            q_copy(b, half).start()

    def core(n):
        return c + n * (oc - c)

    def own_piece(q):
        def body(n, _):
            b, half = 2 * q + core(n // 2), n % 2
            project(b, half)
            on(b, half)

        lax.fori_loop(0, 4, body, None)

    def side_half(t, n):
        isy = n % 2 if t == 0 else 1 - n // 2
        return 2 * (pX + isy * (pY - pX)) + core(n // 2 if t == 0 else n % 2), (isy + t) % 2

    hold = (p == 0) & (z == 1)
    hold_y = p == 3

    def side_pieces(t):
        def body(n, _):
            b, half = side_half(t, n)
            project(b, half)
            if t == 0:
                on(b, half)
            else:
                @pl.when(jnp.logical_not(hold | (hold_y & (n < 2))))
                def _():
                    on(b, half)

        lax.fori_loop(0, 4, body, None)

    for cp in load_tables:
        cp.wait()
    got_given(0)
    own_piece(p)

    bX, bY, bD = 2 * pX + c, 2 * pY + c, 2 * pD + c
    got_a(bX, 0, 1)
    send_a(bX, 0, 3, Y)
    give_a(bX, 0, 1)
    got_a(bY, 1, 2)
    send_a(bY, 1, 3, X)
    give_a(bY, 1, 1)
    got_given(1)
    side_pieces(0)

    iz = row(p, oz, c)

    def give_wo(i, place):
        send(wov.at[i], wov.at[i], wo_s, woc_r.at[place], C)

    got(wov.at[iz], wo_r.at[2 * p + oz], "wo_z")
    for i, zz in ((me, z), (iz, oz)):
        for dev in (X, Y):
            send(wov.at[i], wov.at[i], wo_s, wo_r.at[2 * p + zz], dev)
        give_wo(i, 0)

    e = HEAD**-0.5 * LOG2E
    top_s[...] = jnp.full(top_s.shape, NEG, F32)
    mix_s[...] = jnp.zeros(mix_s.shape, F32)

    def tile(zz, kb, bq, masked, rows):
        s = _dot(kv_k[zz, kb, rows, :], qv[bq], 1, 1)
        if masked:
            ok = lax.broadcasted_iota(jnp.int32, s.shape, 1) >= lax.broadcasted_iota(jnp.int32, s.shape, 0)
            s = jnp.where(ok, s, HIDDEN)
        return s

    every = pl.ds(0, OWN)

    def attend(work, rows=every):
        scores = [[tile(zz, kb, bq, masked, rows) for zz, kb, masked in keys] for bq, keys in work]
        for (bq, keys), ss in zip(work, scores):
            old = top_s[bq]
            top = old
            for s in ss:
                top = jnp.maximum(top, s.max(axis=0, keepdims=True))
            top_s[bq] = top
            keep = jnp.exp2((old - top) * e)
            total = mix_s[bq] * keep
            for (zz, kb, _), s in zip(keys, ss):
                w = jnp.exp2((s - top) * e).astype(BF16)
                total = total + _dot(jnp.concatenate([kv_v[zz, kb, :, rows], jnp.ones((SUM, rows.size), BF16)], axis=0), w, 1, 0)
            mix_s[bq] = total

    @jax.named_scope("pair")
    def pair(zz, kp, qp):
        keys = [(zz, 2 * kp, False), (zz, 2 * kp + 1, False)]
        attend([(2 * qp, keys), (2 * qp + 1, keys)])

    @jax.named_scope("diagonal")
    def diagonal(kp):
        attend([(2 * kp, [(z, 2 * kp, True)]), (2 * kp + 1, [(z, 2 * kp, False), (z, 2 * kp + 1, True)])])

    diagonal(p)

    got_a(bX, 1, 1)
    give_a(bX, 1, 2)
    got_a(bY, 0, 2)
    give_a(bY, 0, 2)
    got_given(2)
    side_pieces(1)
    even = 1 - (x + y) % 2

    def near(n, _):
        @pl.when(n > 0)
        def _():
            diagonal(pX * (n == 1) + pY * (n == 2))

        low = y * (n == 0) + 2 * x * (n == 1) + even * (n == 2)
        high = (y + 2) * (n == 0) + (2 * x + 1) * (n == 1) + (3 - even) * (n == 2)
        pair(z, low, high)

    lax.fori_loop(0, 3, near, None)

    def part_copies():
        return (rc(part.at[0], part.at[1], part_s.at[0], part_r.at[0], Z), rc(part_f.at[0], part_f.at[1], part_s.at[1], part_r.at[1], Z))

    def send_part():
        got(qv.at[pl.ds(8, 2)], q_r, "q")
        pair(z, 3, 4)
        for n in (0, 1):
            mix = mix_s[8 + n]
            total = mix[HEAD : HEAD + 1]
            part[0, n] = (mix[:HEAD] * (1 / total)).astype(BF16)
            part_f[0, n] = jnp.concatenate([top_s[8 + n], total], axis=0)
        for cp in part_copies():
            cp.start()

    @pl.when((z == 0) & (p == 3))
    def _():
        send_part()

    def got_kv(b, half):
        got(kv_k.at[oz, b], kv_r.at[b, half], "kv")

    def got_piece(kp):
        for n in (0, 1):
            for half in (0, 1):
                got_kv(2 * kp + n, half)

    def near_remote(n, _):
        qp = p * (n == 0) + pX * (n == 1) + pY * (n == 2)
        pl.when(qp >= p + oz)(lambda: pair(oz, p, qp))

    @pl.when(p < 3)
    def _():
        got_piece(p)
        lax.fori_loop(0, 3, near_remote, None)

    for half in (0, 1):
        got_a(bD, half, 3)
        give_a(bD, half, 3)
    got_given(3)
    own_piece(pD)

    @pl.when(hold)
    def _():
        for n in range(4):
            send_kv(*side_half(1, n))

    @pl.when(hold_y)
    def _():
        for n in range(2):
            send_kv(*side_half(1, n))

    diagonal(pD)

    def far(n, _):
        low = (1 - even) * (n == 0) + 2 * (1 - x) * (n == 1) + (1 - y) * (n == 2)
        high = (2 + even) * (n == 0) + (3 - 2 * x) * (n == 1) + (3 - y) * (n == 2)
        pair(z, low, high)

    lax.fori_loop(0, 3, far, None)

    iX, iY, iD = row(pX, z, c), row(pY, z, c), row(pD, z, c)
    for n, (i, q, dev) in enumerate(((iX, pX, Y), (iY, pY, X))):
        got(wov.at[i], wo_r.at[2 * q + z], f"wo{n}")
        rows = pl.ds(n * 64, 64)
        send(wov.at[i, rows], wov.at[i, rows], wo_s, wod_r.at[n], dev)
        give_wo(i, 1 + n)

    def wo_rest():
        for n in (0, 1):
            got(wov.at[iD, pl.ds(n * 64, 64)], wod_r.at[n], f"wod{n}")
        send(wov.at[iD], wov.at[iD], wo_s, wo_r.at[2 * pD + z], Z)
        give_wo(iD, 3)
        for n, q in enumerate((pX, pY)):
            i = row(q, oz, c)
            got(wov.at[i], wo_r.at[2 * q + oz], f"wo_oz{n}")
            give_wo(i, 1 + n)

    cols = pl.ds(pl.multiple_of(head * HEAD, HEAD), HEAD)

    def o_copy(b):
        place = 2 * ((b // 2 % 2 + y) % 2) + (b // 4 + x) % 2
        return rc(qv.at[b], og.at[:, cols], o_s, o_r.at[place], row(b // 2, z, b % 2))

    by_y = 2 * pD + 1

    def finish(n, _):
        b = n + 1 - 2 * (n % 2)
        with jax.named_scope("finish"):
            mix = mix_s[b]
            qv[b] = (mix[:HEAD] * (1 / mix[HEAD : HEAD + 1])).T.astype(BF16)

        @pl.when((b != mine) & (b != by_y))
        def _():
            o_copy(b).start()

        @pl.when(b == by_y)
        def _():
            send(qv.at[b], orl, o_s, orl_r, Y)

    def finish_pieces(first, last):
        lax.fori_loop(2 * first, 2 * last, finish, None)

    first, last = (3 - p) // 3, p // 3
    kp0, kp1 = p - 2 * last, first
    done0, done1 = first, 2 - p // 2 * (3 - p)

    def remote_piece(kp, done):
        got_piece(kp)

        def body(qp, _):
            pair(oz, kp, qp)
            pl.when(qp < done)(lambda: finish_pieces(qp, qp + 1))

        lax.fori_loop(kp + oz, 4, body, None)

    def remote_blocks(kp, done):
        for n in (0, 1):
            block = 2 * kp + core(n)
            got_kv(block, 0)
            got_kv(block, 1)

            def body(qp, _):
                with jax.named_scope("one"):
                    attend([(2 * qp + m, [(oz, block, False)]) for m in (0, 1)])
                if n:
                    pl.when(qp < done)(lambda: finish_pieces(qp, qp + 1))

            lax.fori_loop(kp + oz, 4, body, None)

    def last_piece(kp):
        block = 2 * kp + core(0)
        got_kv(block, 0)
        got_kv(block, 1)

        def piece(n):
            return z * (kp + oz + n) + oz * (3 - n)

        def first(n, _):
            with jax.named_scope("one"):
                attend([(2 * piece(n) + m, [(oz, block, False)]) for m in (0, 1)])

        lax.fori_loop(0, 4 - kp - oz, first, None)
        wo_rest()
        block2 = 2 * kp + core(1)
        for k in (0, 1):
            half = k + last * (1 - 2 * k)
            got_kv(block2, half)

            def second(n, _):
                qp = piece(n)
                with jax.named_scope("half"):
                    attend([(2 * qp + m, [(oz, block2, False)]) for m in (0, 1)], half_rows(half))
                if k:
                    @pl.when((qp < 3) | (z == 0))
                    def _():
                        finish_pieces(qp, qp + 1)

            lax.fori_loop(0, 4 - kp - oz, second, None)

    finish_pieces(0, oz)

    @pl.when(last == 0)
    def _():
        pl.when(pD >= p + oz)(lambda: pair(oz, p, pD))
        finish_pieces(oz, done0 + oz)

    @pl.when(last == 1)
    def _():
        remote_piece(kp0, 0)

    @pl.when((z == 0) & (p < 3))
    def _():
        send_part()


    @pl.when(last == 0)
    def _():
        remote_piece(kp1, done1 + oz)

    @pl.when(last == 1)
    def _():
        remote_blocks(kp1, done1 + oz)

    last_piece(3 - kp0 - kp1)

    @pl.when(z == 1)
    def _():
        got(qv.at[pl.ds(0, 2)], q_s, "q_left")
        got(part.at[1], part_r.at[0], "part")
        got(part_f.at[1], part_r.at[1], "part")
        for n in (0, 1):
            old, came, count = top_s[6 + n], part_f[1, n, 0:1], part_f[1, n, 1:2]
            top = jnp.maximum(old, came)
            keep, add = jnp.exp2((old - top) * e), jnp.exp2((came - top) * e) * count
            mix = mix_s[6 + n]
            more = jnp.concatenate([part[1, n].astype(F32) * add, jnp.broadcast_to(add, (SUM, OWN))], axis=0)
            mix_s[6 + n] = mix * keep + more

        finish_pieces(3, 4)

    og[:, cols] = qv[mine]
    def relay():
        from_y = pl.ds(pl.multiple_of((2 * pY + c) * HEAD, HEAD), HEAD)
        return rc(orl, og.at[:, from_y], orl_s, o_r.at[3], row(pX, z, 1))

    def heads(q):
        return pl.ds(pl.multiple_of(q * 2 * HEAD, 2 * HEAD), 2 * HEAD)

    third, fourth = 3 - c, 2 + c
    for step, (k, q) in enumerate(((0, p), (1, pX), (third, pD + c * (pY - pD)), (fourth, pY + c * (pD - pY)))):
        if step == 1:
            got(orl, orl_r, "relay")
            relay().start()
        if step == 2:
            i = row(pD, oz, c)
            got(wov.at[i], wo_r.at[2 * pD + oz], "wo_dz")
            give_wo(i, 3)
        got(wov.at[pl.ds(0, 2)], woc_r.at[k], "wo_c")
        got(og.at[:, heads(q)] if step else qv.at[0], o_r.at[k], f"og{step}")

        def out(n, _):
            with jax.named_scope("out"):
                for t in (2 * n, 2 * n + 1):
                    cols = pl.ds(pl.multiple_of(t * 512, 512), 512)
                    u = _dot(og[:, heads(q)], wov[pl.ds(4 * q, 4), :, cols].reshape(2 * HEAD, 512), 1, 0)
                    for m in range(2):
                        rows = pl.ds(m * HEAD, HEAD)
                        v = u[m * HEAD : (m + 1) * HEAD]
                        if step:
                            v = mix_s[2 * t + m, :HEAD, :] + v
                        if step < 3:
                            mix_s[2 * t + m, :HEAD, :] = v
                        else:
                            y_ref[rows, cols] = (y_ref[rows, cols].astype(F32) + v).astype(BF16)

        lax.fori_loop(0, D // 1024, out, None)

    got(wf, w_s.at[0])
    got(ws.at[:, pl.ds(0, 6)], w_s.at[1])
    got(av.at[pl.ds(0, 7)], a_s)
    got(wov.at[pl.ds(0, 15)], wo_s)
    got(kv_k.at[:, pl.ds(0, 6)], kv_s)
    got(qv.at[pl.ds(0, 7)], o_s)
    relay().wait_send()

    @pl.when(z == 0)
    def _():
        for cp in part_copies():
            cp.wait_send()


def tables():
    half = HEAD // 2
    rate = (THETA ** (-np.arange(half, dtype=np.float64) / half))[None]
    fine = np.arange(OWN, dtype=np.float64)[:, None] * rate
    coarse = np.arange(16, dtype=np.float64)[:, None] * OWN * rate
    return (np.stack([np.cos(t), np.sin(t)]).astype(np.float32) for t in (fine, coarse))


def solution(mesh):
    def step(x, gain, wq, wk, wv, wo):
        fine, coarse = tables()
        anywhere = pl.BlockSpec(memory_space=pltpu.HBM)
        dma = pltpu.SemaphoreType.DMA
        return pl.pallas_call(
            kernel,
            out_shape=pltpu.VMEM((OWN, D), BF16),
            in_specs=[anywhere] * 8,
            out_specs=pl.BlockSpec(memory_space=pltpu.VMEM),
            scratch_shapes=[
                pltpu.VMEM((D,), BF16),
                pltpu.VMEM((2, OWN, HEAD // 2), F32),
                pltpu.VMEM((2, 16, HEAD // 2), F32),
                pltpu.VMEM((8, OWN, D), BF16),
                pltpu.VMEM((3, 128, D), BF16),
                pltpu.VMEM((3, 16, 128, HEAD), BF16),
                pltpu.VMEM((3, 8, 128, HEAD), BF16),
                pltpu.VMEM((16, 128, D), BF16),
                pltpu.VMEM((2, 8, OWN, HEAD), BF16),
                pltpu.VMEM((2, 8, HEAD, OWN), BF16),
                pltpu.VMEM((10, OWN, HEAD), BF16),
                pltpu.VMEM((OWN, D), BF16),
                pltpu.VMEM((10, 1, OWN), F32),
                pltpu.VMEM((10, HEAD + SUM, OWN), F32),
                pltpu.VMEM((2, 2, HEAD, OWN), BF16),
                pltpu.VMEM((2, 2, 2, OWN), F32),
                pltpu.VMEM((OWN, HEAD), BF16),
                dma((8,)),
                dma((2,)), dma((8,)), dma(()), dma((8,)),
                dma(()), dma((4, 2)), dma((4,)),
                dma(()), dma((8,)), dma((2,)), dma((4,)),
                dma(()), dma((8, 2)), dma(()), dma((4,)), dma(()), dma(()),
                dma(()), dma(()), dma((2,)), dma((2,)),
            ],
            compiler_params=pltpu.CompilerParams(collective_id=0, has_side_effects=True, vmem_limit_bytes=61 * 2**20),
            name="decoder_attention",
        )(x, gain, wq, wk, wv, wo, jnp.asarray(fine), jnp.asarray(coarse))

    tokens, whole = P(("dp", "sp"), None), P("sp", None)
    return jax.shard_map(
        step,
        mesh=mesh,
        in_specs=(tokens, P(None), whole, whole, whole, whole),
        out_specs=tokens,
        check_vma=False,
    )
```

```python
import functools

import jax
import jax.numpy as jnp
import numpy as np
from jax import lax
from jax.experimental import pallas as pl
from jax.experimental.pallas import tpu as pltpu
from jax.sharding import PartitionSpec as P

HIDDEN = -jnp.inf
LOG2E = 1.4426950408889634
HEAD = 256
THETA = 10000
D = 2048
OWN = 512
HALF = 256
SUM = 8
F32, BF16 = jnp.float32, jnp.bfloat16
MESH = pl.DeviceIdType.MESH


def _dot(a, b, ca, cb):
    return lax.dot_general(a, b, (((ca,), (cb,)), ((), ())), preferred_element_type=F32)


def kernel(x_h, gain_h, wq_h, wk_h, wv_h, wo_h, fine_h, coarse_h, y_ref,
           gain_ref, fine_ref, coarse_ref, av, wi, wf, ws, wov, kv_k, kv_v, qv, og, top_s, mix_s, part, part_f, orl,
           ld, w_s, wf_r, wfc_r, ws_r, a_s, a_r, ac_r, wo_s, wo_r, wod_r, woc_r, kv_s, kv_r, o_s, o_r, orl_s, orl_r, q_s, q_r, part_s, part_r):
    me = lax.axis_index("sp")
    x, y, z, c, p = me // 8, (me // 4) % 2, (me // 2) % 2, me % 2, me // 4
    X, Y, Z, C = me + 8 - 16 * x, me + 4 - 8 * y, me + 2 - 4 * z, me + 1 - 2 * c
    Dg = X + Y - me
    pX, pY, pD = X // 4, Y // 4, Dg // 4
    oc, oz = 1 - c, 1 - z
    head = 2 * p + c
    mine = 2 * p + c
    planes = (p, pX, pY, pD)

    def row(q, zz, cc):
        return 4 * q + 2 * zz + cc

    def rc(src, dst, ssem, rsem, dev):
        return pltpu.make_async_remote_copy(src_ref=src, dst_ref=dst, send_sem=ssem, recv_sem=rsem, device_id={"sp": dev}, device_id_type=MESH)

    def got(ref, sem, name="wait"):
        with jax.named_scope(name):
            pltpu.make_async_copy(ref, ref, sem).wait()

    def local(src, dst, n):
        cp = pltpu.make_async_copy(src, dst, ld.at[n])
        cp.start()
        return cp

    loads = (wk_h, wv_h, wq_h)
    for n, w in enumerate(loads):
        local(w, wi.at[n], 0)
    here = pl.ds(pl.multiple_of(head * HEAD, HEAD), HEAD)
    other = pl.ds(pl.multiple_of((2 * p + oc) * HEAD, HEAD), HEAD)
    sme = 2 * p + z
    load_x = local(x_h, y_ref, 1)
    load_gain = local(gain_h, gain_ref, 2)
    load_tables = (local(fine_h, fine_ref, 3), local(coarse_h, coarse_ref, 4))
    load_wo = local(wo_h, wov.at[me], 5)
    for n, w in enumerate(loads):
        local(w.at[:, here], wf.at[n, me], 6)
        local(w.at[:, other], ws.at[n, sme], 7)

    barrier = pltpu.get_barrier_semaphore()
    partners = (X, Y, Dg, X + C - me, Y + C - me, Dg + C - me, C, Z)
    for dev in partners:
        pl.semaphore_signal(barrier, inc=1, device_id={"sp": dev}, device_id_type=MESH)
    with jax.named_scope("barrier"):
        pl.semaphore_wait(barrier, len(partners))

    def send(src, dst, ssem, rsem, dev):
        rc(src, dst, ssem, rsem, dev).start()

    got(wi, ld.at[0], "load")
    for dev, q in ((X, pX), (Y, pY), (Dg, pD)):
        for hd, dst, rs in ((2 * q + c, wf.at[:, me], wf_r.at[sme]), (2 * q + oc, ws.at[:, sme], ws_r.at[sme])):
            cols = pl.ds(pl.multiple_of(hd * HEAD, HEAD), HEAD)
            send(wi.at[:, :, cols], dst, w_s.at[1], rs, dev)

    def wf_on(q, zz):
        i = row(q, zz, c)
        send(wf.at[:, i], wf.at[:, i], w_s.at[0], wf_r.at[2 * q + zz], Z)

    def ws_on(q, zz, on):
        i, s = row(q, zz, c), 2 * q + zz
        if on:
            send(ws.at[:, s], ws.at[:, s], w_s.at[0], ws_r.at[s], Z)
        send(ws.at[:, s], wf.at[:, i], w_s.at[0], wfc_r, C)

    def got_wf(n, q, zz):
        got(wf.at[:, row(q, zz, c)], wf_r.at[2 * q + zz], f"wf{n}")

    def got_ws(n, q, zz):
        got(ws.at[:, 2 * q + zz], ws_r.at[2 * q + zz], f"ws{n}")

    got(wf.at[:, me], ld.at[6])
    got(ws.at[:, sme], ld.at[7])
    wf_on(p, z)
    ws_on(p, z, True)

    load_x.wait()
    load_gain.wait()

    @jax.named_scope("norm")
    def norm(n, _):
        rows = pl.ds(pl.multiple_of(n * 128, 128), 128)
        wide = y_ref[rows, :].astype(F32)
        scale = lax.rsqrt(jnp.mean(wide * wide, -1, keepdims=True) + 1e-6)
        av[mine, rows, :] = (wide * scale * gain_ref[...].reshape(1, D).astype(F32)).astype(BF16)

    lax.fori_loop(0, OWN // 128, norm, None)

    def half_rows(half):
        return pl.ds(half * HALF if isinstance(half, int) else pl.multiple_of(half * HALF, HALF), HALF)

    def send_a(b, half, place, dev):
        rows = half_rows(half)
        send(av.at[b, rows], av.at[b, rows], a_s, a_r.at[place, half], dev)

    def give_a(b, half, n):
        rows = half_rows(half)
        send(av.at[b, rows], av.at[b, rows], a_s, ac_r.at[n], C)

    def got_a(b, half, place):
        got(av.at[b, half_rows(half)], a_r.at[place, half], f"a{half}")

    def got_given(n):
        got(av.at[0], ac_r.at[n], "given")

    send_a(mine, 0, 1, X)
    send_a(mine, 1, 2, Y)
    send_a(mine, 1, 1, X)
    send_a(mine, 0, 2, Y)
    give_a(mine, 0, 0)
    give_a(mine, 1, 0)

    for n, q in ((1, pX), (2, pY)):
        got_wf(n, q, z)
        wf_on(q, z)
    for n, q in ((1, pX), (2, pY)):
        got_ws(n, q, z)
        ws_on(q, z, True)
    got_wf(3, pD, z)
    wf_on(pD, z)
    got_ws(3, pD, z)
    ws_on(pD, z, True)
    load_wo.wait()
    send(wov.at[me], wov.at[me], wo_s, wo_r.at[sme], Z)

    for n, q in enumerate(planes):
        got_wf(n, q, oz)
        got_ws(n, q, oz)
        ws_on(q, oz, False)
    got(wf.at[:, pl.ds(0, 8)], wfc_r, "wfc")

    @jax.named_scope("project")
    def project(b, half):
        rows = half_rows(half)
        a = av[b, rows, :]
        i = 4 * (b // 2) + 2 * z + b % 2
        cb, sb = coarse_ref[0, pl.ds(i, 1), :], coarse_ref[1, pl.ds(i, 1), :]
        cf, sf = fine_ref[0, rows, :], fine_ref[1, rows, :]
        cos = cb * cf - sb * sf
        sin = sb * cf + cb * sf

        def turned(t):
            t = t.astype(BF16).astype(F32)
            u, v = t[:, : HEAD // 2], t[:, HEAD // 2 :]
            return jnp.concatenate([u * cos - v * sin, v * cos + u * sin], -1).astype(BF16)

        kv_k[z, b, rows, :] = turned(_dot(a, wf[0].reshape(D, HEAD), 1, 0))
        kv_v[z, b, :, rows] = _dot(a, wf[1].reshape(D, HEAD), 1, 0).astype(BF16).T
        qv[b, rows, :] = turned(_dot(a, wf[2].reshape(D, HEAD), 1, 0))

    def kv_copies(b, half):
        rows = half_rows(half)
        return (rc(kv_k.at[z, b, rows, :], kv_k.at[z, b, rows, :], kv_s, kv_r.at[b, half], Z),
                rc(kv_v.at[z, b, :, rows], kv_v.at[z, b, :, rows], kv_s, kv_r.at[b, half], Z))

    def q_copy(b, half):
        rows = half_rows(half)
        return rc(qv.at[b, rows, :], qv.at[b + 2, rows, :], q_s, q_r, Z)

    def send_kv(b, half):
        for cp in kv_copies(b, half):
            cp.start()

    def on(b, half):
        @pl.when(b < 6)
        def _():
            send_kv(b, half)

        @pl.when((b >= 6) & (z == 1))
        def _():
            q_copy(b, half).start()

    def core(n):
        return c + n * (oc - c)

    def own_piece(q):
        def body(n, _):
            b, half = 2 * q + core(n // 2), n % 2
            project(b, half)
            on(b, half)

        lax.fori_loop(0, 4, body, None)

    def side_half(t, n):
        isy = n % 2 if t == 0 else 1 - n // 2
        return 2 * (pX + isy * (pY - pX)) + core(n // 2 if t == 0 else n % 2), (isy + t) % 2

    hold = (p == 0) & (z == 1)
    hold_y = p == 3

    def side_pieces(t):
        def body(n, _):
            b, half = side_half(t, n)
            project(b, half)
            if t == 0:
                on(b, half)
            else:
                @pl.when(jnp.logical_not(hold | (hold_y & (n < 2))))
                def _():
                    on(b, half)

        lax.fori_loop(0, 4, body, None)

    for cp in load_tables:
        cp.wait()
    got_given(0)
    own_piece(p)

    bX, bY, bD = 2 * pX + c, 2 * pY + c, 2 * pD + c
    got_a(bX, 0, 1)
    send_a(bX, 0, 3, Y)
    give_a(bX, 0, 1)
    got_a(bY, 1, 2)
    send_a(bY, 1, 3, X)
    give_a(bY, 1, 1)
    got_given(1)
    side_pieces(0)

    iz = row(p, oz, c)

    def give_wo(i, place):
        send(wov.at[i], wov.at[i], wo_s, woc_r.at[place], C)

    got(wov.at[iz], wo_r.at[2 * p + oz], "wo_z")
    for i, zz in ((me, z), (iz, oz)):
        for dev in (X, Y):
            send(wov.at[i], wov.at[i], wo_s, wo_r.at[2 * p + zz], dev)
        give_wo(i, 0)

    e = HEAD**-0.5 * LOG2E
    top_s[...] = jnp.full(top_s.shape, HIDDEN, F32)
    mix_s[...] = jnp.zeros(mix_s.shape, F32)

    def tile(zz, kb, bq, masked, rows):
        s = _dot(kv_k[zz, kb, rows, :], qv[bq], 1, 1)
        if masked:
            ok = lax.broadcasted_iota(jnp.int32, s.shape, 1) >= lax.broadcasted_iota(jnp.int32, s.shape, 0)
            s = jnp.where(ok, s, HIDDEN)
        return s

    every = pl.ds(0, OWN)

    def attend(work, rows=every):
        scores = [[tile(zz, kb, bq, masked, rows) for zz, kb, masked in keys] for bq, keys in work]
        for (bq, keys), ss in zip(work, scores):
            old = top_s[bq]
            top = old
            for s in ss:
                top = jnp.maximum(top, s.max(axis=0, keepdims=True))
            top_s[bq] = top
            keep = jnp.exp2((old - top) * e)
            total = mix_s[bq] * keep
            for (zz, kb, _), s in zip(keys, ss):
                w = jnp.exp2((s - top) * e).astype(BF16)
                total = total + _dot(jnp.concatenate([kv_v[zz, kb, :, rows], jnp.ones((SUM, rows.size), BF16)], axis=0), w, 1, 0)
            mix_s[bq] = total

    @jax.named_scope("pair")
    def pair(zz, kp, qp):
        keys = [(zz, 2 * kp, False), (zz, 2 * kp + 1, False)]
        attend([(2 * qp, keys), (2 * qp + 1, keys)])

    @jax.named_scope("diagonal")
    def diagonal(kp):
        attend([(2 * kp, [(z, 2 * kp, True)]), (2 * kp + 1, [(z, 2 * kp, False), (z, 2 * kp + 1, True)])])

    diagonal(p)

    got_a(bX, 1, 1)
    give_a(bX, 1, 2)
    got_a(bY, 0, 2)
    give_a(bY, 0, 2)
    got_given(2)
    side_pieces(1)
    even = 1 - (x + y) % 2

    def near(n, _):
        @pl.when(n > 0)
        def _():
            diagonal(pX * (n == 1) + pY * (n == 2))

        low = y * (n == 0) + 2 * x * (n == 1) + even * (n == 2)
        high = (y + 2) * (n == 0) + (2 * x + 1) * (n == 1) + (3 - even) * (n == 2)
        pair(z, low, high)

    lax.fori_loop(0, 3, near, None)

    def part_copies():
        return (rc(part.at[0], part.at[1], part_s.at[0], part_r.at[0], Z), rc(part_f.at[0], part_f.at[1], part_s.at[1], part_r.at[1], Z))

    def send_part():
        got(qv.at[pl.ds(8, 2)], q_r, "q")
        pair(z, 3, 4)
        for n in (0, 1):
            mix = mix_s[8 + n]
            total = mix[HEAD : HEAD + 1]
            part[0, n] = (mix[:HEAD] * (1 / total)).astype(BF16)
            part_f[0, n] = jnp.concatenate([top_s[8 + n], total], axis=0)
        for cp in part_copies():
            cp.start()

    @pl.when((z == 0) & (p == 3))
    def _():
        send_part()

    def got_kv(b, half):
        got(kv_k.at[oz, b], kv_r.at[b, half], "kv")

    def got_piece(kp):
        for n in (0, 1):
            for half in (0, 1):
                got_kv(2 * kp + n, half)

    def near_remote(n, _):
        qp = p * (n == 0) + pX * (n == 1) + pY * (n == 2)
        pl.when(qp >= p + oz)(lambda: pair(oz, p, qp))

    @pl.when(p < 3)
    def _():
        got_piece(p)
        lax.fori_loop(0, 3, near_remote, None)

    for half in (0, 1):
        got_a(bD, half, 3)
        give_a(bD, half, 3)
    got_given(3)
    own_piece(pD)

    @pl.when(hold)
    def _():
        for n in range(4):
            send_kv(*side_half(1, n))

    @pl.when(hold_y)
    def _():
        for n in range(2):
            send_kv(*side_half(1, n))

    diagonal(pD)

    def far(n, _):
        low = (1 - even) * (n == 0) + 2 * (1 - x) * (n == 1) + (1 - y) * (n == 2)
        high = (2 + even) * (n == 0) + (3 - 2 * x) * (n == 1) + (3 - y) * (n == 2)
        pair(z, low, high)

    lax.fori_loop(0, 3, far, None)

    iX, iY, iD = row(pX, z, c), row(pY, z, c), row(pD, z, c)
    for n, (i, q, dev) in enumerate(((iX, pX, Y), (iY, pY, X))):
        got(wov.at[i], wo_r.at[2 * q + z], f"wo{n}")
        rows = pl.ds(n * 64, 64)
        send(wov.at[i, rows], wov.at[i, rows], wo_s, wod_r.at[n], dev)
        give_wo(i, 1 + n)

    def wo_rest():
        for n in (0, 1):
            got(wov.at[iD, pl.ds(n * 64, 64)], wod_r.at[n], f"wod{n}")
        send(wov.at[iD], wov.at[iD], wo_s, wo_r.at[2 * pD + z], Z)
        give_wo(iD, 3)
        for n, q in enumerate((pX, pY)):
            i = row(q, oz, c)
            got(wov.at[i], wo_r.at[2 * q + oz], f"wo_oz{n}")
            give_wo(i, 1 + n)

    cols = pl.ds(pl.multiple_of(head * HEAD, HEAD), HEAD)

    def o_copy(b):
        place = 2 * ((b // 2 % 2 + y) % 2) + (b // 4 + x) % 2
        return rc(qv.at[b], og.at[:, cols], o_s, o_r.at[place], row(b // 2, z, b % 2))

    by_y = 2 * pD + 1

    def finish(b):
        with jax.named_scope("finish"):
            mix = mix_s[b]
            qv[b] = (mix[:HEAD] * (1 / mix[HEAD : HEAD + 1])).T.astype(BF16)

        @pl.when((b != mine) & (b != by_y))
        def _():
            o_copy(b).start()

        @pl.when(b == by_y)
        def _():
            send(qv.at[b], orl, o_s, orl_r, Y)

    def finish_pieces(first, last):
        lax.fori_loop(2 * first, 2 * last, lambda n, _: finish(n + 1 - 2 * (n % 2)), None)

    first, last = (3 - p) // 3, p // 3
    kp0, kp1 = p - 2 * last, first
    done0, done1 = first, 2 - p // 2 * (3 - p)

    def remote_piece(kp, done):
        got_piece(kp)

        def body(qp, _):
            pair(oz, kp, qp)
            pl.when(qp < done)(lambda: finish_pieces(qp, qp + 1))

        lax.fori_loop(kp + oz, 4, body, None)

    def remote_blocks(kp, done):
        for n in (0, 1):
            block = 2 * kp + core(n)
            got_kv(block, 0)
            got_kv(block, 1)

            def body(qp, _):
                with jax.named_scope("one"):
                    attend([(2 * qp + m, [(oz, block, False)]) for m in (0, 1)])
                if n:
                    pl.when(qp < done)(lambda: finish_pieces(qp, qp + 1))

            lax.fori_loop(kp + oz, 4, body, None)

    def last_piece(kp):
        block = 2 * kp + core(0)
        got_kv(block, 0)
        got_kv(block, 1)

        def piece(n):
            return z * (kp + oz + n) + oz * (3 - n)

        def first(n, _):
            with jax.named_scope("one"):
                attend([(2 * piece(n) + m, [(oz, block, False)]) for m in (0, 1)])

        lax.fori_loop(0, 4 - kp - oz, first, None)
        wo_rest()
        block2 = 2 * kp + core(1)
        for k in (0, 1):
            half = k + last * (1 - 2 * k)
            got_kv(block2, half)

            def second(n, _):
                qp = piece(n)
                work = [(2 * qp + m, [(oz, block2, False)]) for m in (1, 0)]
                if k:
                    for one in work:
                        attend([one], half_rows(half))

                        @pl.when((qp < 3) | (z == 0))
                        def _():
                            finish(one[0])

                else:
                    attend(work, half_rows(half))

            lax.fori_loop(0, 4 - kp - oz, second, None)

    finish_pieces(0, oz)

    @pl.when(last == 0)
    def _():
        pl.when(pD >= p + oz)(lambda: pair(oz, p, pD))
        finish_pieces(oz, done0 + oz)

    @pl.when(last == 1)
    def _():
        remote_piece(kp0, 0)

    @pl.when((z == 0) & (p < 3))
    def _():
        send_part()


    @pl.when(last == 0)
    def _():
        remote_piece(kp1, done1 + oz)

    @pl.when(last == 1)
    def _():
        remote_blocks(kp1, done1 + oz)

    last_piece(3 - kp0 - kp1)

    @pl.when(z == 1)
    def _():
        got(qv.at[pl.ds(0, 2)], q_s, "q_left")
        got(part.at[1], part_r.at[0], "part")
        got(part_f.at[1], part_r.at[1], "part")
        for n in (1, 0):
            old, came, count = top_s[6 + n], part_f[1, n, 0:1], part_f[1, n, 1:2]
            top = jnp.maximum(old, came)
            keep, add = jnp.exp2((old - top) * e), jnp.exp2((came - top) * e) * count
            mix = mix_s[6 + n]
            more = jnp.concatenate([part[1, n].astype(F32) * add, jnp.broadcast_to(add, (SUM, OWN))], axis=0)
            mix_s[6 + n] = mix * keep + more
            finish(6 + n)

    og[:, cols] = qv[mine]
    def relay():
        from_y = pl.ds(pl.multiple_of((2 * pY + c) * HEAD, HEAD), HEAD)
        return rc(orl, og.at[:, from_y], orl_s, o_r.at[3], row(pX, z, 1))

    def heads(q):
        return pl.ds(pl.multiple_of(q * 2 * HEAD, 2 * HEAD), 2 * HEAD)

    third, fourth = 3 - c, 2 + c
    for step, (k, q) in enumerate(((0, p), (1, pX), (third, pD + c * (pY - pD)), (fourth, pY + c * (pD - pY)))):
        if step == 1:
            got(orl, orl_r, "relay")
            relay().start()
        if step == 2:
            i = row(pD, oz, c)
            got(wov.at[i], wo_r.at[2 * pD + oz], "wo_dz")
            give_wo(i, 3)
        got(wov.at[pl.ds(0, 2)], woc_r.at[k], "wo_c")
        got(og.at[:, heads(q)] if step else qv.at[0], o_r.at[k], f"og{step}")

        def out(n, _):
            with jax.named_scope("out"):
                for t in (2 * n, 2 * n + 1):
                    cols = pl.ds(pl.multiple_of(t * 512, 512), 512)
                    u = _dot(og[:, heads(q)], wov[pl.ds(4 * q, 4), :, cols].reshape(2 * HEAD, 512), 1, 0)
                    for m in range(2):
                        rows = pl.ds(m * HEAD, HEAD)
                        v = u[m * HEAD : (m + 1) * HEAD]
                        if step:
                            v = mix_s[2 * t + m, :HEAD, :] + v
                        if step < 3:
                            mix_s[2 * t + m, :HEAD, :] = v
                        else:
                            y_ref[rows, cols] = (y_ref[rows, cols].astype(F32) + v).astype(BF16)

        lax.fori_loop(0, D // 1024, out, None)

    got(wf, w_s.at[0])
    got(ws.at[:, pl.ds(0, 6)], w_s.at[1])
    got(av.at[pl.ds(0, 7)], a_s)
    got(wov.at[pl.ds(0, 15)], wo_s)
    got(kv_k.at[:, pl.ds(0, 6)], kv_s)
    got(qv.at[pl.ds(0, 7)], o_s)
    relay().wait_send()

    @pl.when(z == 0)
    def _():
        for cp in part_copies():
            cp.wait_send()


def tables():
    half = HEAD // 2
    rate = (THETA ** (-np.arange(half, dtype=np.float64) / half))[None]
    fine = np.arange(OWN, dtype=np.float64)[:, None] * rate
    coarse = np.arange(16, dtype=np.float64)[:, None] * OWN * rate
    return (np.stack([np.cos(t), np.sin(t)]).astype(np.float32) for t in (fine, coarse))


def solution(mesh):
    def step(x, gain, wq, wk, wv, wo):
        fine, coarse = tables()
        anywhere = pl.BlockSpec(memory_space=pltpu.HBM)
        dma = pltpu.SemaphoreType.DMA
        return pl.pallas_call(
            kernel,
            out_shape=pltpu.VMEM((OWN, D), BF16),
            in_specs=[anywhere] * 8,
            out_specs=pl.BlockSpec(memory_space=pltpu.VMEM),
            scratch_shapes=[
                pltpu.VMEM((D,), BF16),
                pltpu.VMEM((2, OWN, HEAD // 2), F32),
                pltpu.VMEM((2, 16, HEAD // 2), F32),
                pltpu.VMEM((8, OWN, D), BF16),
                pltpu.VMEM((3, 128, D), BF16),
                pltpu.VMEM((3, 16, 128, HEAD), BF16),
                pltpu.VMEM((3, 8, 128, HEAD), BF16),
                pltpu.VMEM((16, 128, D), BF16),
                pltpu.VMEM((2, 8, OWN, HEAD), BF16),
                pltpu.VMEM((2, 8, HEAD, OWN), BF16),
                pltpu.VMEM((10, OWN, HEAD), BF16),
                pltpu.VMEM((OWN, D), BF16),
                pltpu.VMEM((10, 1, OWN), F32),
                pltpu.VMEM((10, HEAD + SUM, OWN), F32),
                pltpu.VMEM((2, 2, HEAD, OWN), BF16),
                pltpu.VMEM((2, 2, 2, OWN), F32),
                pltpu.VMEM((OWN, HEAD), BF16),
                dma((8,)),
                dma((2,)), dma((8,)), dma(()), dma((8,)),
                dma(()), dma((4, 2)), dma((4,)),
                dma(()), dma((8,)), dma((2,)), dma((4,)),
                dma(()), dma((8, 2)), dma(()), dma((4,)), dma(()), dma(()),
                dma(()), dma(()), dma((2,)), dma((2,)),
            ],
            compiler_params=pltpu.CompilerParams(collective_id=0, has_side_effects=True, vmem_limit_bytes=61 * 2**20),
            name="decoder_attention",
        )(x, gain, wq, wk, wv, wo, jnp.asarray(fine), jnp.asarray(coarse))

    tokens, whole = P(("dp", "sp"), None), P("sp", None)
    return jax.shard_map(
        step,
        mesh=mesh,
        in_specs=(tokens, P(None), whole, whole, whole, whole),
        out_specs=tokens,
        check_vma=False,
    )
```

```python
import functools

import jax
import jax.numpy as jnp
import numpy as np
from jax import lax
from jax.experimental import pallas as pl
from jax.experimental.pallas import tpu as pltpu
from jax.sharding import PartitionSpec as P

HIDDEN = -jnp.inf
LOG2E = 1.4426950408889634
HEAD = 256
THETA = 10000
D = 2048
OWN = 512
HALF = 256
SUM = 8
F32, BF16 = jnp.float32, jnp.bfloat16
MESH = pl.DeviceIdType.MESH


def _dot(a, b, ca, cb):
    return lax.dot_general(a, b, (((ca,), (cb,)), ((), ())), preferred_element_type=F32)


def kernel(x_h, gain_h, wq_h, wk_h, wv_h, wo_h, fine_h, coarse_h, y_ref,
           gain_ref, fine_ref, coarse_ref, av, wi, wf, ws, wov, kv_k, kv_v, qv, og, top_s, mix_s, part, part_f, orl,
           ld, w_s, wf_r, wfc_r, ws_r, a_s, a_r, ac_r, wo_s, wo_r, wod_r, woc_r, kv_s, kv_r, o_s, o_r, orl_s, orl_r, q_s, q_r, part_s, part_r):
    me = lax.axis_index("sp")
    x, y, z, c, p = me // 8, (me // 4) % 2, (me // 2) % 2, me % 2, me // 4
    X, Y, Z, C = me + 8 - 16 * x, me + 4 - 8 * y, me + 2 - 4 * z, me + 1 - 2 * c
    Dg = X + Y - me
    pX, pY, pD = X // 4, Y // 4, Dg // 4
    oc, oz = 1 - c, 1 - z
    head = 2 * p + c
    mine = 2 * p + c
    planes = (p, pX, pY, pD)

    def row(q, zz, cc):
        return 4 * q + 2 * zz + cc

    def rc(src, dst, ssem, rsem, dev):
        return pltpu.make_async_remote_copy(src_ref=src, dst_ref=dst, send_sem=ssem, recv_sem=rsem, device_id={"sp": dev}, device_id_type=MESH)

    def got(ref, sem, name="wait"):
        with jax.named_scope(name):
            pltpu.make_async_copy(ref, ref, sem).wait()

    def local(src, dst, n):
        cp = pltpu.make_async_copy(src, dst, ld.at[n])
        cp.start()
        return cp

    loads = (wk_h, wv_h, wq_h)
    for n, w in enumerate(loads):
        local(w, wi.at[n], 0)
    here = pl.ds(pl.multiple_of(head * HEAD, HEAD), HEAD)
    other = pl.ds(pl.multiple_of((2 * p + oc) * HEAD, HEAD), HEAD)
    sme = 2 * p + z
    load_x = local(x_h, y_ref, 1)
    load_gain = local(gain_h, gain_ref, 2)
    load_tables = (local(fine_h, fine_ref, 3), local(coarse_h, coarse_ref, 4))
    load_wo = local(wo_h, wov.at[me], 5)
    for n, w in enumerate(loads):
        local(w.at[:, here], wf.at[n, me], 6)
        local(w.at[:, other], ws.at[n, sme], 7)

    barrier = pltpu.get_barrier_semaphore()
    partners = (X, Y, Dg, X + C - me, Y + C - me, Dg + C - me, C, Z)
    for dev in partners:
        pl.semaphore_signal(barrier, inc=1, device_id={"sp": dev}, device_id_type=MESH)
    with jax.named_scope("barrier"):
        pl.semaphore_wait(barrier, len(partners))

    def send(src, dst, ssem, rsem, dev):
        rc(src, dst, ssem, rsem, dev).start()

    got(wi, ld.at[0], "load")
    send(wi.at[:, :, here], wf.at[:, me], w_s.at[0], wf_r.at[sme], Z)
    send(wi.at[:, :, other], ws.at[:, sme], w_s.at[0], ws_r.at[sme], Z)
    for dev, q in ((X, pX), (Y, pY), (Dg, pD)):
        for hd, dst, rs in ((2 * q + c, wf.at[:, me], wf_r.at[sme]), (2 * q + oc, ws.at[:, sme], ws_r.at[sme])):
            cols = pl.ds(pl.multiple_of(hd * HEAD, HEAD), HEAD)
            send(wi.at[:, :, cols], dst, w_s.at[1], rs, dev)

    def wf_on(q, zz):
        i = row(q, zz, c)
        send(wf.at[:, i], wf.at[:, i], w_s.at[0], wf_r.at[2 * q + zz], Z)

    def ws_on(q, zz, on):
        i, s = row(q, zz, c), 2 * q + zz
        if on:
            send(ws.at[:, s], ws.at[:, s], w_s.at[0], ws_r.at[s], Z)
        send(ws.at[:, s], wf.at[:, i], w_s.at[0], wfc_r, C)

    def got_wf(n, q, zz):
        got(wf.at[:, row(q, zz, c)], wf_r.at[2 * q + zz], f"wf{n}")

    def got_ws(n, q, zz):
        got(ws.at[:, 2 * q + zz], ws_r.at[2 * q + zz], f"ws{n}")

    got(wf.at[:, me], ld.at[6])
    got(ws.at[:, sme], ld.at[7])
    ws_on(p, z, False)

    load_x.wait()
    load_gain.wait()

    @jax.named_scope("norm")
    def norm(n, _):
        rows = pl.ds(pl.multiple_of(n * 128, 128), 128)
        wide = y_ref[rows, :].astype(F32)
        scale = lax.rsqrt(jnp.mean(wide * wide, -1, keepdims=True) + 1e-6)
        av[mine, rows, :] = (wide * scale * gain_ref[...].reshape(1, D).astype(F32)).astype(BF16)

    lax.fori_loop(0, OWN // 128, norm, None)

    def half_rows(half):
        return pl.ds(half * HALF if isinstance(half, int) else pl.multiple_of(half * HALF, HALF), HALF)

    def send_a(b, half, place, dev):
        rows = half_rows(half)
        send(av.at[b, rows], av.at[b, rows], a_s, a_r.at[place, half], dev)

    def give_a(b, half, n):
        rows = half_rows(half)
        send(av.at[b, rows], av.at[b, rows], a_s, ac_r.at[n], C)

    def got_a(b, half, place):
        got(av.at[b, half_rows(half)], a_r.at[place, half], f"a{half}")

    def got_given(n):
        got(av.at[0], ac_r.at[n], "given")

    send_a(mine, 0, 1, X)
    send_a(mine, 1, 2, Y)
    send_a(mine, 1, 1, X)
    send_a(mine, 0, 2, Y)
    give_a(mine, 0, 0)
    give_a(mine, 1, 0)

    for n, q in ((1, pX), (2, pY)):
        got_wf(n, q, z)
        wf_on(q, z)
    for n, q in ((1, pX), (2, pY)):
        got_ws(n, q, z)
        ws_on(q, z, True)
    got_wf(3, pD, z)
    wf_on(pD, z)
    got_ws(3, pD, z)
    ws_on(pD, z, True)
    load_wo.wait()
    send(wov.at[me], wov.at[me], wo_s, wo_r.at[sme], Z)

    for n, q in enumerate(planes):
        got_wf(n, q, oz)
        got_ws(n, q, oz)
        ws_on(q, oz, False)
    got(wf.at[:, pl.ds(0, 8)], wfc_r, "wfc")

    @jax.named_scope("project")
    def project(b, half):
        rows = half_rows(half)
        a = av[b, rows, :]
        i = 4 * (b // 2) + 2 * z + b % 2
        cb, sb = coarse_ref[0, pl.ds(i, 1), :], coarse_ref[1, pl.ds(i, 1), :]
        cf, sf = fine_ref[0, rows, :], fine_ref[1, rows, :]
        cos = cb * cf - sb * sf
        sin = sb * cf + cb * sf

        def turned(t):
            t = t.astype(BF16).astype(F32)
            u, v = t[:, : HEAD // 2], t[:, HEAD // 2 :]
            return jnp.concatenate([u * cos - v * sin, v * cos + u * sin], -1).astype(BF16)

        kv_k[z, b, rows, :] = turned(_dot(a, wf[0].reshape(D, HEAD), 1, 0))
        kv_v[z, b, :, rows] = _dot(a, wf[1].reshape(D, HEAD), 1, 0).astype(BF16).T
        qv[b, rows, :] = turned(_dot(a, wf[2].reshape(D, HEAD), 1, 0))

    def kv_copies(b, half):
        rows = half_rows(half)
        return (rc(kv_k.at[z, b, rows, :], kv_k.at[z, b, rows, :], kv_s, kv_r.at[b, half], Z),
                rc(kv_v.at[z, b, :, rows], kv_v.at[z, b, :, rows], kv_s, kv_r.at[b, half], Z))

    def q_copy(b, half):
        rows = half_rows(half)
        return rc(qv.at[b, rows, :], qv.at[b + 2, rows, :], q_s, q_r, Z)

    def send_kv(b, half):
        for cp in kv_copies(b, half):
            cp.start()

    def on(b, half):
        @pl.when(b < 6)
        def _():
            send_kv(b, half)

        @pl.when((b >= 6) & (z == 1))
        def _():
            q_copy(b, half).start()

    def core(n):
        return c + n * (oc - c)

    def own_piece(q):
        def body(n, _):
            b, half = 2 * q + core(n // 2), n % 2
            project(b, half)
            on(b, half)

        lax.fori_loop(0, 4, body, None)

    def side_half(t, n):
        isy = n % 2 if t == 0 else 1 - n // 2
        return 2 * (pX + isy * (pY - pX)) + core(n // 2 if t == 0 else n % 2), (isy + t) % 2

    hold = (p == 0) & (z == 1)
    hold_y = p == 3

    def side_pieces(t):
        def body(n, _):
            b, half = side_half(t, n)
            project(b, half)
            if t == 0:
                on(b, half)
            else:
                @pl.when(jnp.logical_not(hold | (hold_y & (n < 2))))
                def _():
                    on(b, half)

        lax.fori_loop(0, 4, body, None)

    for cp in load_tables:
        cp.wait()
    got_given(0)
    own_piece(p)

    bX, bY, bD = 2 * pX + c, 2 * pY + c, 2 * pD + c
    got_a(bX, 0, 1)
    send_a(bX, 0, 3, Y)
    give_a(bX, 0, 1)
    got_a(bY, 1, 2)
    send_a(bY, 1, 3, X)
    give_a(bY, 1, 1)
    got_given(1)
    side_pieces(0)

    iz = row(p, oz, c)

    def give_wo(i, place):
        send(wov.at[i], wov.at[i], wo_s, woc_r.at[place], C)

    got(wov.at[iz], wo_r.at[2 * p + oz], "wo_z")
    for i, zz in ((me, z), (iz, oz)):
        for dev in (X, Y):
            send(wov.at[i], wov.at[i], wo_s, wo_r.at[2 * p + zz], dev)
        give_wo(i, 0)

    e = HEAD**-0.5 * LOG2E
    top_s[...] = jnp.full(top_s.shape, HIDDEN, F32)
    mix_s[...] = jnp.zeros(mix_s.shape, F32)

    def tile(zz, kb, bq, masked, rows):
        s = _dot(kv_k[zz, kb, rows, :], qv[bq], 1, 1)
        if masked:
            ok = lax.broadcasted_iota(jnp.int32, s.shape, 1) >= lax.broadcasted_iota(jnp.int32, s.shape, 0)
            s = jnp.where(ok, s, HIDDEN)
        return s

    every = pl.ds(0, OWN)

    def attend(work, rows=every):
        scores = [[tile(zz, kb, bq, masked, rows) for zz, kb, masked in keys] for bq, keys in work]
        for (bq, keys), ss in zip(work, scores):
            old = top_s[bq]
            top = old
            for s in ss:
                top = jnp.maximum(top, s.max(axis=0, keepdims=True))
            top_s[bq] = top
            keep = jnp.exp2((old - top) * e)
            total = mix_s[bq] * keep
            for (zz, kb, _), s in zip(keys, ss):
                w = jnp.exp2((s - top) * e).astype(BF16)
                total = total + _dot(jnp.concatenate([kv_v[zz, kb, :, rows], jnp.ones((SUM, rows.size), BF16)], axis=0), w, 1, 0)
            mix_s[bq] = total

    @jax.named_scope("pair")
    def pair(zz, kp, qp):
        keys = [(zz, 2 * kp, False), (zz, 2 * kp + 1, False)]
        attend([(2 * qp, keys), (2 * qp + 1, keys)])

    @jax.named_scope("diagonal")
    def diagonal(kp):
        attend([(2 * kp, [(z, 2 * kp, True)]), (2 * kp + 1, [(z, 2 * kp, False), (z, 2 * kp + 1, True)])])

    diagonal(p)

    got_a(bX, 1, 1)
    give_a(bX, 1, 2)
    got_a(bY, 0, 2)
    give_a(bY, 0, 2)
    got_given(2)
    side_pieces(1)
    even = 1 - (x + y) % 2

    def near(n, _):
        @pl.when(n > 0)
        def _():
            diagonal(pX * (n == 1) + pY * (n == 2))

        low = y * (n == 0) + 2 * x * (n == 1) + even * (n == 2)
        high = (y + 2) * (n == 0) + (2 * x + 1) * (n == 1) + (3 - even) * (n == 2)
        pair(z, low, high)

    lax.fori_loop(0, 3, near, None)

    def part_copies():
        return (rc(part.at[0], part.at[1], part_s.at[0], part_r.at[0], Z), rc(part_f.at[0], part_f.at[1], part_s.at[1], part_r.at[1], Z))

    def send_part():
        got(qv.at[pl.ds(8, 2)], q_r, "q")
        pair(z, 3, 4)
        for n in (0, 1):
            mix = mix_s[8 + n]
            total = mix[HEAD : HEAD + 1]
            part[0, n] = (mix[:HEAD] * (1 / total)).astype(BF16)
            part_f[0, n] = jnp.concatenate([top_s[8 + n], total], axis=0)
        for cp in part_copies():
            cp.start()

    @pl.when((z == 0) & (p == 3))
    def _():
        send_part()

    def got_kv(b, half):
        got(kv_k.at[oz, b], kv_r.at[b, half], "kv")

    def got_piece(kp):
        for n in (0, 1):
            for half in (0, 1):
                got_kv(2 * kp + n, half)

    def near_remote(n, _):
        qp = p * (n == 0) + pX * (n == 1) + pY * (n == 2)
        pl.when(qp >= p + oz)(lambda: pair(oz, p, qp))

    @pl.when(p < 3)
    def _():
        got_piece(p)
        lax.fori_loop(0, 3, near_remote, None)

    for half in (0, 1):
        got_a(bD, half, 3)
        give_a(bD, half, 3)
    got_given(3)
    own_piece(pD)

    @pl.when(hold)
    def _():
        for n in range(4):
            send_kv(*side_half(1, n))

    @pl.when(hold_y)
    def _():
        for n in range(2):
            send_kv(*side_half(1, n))

    diagonal(pD)

    def far(n, _):
        low = (1 - even) * (n == 0) + 2 * (1 - x) * (n == 1) + (1 - y) * (n == 2)
        high = (2 + even) * (n == 0) + (3 - 2 * x) * (n == 1) + (3 - y) * (n == 2)
        pair(z, low, high)

    lax.fori_loop(0, 3, far, None)

    iX, iY, iD = row(pX, z, c), row(pY, z, c), row(pD, z, c)
    for n, (i, q, dev) in enumerate(((iX, pX, Y), (iY, pY, X))):
        got(wov.at[i], wo_r.at[2 * q + z], f"wo{n}")
        rows = pl.ds(n * 64, 64)
        send(wov.at[i, rows], wov.at[i, rows], wo_s, wod_r.at[n], dev)
        give_wo(i, 1 + n)

    def wo_rest():
        for n in (0, 1):
            got(wov.at[iD, pl.ds(n * 64, 64)], wod_r.at[n], f"wod{n}")
        send(wov.at[iD], wov.at[iD], wo_s, wo_r.at[2 * pD + z], Z)
        give_wo(iD, 3)
        for n, q in enumerate((pX, pY)):
            i = row(q, oz, c)
            got(wov.at[i], wo_r.at[2 * q + oz], f"wo_oz{n}")
            give_wo(i, 1 + n)

    cols = pl.ds(pl.multiple_of(head * HEAD, HEAD), HEAD)

    def o_copy(b):
        place = 2 * ((b // 2 % 2 + y) % 2) + (b // 4 + x) % 2
        return rc(qv.at[b], og.at[:, cols], o_s, o_r.at[place], row(b // 2, z, b % 2))

    by_y = 2 * pD + 1

    def finish(b):
        with jax.named_scope("finish"):
            mix = mix_s[b]
            qv[b] = (mix[:HEAD] * (1 / mix[HEAD : HEAD + 1])).T.astype(BF16)

        @pl.when((b != mine) & (b != by_y))
        def _():
            o_copy(b).start()

        @pl.when(b == by_y)
        def _():
            send(qv.at[b], orl, o_s, orl_r, Y)

    def finish_pieces(first, last):
        lax.fori_loop(2 * first, 2 * last, lambda n, _: finish(n + 1 - 2 * (n % 2)), None)

    first, last = (3 - p) // 3, p // 3
    kp0, kp1 = p - 2 * last, first
    done0, done1 = first, 2 - p // 2 * (3 - p)

    def remote_piece(kp, done):
        got_piece(kp)

        def body(qp, _):
            pair(oz, kp, qp)
            pl.when(qp < done)(lambda: finish_pieces(qp, qp + 1))

        lax.fori_loop(kp + oz, 4, body, None)

    def remote_blocks(kp, done):
        for n in (0, 1):
            block = 2 * kp + core(n)
            got_kv(block, 0)
            got_kv(block, 1)

            def body(qp, _):
                with jax.named_scope("one"):
                    attend([(2 * qp + m, [(oz, block, False)]) for m in (0, 1)])
                if n:
                    pl.when(qp < done)(lambda: finish_pieces(qp, qp + 1))

            lax.fori_loop(kp + oz, 4, body, None)

    def last_piece(kp):
        block = 2 * kp + core(0)
        got_kv(block, 0)
        got_kv(block, 1)

        def piece(n):
            return z * (kp + oz + n) + oz * (3 - n)

        def first(n, _):
            with jax.named_scope("one"):
                attend([(2 * piece(n) + m, [(oz, block, False)]) for m in (0, 1)])

        lax.fori_loop(0, 4 - kp - oz, first, None)
        wo_rest()
        block2 = 2 * kp + core(1)
        for k in (0, 1):
            half = k + last * (1 - 2 * k)
            got_kv(block2, half)

            def second(n, _):
                qp = piece(n)
                work = [(2 * qp + m, [(oz, block2, False)]) for m in (1, 0)]
                if k:
                    for one in work:
                        attend([one], half_rows(half))

                        @pl.when((qp < 3) | (z == 0))
                        def _():
                            finish(one[0])

                else:
                    attend(work, half_rows(half))

            lax.fori_loop(0, 4 - kp - oz, second, None)

    finish_pieces(0, oz)

    @pl.when(last == 0)
    def _():
        pl.when(pD >= p + oz)(lambda: pair(oz, p, pD))
        finish_pieces(oz, done0 + oz)

    @pl.when(last == 1)
    def _():
        remote_piece(kp0, 0)

    @pl.when((z == 0) & (p < 3))
    def _():
        send_part()


    @pl.when(last == 0)
    def _():
        remote_piece(kp1, done1 + oz)

    @pl.when(last == 1)
    def _():
        remote_blocks(kp1, done1 + oz)

    last_piece(3 - kp0 - kp1)

    @pl.when(z == 1)
    def _():
        got(qv.at[pl.ds(0, 2)], q_s, "q_left")
        got(part.at[1], part_r.at[0], "part")
        got(part_f.at[1], part_r.at[1], "part")
        for n in (1, 0):
            old, came, count = top_s[6 + n], part_f[1, n, 0:1], part_f[1, n, 1:2]
            top = jnp.maximum(old, came)
            keep, add = jnp.exp2((old - top) * e), jnp.exp2((came - top) * e) * count
            mix = mix_s[6 + n]
            more = jnp.concatenate([part[1, n].astype(F32) * add, jnp.broadcast_to(add, (SUM, OWN))], axis=0)
            mix_s[6 + n] = mix * keep + more
            finish(6 + n)

    og[:, cols] = qv[mine]
    def relay():
        from_y = pl.ds(pl.multiple_of((2 * pY + c) * HEAD, HEAD), HEAD)
        return rc(orl, og.at[:, from_y], orl_s, o_r.at[3], row(pX, z, 1))

    def heads(q):
        return pl.ds(pl.multiple_of(q * 2 * HEAD, 2 * HEAD), 2 * HEAD)

    third, fourth = 3 - c, 2 + c
    for step, (k, q) in enumerate(((0, p), (1, pX), (third, pD + c * (pY - pD)), (fourth, pY + c * (pD - pY)))):
        if step == 1:
            got(orl, orl_r, "relay")
            relay().start()
        if step == 2:
            i = row(pD, oz, c)
            got(wov.at[i], wo_r.at[2 * pD + oz], "wo_dz")
            give_wo(i, 3)
        got(wov.at[pl.ds(0, 2)], woc_r.at[k], "wo_c")
        got(og.at[:, heads(q)] if step else qv.at[0], o_r.at[k], f"og{step}")

        def out(n, _):
            with jax.named_scope("out"):
                for t in (2 * n, 2 * n + 1):
                    cols = pl.ds(pl.multiple_of(t * 512, 512), 512)
                    u = _dot(og[:, heads(q)], wov[pl.ds(4 * q, 4), :, cols].reshape(2 * HEAD, 512), 1, 0)
                    for m in range(2):
                        rows = pl.ds(m * HEAD, HEAD)
                        v = u[m * HEAD : (m + 1) * HEAD]
                        if step:
                            v = mix_s[2 * t + m, :HEAD, :] + v
                        if step < 3:
                            mix_s[2 * t + m, :HEAD, :] = v
                        else:
                            y_ref[rows, cols] = (y_ref[rows, cols].astype(F32) + v).astype(BF16)

        lax.fori_loop(0, D // 1024, out, None)

    got(wf, w_s.at[0])
    got(ws.at[:, pl.ds(0, 6)], w_s.at[1])
    got(av.at[pl.ds(0, 7)], a_s)
    got(wov.at[pl.ds(0, 15)], wo_s)
    got(kv_k.at[:, pl.ds(0, 6)], kv_s)
    got(qv.at[pl.ds(0, 7)], o_s)
    relay().wait_send()

    @pl.when(z == 0)
    def _():
        for cp in part_copies():
            cp.wait_send()


def tables():
    half = HEAD // 2
    rate = (THETA ** (-np.arange(half, dtype=np.float64) / half))[None]
    fine = np.arange(OWN, dtype=np.float64)[:, None] * rate
    coarse = np.arange(16, dtype=np.float64)[:, None] * OWN * rate
    return (np.stack([np.cos(t), np.sin(t)]).astype(np.float32) for t in (fine, coarse))


def solution(mesh):
    def step(x, gain, wq, wk, wv, wo):
        fine, coarse = tables()
        anywhere = pl.BlockSpec(memory_space=pltpu.HBM)
        dma = pltpu.SemaphoreType.DMA
        return pl.pallas_call(
            kernel,
            out_shape=pltpu.VMEM((OWN, D), BF16),
            in_specs=[anywhere] * 8,
            out_specs=pl.BlockSpec(memory_space=pltpu.VMEM),
            scratch_shapes=[
                pltpu.VMEM((D,), BF16),
                pltpu.VMEM((2, OWN, HEAD // 2), F32),
                pltpu.VMEM((2, 16, HEAD // 2), F32),
                pltpu.VMEM((8, OWN, D), BF16),
                pltpu.VMEM((3, 128, D), BF16),
                pltpu.VMEM((3, 16, 128, HEAD), BF16),
                pltpu.VMEM((3, 8, 128, HEAD), BF16),
                pltpu.VMEM((16, 128, D), BF16),
                pltpu.VMEM((2, 8, OWN, HEAD), BF16),
                pltpu.VMEM((2, 8, HEAD, OWN), BF16),
                pltpu.VMEM((10, OWN, HEAD), BF16),
                pltpu.VMEM((OWN, D), BF16),
                pltpu.VMEM((10, 1, OWN), F32),
                pltpu.VMEM((10, HEAD + SUM, OWN), F32),
                pltpu.VMEM((2, 2, HEAD, OWN), BF16),
                pltpu.VMEM((2, 2, 2, OWN), F32),
                pltpu.VMEM((OWN, HEAD), BF16),
                dma((8,)),
                dma((2,)), dma((8,)), dma(()), dma((8,)),
                dma(()), dma((4, 2)), dma((4,)),
                dma(()), dma((8,)), dma((2,)), dma((4,)),
                dma(()), dma((8, 2)), dma(()), dma((4,)), dma(()), dma(()),
                dma(()), dma(()), dma((2,)), dma((2,)),
            ],
            compiler_params=pltpu.CompilerParams(collective_id=0, has_side_effects=True, vmem_limit_bytes=61 * 2**20),
            name="decoder_attention",
        )(x, gain, wq, wk, wv, wo, jnp.asarray(fine), jnp.asarray(coarse))

    tokens, whole = P(("dp", "sp"), None), P("sp", None)
    return jax.shard_map(
        step,
        mesh=mesh,
        in_specs=(tokens, P(None), whole, whole, whole, whole),
        out_specs=tokens,
        check_vma=False,
    )
```
